32 devices in a mesh: seg: 8 (over z, core), tok: 4 (over y, x).
Axes of the slice: x: 2, y: 2, z: 4, core: 2. Of those that a mesh axis runs over, the one named last changes fastest.
Arguments:
- queries: bfloat16 [2, 8, 2, 5120, 256], P(None, 'seg', None, 'tok'), may hold values from -6 to 6
- key_vectors: bfloat16 [2, 8, 2, 5120, 256], P(None, 'seg', None, 'tok'), may hold values from -6 to 6
- values: bfloat16 [2, 8, 2, 5120, 256], P(None, 'seg', None, 'tok'), may hold values from -6 to 6
- token_rates: float32 [2, 8, 2, 5120], P(None, 'seg', None, 'tok'), may hold values from 0.05 to 3
- fast_weights: float32 [8, 3, 256, 256], P('seg', None, None, 'tok'), may hold values from -0.375 to 0.375
- momenta: float32 [8, 3, 256, 256], P('seg', None, None, 'tok'), may hold values from -3 to 3
- fresh_weights: float32 [3, 256, 256], P(None, None, 'tok'), may hold values from -0.375 to 0.375
- fresh_momenta: float32 [3, 256, 256], P(None, None, 'tok'), may hold values from -3 to 3
Outputs:
- outputs: bfloat16 [2, 8, 2, 5120, 256], P(None, 'seg', None, 'tok')
- final_weights: float32 [8, 3, 256, 256], P('seg', None, None, 'tok')
- final_momenta: float32 [8, 3, 256, 256], P('seg', None, None, 'tok')
The draws below stay inside these ranges and needn't reach their ends.
All inputs are finite; a program needn't handle non-finite values.
Results may differ from the reference program's by a relative error of at most 0.033.
Values may be sent and summed in bfloat16 or wider, within the bound.
A program may use at most 64 MiB of HBM per device.

```python
import math
import jax
import jax.numpy as jnp
from jax import lax

HEAD = 256
GROUPS = 2
STEPS = 2
SEGS = 8
GROUP = 5120


def draw_token_rates(key, part):
    shape = (STEPS, SEGS, GROUPS, GROUP)
    level = jnp.exp(jax.random.uniform(key, shape, jnp.float32, math.log(0.05), 0.0))
    ramp = 1.0 + 2.0 * jnp.arange(GROUP, dtype=jnp.float32) / GROUP
    return level * ramp


def block_levels(stream_key, extent, shards, least, top_value):
    level = 1.0
    for dim, blocks in shards:
        draws = jax.random.uniform(jax.random.fold_in(jax.random.fold_in(stream_key, 6), dim), (blocks,), jnp.float32, least / len(shards), top_value / len(shards))
        level = level * jnp.repeat(jnp.exp(draws), extent[dim] // blocks).reshape((-1,) + (1,) * (len(extent) - 1 - dim))
    return level


def normal_values(key, shape, scale, reach, pieces=(), kind=jnp.bfloat16):
    values = jax.random.normal(key, shape, jnp.float32) * scale
    if len(pieces) > 0:
        values = block_levels(key, shape, pieces, -0.22, 0.18) * values
    return jnp.clip(values, min=-reach, max=reach).astype(kind)


def setup_inputs(seed: int = 0) -> dict:
    arg_keys = jax.random.split(jax.random.key(seed), 9)
    queries = normal_values(arg_keys[0], (STEPS, SEGS, GROUPS, GROUP, HEAD), 1.0, 6.0, ((1, 8), (3, 4)))
    key_vectors = normal_values(arg_keys[1], (STEPS, SEGS, GROUPS, GROUP, HEAD), 1.0, 6.0, ((1, 8), (3, 4)))
    values = normal_values(arg_keys[2], (STEPS, SEGS, GROUPS, GROUP, HEAD), 1.0, 6.0, ((1, 8), (3, 4)))
    token_rates = draw_token_rates(jax.random.fold_in(arg_keys[8], 71), 0)
    fast_weights = normal_values(arg_keys[4], (SEGS, 3, HEAD, HEAD), HEAD ** -0.5, 0.375, ((0, 8), (3, 4)), jnp.float32)
    momenta = normal_values(arg_keys[5], (SEGS, 3, HEAD, HEAD), 0.5, 3.0, ((0, 8), (3, 4)), jnp.float32)
    fresh_weights = normal_values(arg_keys[6], (3, HEAD, HEAD), HEAD ** -0.5, 0.375, ((2, 4),), jnp.float32)
    fresh_momenta = normal_values(arg_keys[7], (3, HEAD, HEAD), 0.5, 3.0, ((2, 4),), jnp.float32)
    return {"queries": queries, "key_vectors": key_vectors, "values": values, "token_rates": token_rates, "fast_weights": fast_weights, "momenta": momenta, "fresh_weights": fresh_weights, "fresh_momenta": fresh_momenta}


momentum_decay = 0.9
learn_rate = 0.05
epsilon = 1e-06

def silu_parts(pre_gate):
    sigmoid_gate = jax.nn.sigmoid(pre_gate)
    return (pre_gate * sigmoid_gate, sigmoid_gate * (1.0 + pre_gate * (1.0 - sigmoid_gate)))

def local_grads(usable_weights, key_rows, value_rows, rate_rows):
    pre_gate = jnp.dot(key_rows, usable_weights[0], preferred_element_type=jnp.float32)
    pre_up = jnp.dot(key_rows, usable_weights[2], preferred_element_type=jnp.float32)
    active, slope_gate = silu_parts(pre_gate)
    hidden = (active * pre_up).astype(jnp.bfloat16)
    scaled = (rate_rows[:, None] * value_rows.astype(jnp.float32)).astype(jnp.bfloat16)
    back_hidden = -lax.dot_general(scaled, usable_weights[1], (((1,), (1,)), ((), ())), preferred_element_type=jnp.float32)
    back_gate = (back_hidden * pre_up * slope_gate).astype(jnp.bfloat16)
    back_up = (back_hidden * active).astype(jnp.bfloat16)
    contract_rows = (((0,), (0,)), ((), ()))
    grad_gate = lax.dot_general(key_rows, back_gate, contract_rows, preferred_element_type=jnp.float32)
    grad_down = -lax.dot_general(hidden, scaled, contract_rows, preferred_element_type=jnp.float32)
    grad_up = lax.dot_general(key_rows, back_up, contract_rows, preferred_element_type=jnp.float32)
    return (jnp.stack([grad_gate, grad_down, grad_up]), jnp.sum(rate_rows * rate_rows))

def update(weights, moment, gradients, rate_total):
    moment = momentum_decay * moment + gradients * lax.rsqrt(rate_total)
    stepped = weights - learn_rate * moment
    rescale = jnp.sqrt(lax.optimization_barrier(jnp.sum(weights * weights, axis=1, keepdims=True)) / (lax.optimization_barrier(jnp.sum(stepped * stepped, axis=1, keepdims=True)) + epsilon))
    return (stepped * rescale, moment)

def apply_fast(usable_weights, query_rows):
    pre_gate = jnp.dot(query_rows, usable_weights[0], preferred_element_type=jnp.float32)
    pre_up = jnp.dot(query_rows, usable_weights[2], preferred_element_type=jnp.float32)
    hidden = (jax.nn.silu(pre_gate) * pre_up).astype(jnp.bfloat16)
    return jnp.dot(hidden, usable_weights[1], preferred_element_type=jnp.float32).astype(jnp.bfloat16)

def run_segment(inputs):
    weights, moment, query_seg, key_seg, value_seg, rate_seg = inputs
    results = []
    for block_index in range(GROUPS):
        usable_weights = weights.astype(jnp.bfloat16)
        gradients, square = local_grads(usable_weights, key_seg[block_index], value_seg[block_index], rate_seg[block_index])
        weights, moment = update(weights, moment, gradients, square)
        results.append(apply_fast(weights.astype(jnp.bfloat16), query_seg[block_index]))
    return (weights, moment, jnp.stack(results))

def reference(queries, key_vectors, values, token_rates, fast_weights, momenta, fresh_weights, fresh_momenta):
    leave_weights, leave_moment, outputs_first = lax.map(run_segment, (fast_weights, momenta, queries[0], key_vectors[0], values[0], token_rates[0]))
    enter_weights = jnp.concatenate([fresh_weights[None], leave_weights[:-1]], axis=0)
    enter_moment = jnp.concatenate([fresh_momenta[None], leave_moment[:-1]], axis=0)
    final_weights, final_momenta, outputs_second = lax.map(run_segment, (enter_weights, enter_moment, queries[1], key_vectors[1], values[1], token_rates[1]))
    return (jnp.stack([outputs_first, outputs_second]), final_weights, final_momenta)
```

```python
import functools
import jax
import jax.numpy as jnp
from jax import lax
from jax.experimental import pallas as pl
from jax.experimental.pallas import tpu as pltpu
from jax.sharding import PartitionSpec as P

momentum_decay = 0.9
learn_rate = 0.05
epsilon = 1e-06
LANES = 128
UNROLL = 5
MESH = pl.DeviceIdType.MESH
f32 = jnp.float32
bf16 = jnp.bfloat16


def flip(index, mask):
    out, bit = index, 1
    while bit <= mask:
        if mask & bit:
            out = out + bit * (1 - 2 * lax.rem(index // bit, 2))
        bit *= 2
    return out


def sigmoid(x):
    return 0.5 + 0.5 * jnp.tanh(0.5 * x)


def mm(a, b):
    return jnp.dot(a, b, preferred_element_type=f32)


def mm_t(a, b):
    return lax.dot_general(a, b, (((1,), (1,)), ((), ())), preferred_element_type=f32)


def kernel(
    n, segs, steps, blocks, tile,
    k_hbm, v_hbm, q_hbm, rates, w_in, m_in, fw_in, fm_in,
    out_hbm, wstate, mstate,
    kbuf, vbuf, qbuf, obuf, kt, scaled, scaled_t, hid, bgate, bup,
    gsend, grecv, bank, msend, mrecv, sq,
    load_sem, store_sem, gs_sem, gr_sem, os_sem, or_sem, es_sem, er_sem, ms_sem, mr_sem,
    qs_sem, qr_sem,
):
    total = steps * blocks
    rows, head = kbuf.shape[1], kbuf.shape[2]
    width = head // n
    tiles = rows // tile
    order = (1, 0, 2)
    around = tuple(range(n - 1, 0, -1))
    seg = lax.axis_index("seg")
    tok = lax.axis_index("tok")
    first = seg == 0
    last = seg == segs - 1
    peers = [flip(tok, d) for d in range(n)]

    def part(p):
        return pl.ds(pl.multiple_of(p * width, width), width)

    mine = part(tok)

    def to_peer(d):
        return {"seg": seg, "tok": peers[d]}

    down = {"seg": lax.rem(seg + 1, segs), "tok": tok}
    up = {"seg": lax.rem(seg + segs - 1, segs), "tok": tok}

    def rcopy(src, dst, send, recv, device):
        return pltpu.make_async_remote_copy(
            src_ref=src, dst_ref=dst, send_sem=send, recv_sem=recv,
            device_id=device, device_id_type=MESH,
        )

    loads = [[
        pltpu.make_async_copy(src.at[b], dst.at[b], load_sem.at[j, b])
        for b in range(total)
    ] for j, (src, dst) in enumerate(((k_hbm, kbuf), (v_hbm, vbuf), (q_hbm, qbuf)))]

    barrier = pltpu.get_barrier_semaphore()
    for d in range(1, n):
        pl.semaphore_signal(barrier, inc=1, device_id=to_peer(d), device_id_type=MESH)

    @pl.when(jnp.logical_not(last))
    def _():
        pl.semaphore_signal(barrier, inc=1, device_id=down, device_id_type=MESH)

    @pl.when(jnp.logical_not(first))
    def _():
        pl.semaphore_signal(barrier, inc=1, device_id=up, device_id_type=MESH)

    for b in range(total):
        loads[0][b].start()
        loads[1][b].start()
    for b in range(total):
        loads[2][b].start()

    wstate[...] = w_in[...]
    mstate[...] = m_in[...]
    for m in range(3):
        bank[total, m, mine, :] = w_in[m].astype(bf16)
    for s in range(steps):
        drawn = rates[s]
        sums = jnp.sum(drawn * drawn, axis=1, keepdims=True)
        sq[tok, s] = jnp.broadcast_to(sums, (blocks, LANES))

    @pl.when(first)
    def _():
        for s in range(1, steps):
            for m in range(3):
                bank[total + s, m, mine, :] = fw_in[m].astype(bf16)

    neighbours = (seg + segs - 1) // segs + (2 * segs - 2 - seg) // segs
    pl.semaphore_wait(barrier, n - 1 + neighbours)

    def ent_copy(s, d, m):
        place = bank.at[total + s, m, mine, :]
        return rcopy(place, place, es_sem.at[s, d, m], er_sem.at[s, d, m], to_peer(d))

    def sq_copy(d):
        return rcopy(sq.at[tok], sq.at[tok], qs_sem.at[d], qr_sem.at[d], to_peer(d))

    for m in order:
        for d in around:
            ent_copy(0, d, m).start()
    for d in around:
        sq_copy(d).start()

    @pl.when(first)
    def _():
        for s in range(1, steps):
            for m in order:
                for d in around:
                    ent_copy(s, d, m).start()

    def g_copy(b, d, m):
        return rcopy(
            gsend.at[m, part(peers[d]), :], grecv.at[b, d, m],
            gs_sem.at[b, d, m], gr_sem.at[b, d, m], to_peer(d),
        )

    def own_copy(b, d, m):
        place = bank.at[b, m, mine, :]
        return rcopy(place, place, os_sem.at[b, d, m], or_sem.at[b, d, m], to_peer(d))

    def relay_copy(b, s, d, m):
        piece = part(peers[d])
        return rcopy(
            bank.at[b, m, piece, :], bank.at[total + s + 1, m, piece, :],
            es_sem.at[s + 1, d, m], er_sem.at[s + 1, d, m], down,
        )

    def m_copy(s):
        return rcopy(msend.at[s], mrecv.at[s], ms_sem.at[s], mr_sem.at[s], down)

    def prepare(b):
        pltpu.make_async_copy(k_hbm.at[b], kbuf.at[b], load_sem.at[0, b]).wait()
        pltpu.make_async_copy(v_hbm.at[b], vbuf.at[b], load_sem.at[1, b]).wait()
        kt[...] = kbuf[b].T
        s = b // blocks
        row = jnp.broadcast_to(rates[s, pl.ds(b - s * blocks, 1), :], (LANES, rows))
        column = jnp.concatenate([row.T] * (head // LANES), axis=1)
        product = (column * vbuf[b].astype(f32)).astype(bf16)
        scaled[...] = product
        scaled_t[...] = product.T

    def gradients(b, slot):
        w1, w2, w3 = bank[slot, 0], bank[slot, 1], bank[slot, 2]

        @pl.loop(0, tiles, unroll=UNROLL)
        def _(i):
            at = pl.ds(pl.multiple_of(i * tile, tile), tile)
            keys = kbuf[b, at, :]
            back = mm(scaled[at, :], w2)
            gate = mm_t(keys, w1)
            up_pre = mm_t(keys, w3)
            sig = sigmoid(gate)
            act = gate * sig
            slope = sig + act * (1.0 - sig)
            hid[at, :] = (act * up_pre).astype(bf16)
            bgate[at, :] = (back * up_pre * slope).astype(bf16)
            bup[at, :] = (back * act).astype(bf16)

        for m in order:
            if m == 1:
                grad = mm(scaled_t[...], hid[...])
            else:
                grad = mm(kt[...], (bgate if m == 0 else bup)[...]).T
            gsend[m] = grad.astype(bf16)
            for d in around:
                g_copy(b, d, m).start()

    def update(b, m, factor):
        grad = gsend[m, mine, :].astype(f32)
        for d in range(1, n):
            grad = grad + grecv[b, d, m].astype(f32)
        moment = momentum_decay * mstate[m] - grad * factor
        weight = wstate[m]
        stepped = weight - learn_rate * moment
        before = jnp.sum(weight * weight, axis=1, keepdims=True)
        after = jnp.sum(stepped * stepped, axis=1, keepdims=True)
        weight = stepped * jnp.sqrt(before / (after + epsilon))
        mstate[m] = moment
        wstate[m] = weight
        bank[b, m, mine, :] = weight.astype(bf16)

    def apply_fast(b):
        pltpu.make_async_copy(q_hbm.at[b], qbuf.at[b], load_sem.at[2, b]).wait()
        w1, w2, w3 = bank[b, 0], bank[b, 1], bank[b, 2]

        @pl.loop(0, tiles, unroll=UNROLL)
        def _(i):
            at = pl.ds(pl.multiple_of(i * tile, tile), tile)
            asked = qbuf[b, at, :]
            gate = mm_t(asked, w1)
            hidden = (gate * sigmoid(gate) * mm_t(asked, w3)).astype(bf16)
            obuf[b, at, :] = mm_t(hidden, w2).astype(bf16)

        pltpu.make_async_copy(obuf.at[b], out_hbm.at[b], store_sem.at[b]).start()

    prepare(0)
    for d in range(1, n):
        sq_copy(d).wait_recv()

    @pl.loop(0, total)
    def _(b):
        s = b // blocks
        g = b - s * blocks
        inner = (g + blocks - 1) // blocks
        entered = jnp.logical_and(jnp.logical_and(g == 0, s > 0), jnp.logical_not(first))

        @pl.when(g == 0)
        def _():
            for m in order:
                for d in around:
                    ent_copy(s, d, m).wait_recv()

        @pl.when(jnp.logical_and(jnp.logical_and(g == 0, s > 0), first))
        def _():
            wstate[...] = fw_in[...]
            mstate[...] = fm_in[...]

        @pl.when(entered)
        def _():
            for m in order:
                relay_copy(b - 1, s - 1, 0, m).wait_recv()
                wstate[m] = bank[total + s, m, mine, :].astype(f32)

        gradients(b, (total + s) * (1 - inner) + (b - 1) * inner)

        @pl.when(g > 0)
        def _():
            apply_fast(b - 1)

        @pl.when(entered)
        def _():
            m_copy(s - 1).wait_recv()
            mstate[...] = mrecv[s - 1].astype(f32)

        border = jnp.logical_and(g == blocks - 1, s < steps - 1)
        passing = jnp.logical_and(border, jnp.logical_not(last))
        square = sq[0, s, pl.ds(g, 1), :]
        for p in range(1, n):
            square = square + sq[p, s, pl.ds(g, 1), :]
        factor = lax.rsqrt(jnp.concatenate([square] * (head // LANES), axis=1))

        for m in order:
            for d in around:
                g_copy(b, d, m).wait_recv()
            update(b, m, factor)

            @pl.when(passing)
            def _():
                relay_copy(b, s, 0, m).start()

            for d in around:
                own_copy(b, d, m).start()

        @pl.when(passing)
        def _():
            msend[s] = mstate[...].astype(bf16)
            m_copy(s).start()

        for m in order:
            for d in around:
                g_copy(b, d, m).wait_send()

        @pl.when(b < total - 1)
        def _():
            prepare(b + 1)

        for m in order:
            for d in range(1, n):
                own_copy(b, d, m).wait_recv()

                @pl.when(passing)
                def _():
                    relay_copy(b, s, d, m).start()

        @pl.when(g == blocks - 1)
        def _():
            apply_fast(b)

        for m in order:
            for d in around:
                own_copy(b, d, m).wait_send()

        @pl.when(passing)
        def _():
            for m in order:
                for d in range(n):
                    relay_copy(b, s, d, m).wait_send()
            m_copy(s).wait_send()

    for d in around:
        sq_copy(d).wait_send()
        for m in order:
            ent_copy(0, d, m).wait_send()

    @pl.when(first)
    def _():
        for s in range(1, steps):
            for m in order:
                for d in around:
                    ent_copy(s, d, m).wait_send()

    for b in range(total):
        pltpu.make_async_copy(obuf.at[b], out_hbm.at[b], store_sem.at[b]).wait()


def quad_kernel(
    segs, steps, blocks, tile,
    k_hbm, v_hbm, q_hbm, rates, w_in, m_in, fw_in, fm_in,
    out_hbm, w_out, m_out,
    kbuf, vbuf, qbuf, obuf, kt, scaled, scaled_t, hid, bgu,
    bank13, bank2, gs13, gs2, got, mid, wst, mst,
    mx, mr, msend, mrecv, sq, sq_in,
    load_sem, store_sem, st_s, st_r, en_s, en_r, rl_s, rl_r, mm_s, mm_r, mx_s, mx_r, qs, qr,
):
    total = steps * blocks
    rows, head = kbuf.shape[1], kbuf.shape[2]
    unit = head // 8
    half = head // 2
    tiles = rows // tile
    seg = lax.axis_index("seg")
    tok = lax.axis_index("tok")
    inner = lax.rem(tok, 2)
    outer = tok // 2
    first = seg == 0
    last = seg == segs - 1
    own = (inner, outer)
    far = (1 - inner, 1 - outer)
    near_in = {"seg": seg, "tok": 2 * outer + (1 - inner)}
    near_out = {"seg": seg, "tok": 2 * (1 - outer) + inner}
    gather_to = (near_in, near_out)
    cross_to = (near_out, near_in)
    down = {"seg": lax.rem(seg + 1, segs), "tok": tok}
    up = {"seg": lax.rem(seg + segs - 1, segs), "tok": tok}

    def rcopy(src, dst, send, recv, device):
        return pltpu.make_async_remote_copy(
            src_ref=src, dst_ref=dst, send_sem=send, recv_sem=recv,
            device_id=device, device_id_type=MESH,
        )

    def place(slot, item, p, s):
        if item < 2:
            return bank13.at[slot, item, :, s, p]
        return bank2.at[slot, :, s, 0] if p == 0 else bank2.at[slot, s, :, 1]

    def load_place(slot, item, p, s):
        return place(slot, item, p, s)[...]

    def grad_place(b, item, p, s):
        if item < 2:
            return gs13.at[b, item, :, s, p]
        return gs2.at[b, :, s, 0] if p == 0 else gs2.at[b, s, :, 1]

    def swap(x):
        block = lax.broadcasted_iota(jnp.int32, x.shape, 1) // unit
        ahead = pltpu.roll(x, 2 * unit, 1)
        behind = pltpu.roll(x, head - 2 * unit, 1)
        return jnp.where(block == 5, ahead, jnp.where(block == 3, behind, x))

    barrier = pltpu.get_barrier_semaphore()
    for peer in (near_in, near_out):
        pl.semaphore_signal(barrier, inc=1, device_id=peer, device_id_type=MESH)

    @pl.when(jnp.logical_not(last))
    def _():
        pl.semaphore_signal(barrier, inc=1, device_id=down, device_id_type=MESH)

    @pl.when(jnp.logical_not(first))
    def _():
        pl.semaphore_signal(barrier, inc=1, device_id=up, device_id_type=MESH)

    loads = [[
        pltpu.make_async_copy(src.at[b], dst.at[b], load_sem.at[j, b])
        for b in range(total)
    ] for j, (src, dst) in enumerate(((k_hbm, kbuf), (v_hbm, vbuf), (q_hbm, qbuf)))]
    for b in range(total):
        loads[0][b].start()
        loads[1][b].start()
    for b in range(total):
        loads[2][b].start()

    def fill_bank(e, source):
        for k, m in enumerate((0, 2)):
            bank13[e, outer, k, inner, 0] = source[m, :unit, :].astype(bf16)
            bank13[e, inner, k, outer, 1] = source[m, unit:, :].astype(bf16)
        for h in range(2):
            bank2[e, outer, inner, h] = swap(source[1, h * unit:(h + 1) * unit, :]).astype(bf16)

    def fill_moments(s, source):
        for h in range(2):
            at = slice(h * unit, (h + 1) * unit)
            mx[s, h, 0] = source[0, at, :].astype(bf16)
            mx[s, h, 1] = source[2, at, :].astype(bf16)
            mx[s, h, 2] = swap(source[1, at, :]).astype(bf16)

    def fill_state(ref, source):
        for k, m in enumerate((0, 2)):
            ref[outer, 0, k] = source[m, :unit, :]
            ref[inner, 1, k] = source[m, unit:, :]
        ref[2, 0, outer] = swap(source[1, :unit, :])
        ref[2, 1, inner] = swap(source[1, unit:, :])

    fill_bank(total, w_in)
    for s in range(steps):
        drawn = rates[s]
        sums = jnp.sum(drawn * drawn, axis=1, keepdims=True)
        sq[0, s] = jnp.broadcast_to(sums, (blocks, LANES))

    def entry_copies(s):
        e = total + s
        out = []
        for d, peer in enumerate((near_in, near_out)):
            pieces = (
                bank13.at[e, outer, :, inner, 0],
                bank13.at[e, inner, :, outer, 1],
                bank2.at[e, outer, inner],
            )
            for j, piece in enumerate(pieces):
                out.append(rcopy(piece, piece, en_s.at[s, d, j], en_r.at[s, d, j], peer))
        return out

    def forward_copies(s):
        e = total + s
        pieces = (
            (bank13.at[e, 1 - outer, :, inner, 0], bank2.at[e, 1 - outer, inner, 0]),
            (bank13.at[e, 1 - inner, :, outer, 1], bank2.at[e, outer, 1 - inner, 1]),
        )
        return [[
            rcopy(piece, piece, en_s.at[s, d, 3 + j], en_r.at[s, d, 3 + j], peer)
            for j, piece in enumerate(pieces[d])
        ] for d, peer in enumerate((near_in, near_out))]

    def moment_copies(s):
        return [
            rcopy(mx.at[s, h], mr.at[s, h], mx_s.at[s, h], mx_r.at[s, h], cross_to[h])
            for h in range(2)
        ]

    def start_entry(s):
        for copy in entry_copies(s):
            copy.start()

    def pass_entry(s):
        sent, onward = entry_copies(s), forward_copies(s)
        sent[3].wait_recv()
        onward[0][0].start()
        sent[1].wait_recv()
        onward[1][0].start()
        sent[5].wait_recv()
        onward[0][1].start()
        sent[2].wait_recv()
        onward[1][1].start()
        sent[0].wait_recv()
        sent[4].wait_recv()

    def take_entry(s):
        for pair in forward_copies(s):
            for copy in pair:
                copy.wait_recv()

    def take_state(s, weights, moments):
        e = total + s
        fill_state(wst, weights)
        fill_state(mst, moments)
        wst[1 - outer, 0] = bank13[e, 1 - outer, :, inner, 0].astype(f32)
        wst[1 - inner, 1] = bank13[e, 1 - inner, :, outer, 1].astype(f32)
        wst[2, 0, 1 - outer] = bank2[e, 1 - outer, inner, 0].astype(f32)
        wst[2, 1, 1 - inner] = bank2[e, outer, 1 - inner, 1].astype(f32)
        for copy in moment_copies(s):
            copy.wait_recv()
        mst[1 - outer, 0] = mr[s, 0, :2].astype(f32)
        mst[1 - inner, 1] = mr[s, 1, :2].astype(f32)
        mst[2, 0, 1 - outer] = mr[s, 0, 2].astype(f32)
        mst[2, 1, 1 - inner] = mr[s, 1, 2].astype(f32)

    def square_copy(j):
        return rcopy(sq.at[j], sq_in.at[j], qs.at[j], qr.at[j], (near_in, near_out)[j])

    neighbours = (seg + segs - 1) // segs + (2 * segs - 2 - seg) // segs
    pl.semaphore_wait(barrier, 2 + neighbours)
    start_entry(0)
    square_copy(0).start()

    fill_moments(0, m_in)
    for copy in moment_copies(0):
        copy.start()

    @pl.when(first)
    def _():
        for s in range(1, steps):
            fill_bank(total + s, fw_in)
            fill_moments(s, fm_in)

    def prepare_keys(b):
        pltpu.make_async_copy(k_hbm.at[b], kbuf.at[b], load_sem.at[0, b]).wait()
        kt[...] = kbuf[b].T

    def prepare_values(b):
        pltpu.make_async_copy(v_hbm.at[b], vbuf.at[b], load_sem.at[1, b]).wait()
        s = b // blocks
        row = jnp.broadcast_to(rates[s, pl.ds(b - s * blocks, 1), :], (LANES, rows))
        column = jnp.concatenate([row.T] * (head // LANES), axis=1)
        product = (column * vbuf[b].astype(f32)).astype(bf16)
        scaled[...] = product
        scaled_t[...] = product.T

    def stage_copy(b, stage, item, p):
        if stage == 0:
            src, dst, peer = grad_place(b, item, p, far[p]), got.at[b, 0, item, p], gather_to[p]
        elif stage == 1:
            src, dst, peer = mid.at[b, item, p], got.at[b, 1, item, p], cross_to[p]
        else:
            src = place(b, item, p, own[p])
            dst, peer = src, gather_to[p]
        return rcopy(src, dst, st_s.at[b, stage, item, p], st_r.at[b, stage, item, p], peer)

    def relay_copy(b, s, item, j):
        p = j % 2
        piece = own[p] if j < 2 else far[p]
        return rcopy(
            place(b, item, p, piece), place(total + s + 1, item, p, piece),
            rl_s.at[s, item, j], rl_r.at[s, item, j], down,
        )

    def m_copy(s):
        return rcopy(msend.at[s], mrecv.at[s], mm_s.at[s], mm_r.at[s], down)

    def flow(b, slot, c):
        w13 = bank13[slot, c].reshape(head, head)
        w2 = bank2[slot].reshape(head, head)[:, c * half:(c + 1) * half]

        @pl.loop(0, tiles, unroll=UNROLL)
        def _(i):
            at = pl.ds(pl.multiple_of(i * tile, tile), tile)
            both = mm_t(kbuf[b, at, :], w13)
            back = mm(scaled[at, :], w2)
            gate, up_pre = both[:, :half], both[:, half:]
            sig = sigmoid(gate)
            act = gate * sig
            slope = sig + act * (1.0 - sig)
            hid[at, c * half:(c + 1) * half] = (act * up_pre).astype(bf16)
            bgu[c, at, :half] = (back * up_pre * slope).astype(bf16)
            bgu[c, at, half:] = (back * act).astype(bf16)

    def send_grads(b, item):
        if item < 2:
            grad = mm(kt[...], bgu[item]).T.astype(bf16)
            gs13[b, item] = grad.reshape(gs13.shape[2:])
        else:
            gs2[b] = mm(scaled_t[...], hid[...]).astype(bf16).reshape(gs2.shape[1:])
        for p in range(2):
            stage_copy(b, 0, item, p).start()

    def pair_sum(b, item):
        for p in range(2):
            stage_copy(b, 0, item, p).wait_recv()
            mine = grad_place(b, item, p, own[p])[...].astype(f32)
            mid[b, item, p] = (mine + got[b, 0, item, p].astype(f32)).astype(bf16)
            stage_copy(b, 1, item, p).start()

    def update(b, item, factor):
        for p in range(2):
            stage_copy(b, 1, item, p).wait_recv()
            grad = mid[b, item, p].astype(f32) + got[b, 1, item, p].astype(f32)
            moment = momentum_decay * mst[item, p] - grad * factor
            weight = wst[item, p]
            stepped = weight - learn_rate * moment
            before = jnp.sum(weight * weight, axis=2, keepdims=True)
            after = jnp.sum(stepped * stepped, axis=2, keepdims=True)
            weight = stepped * jnp.sqrt(before / (after + epsilon))
            mst[item, p] = moment
            wst[item, p] = weight
            place(b, item, p, own[p])[...] = weight.astype(bf16)
            stage_copy(b, 2, item, p).start()

    def apply_fast(b, start, stop):
        if start == 0:
            pltpu.make_async_copy(q_hbm.at[b], qbuf.at[b], load_sem.at[2, b]).wait()
        wa = bank13[b, 0].reshape(head, head)
        wb = bank13[b, 1].reshape(head, head)
        w2 = bank2[b].reshape(head, head)

        @pl.loop(start, stop, unroll=min(UNROLL, stop - start))
        def _(i):
            at = pl.ds(pl.multiple_of(i * tile, tile), tile)
            asked = qbuf[b, at, :]
            parts = []
            for w13 in (wa, wb):
                both = mm_t(asked, w13)
                gate = both[:, :half]
                parts.append((gate * sigmoid(gate) * both[:, half:]).astype(bf16))
            obuf[b, at, :] = mm_t(jnp.concatenate(parts, axis=1), w2).astype(bf16)

        if stop == tiles:
            pltpu.make_async_copy(obuf.at[b], out_hbm.at[b], store_sem.at[b]).start()

    prepare_keys(0)
    prepare_values(0)
    pass_entry(0)
    square_copy(0).wait_recv()
    sq[1] = sq[0] + sq_in[0]
    square_copy(1).start()

    @pl.when(first)
    def _():
        for s in range(1, steps):
            start_entry(s)
            for copy in moment_copies(s):
                copy.start()

    take_entry(0)
    cut = (tiles + 1) // 2

    @pl.loop(0, total)
    def _(b):
        s = b // blocks
        g = b - s * blocks
        inside = (g + blocks - 1) // blocks
        slot = (total + s) * (1 - inside) + (b - 1) * inside
        entered = jnp.logical_and(jnp.logical_and(g == 0, s > 0), jnp.logical_not(first))
        renewed = jnp.logical_and(jnp.logical_and(g == 0, s > 0), first)
        border = jnp.logical_and(g == blocks - 1, s < steps - 1)
        passing = jnp.logical_and(border, jnp.logical_not(last))

        @pl.when(renewed)
        def _():
            take_entry(s)

        @pl.when(entered)
        def _():
            for item in (0, 2):
                for j in range(4):
                    relay_copy(b - 1, s - 1, item, j).wait_recv()

        flow(b, slot, 0)
        send_grads(b, 0)

        @pl.when(g > 0)
        def _():
            for p in range(2):
                stage_copy(b - 1, 2, 1, p).wait_recv()

        @pl.when(entered)
        def _():
            for j in range(4):
                relay_copy(b - 1, s - 1, 1, j).wait_recv()

        flow(b, slot, 1)
        send_grads(b, 2)
        send_grads(b, 1)

        @pl.when(jnp.logical_and(g == 0, s == 0))
        def _():
            square_copy(1).wait_recv()
            sq[2] = sq[1] + sq_in[1]
            take_state(0, w_in, m_in)

        @pl.when(renewed)
        def _():
            take_state(s, fw_in, fm_in)

        @pl.when(entered)
        def _():
            m_copy(s - 1).wait_recv()
            mst[...] = mrecv[s - 1].astype(f32)
            for item in range(3):
                for p in range(2):
                    wst[item, p] = load_place(total + s, item, p, own[p]).astype(f32)

        square = sq[2, s, pl.ds(g, 1), :]
        factor = lax.rsqrt(jnp.concatenate([square] * (head // LANES), axis=1))

        @pl.when(g > 0)
        def _():
            apply_fast(b - 1, 0, cut)

        pair_sum(b, 0)

        @pl.when(g > 0)
        def _():
            apply_fast(b - 1, cut, tiles)

        pair_sum(b, 2)
        pair_sum(b, 1)

        @pl.when(b < total - 1)
        def _():
            prepare_keys(b + 1)

        @pl.when(jnp.logical_and(first, jnp.logical_and(b == 0, steps > 1)))
        def _():
            for step in range(1, steps):
                pass_entry(step)

        update(b, 0, factor)

        @pl.when(passing)
        def _():
            for j in range(2):
                relay_copy(b, s, 0, j).start()

        @pl.when(b < total - 1)
        def _():
            prepare_values(b + 1)

        for item in (2, 1):
            update(b, item, factor)

            @pl.when(passing)
            def _():
                for j in range(2):
                    relay_copy(b, s, item, j).start()

        for item in (0, 2):
            for p in range(2):
                stage_copy(b, 2, item, p).wait_recv()

                @pl.when(passing)
                def _():
                    relay_copy(b, s, item, 2 + p).start()

        @pl.when(g == blocks - 1)
        def _():
            for p in range(2):
                stage_copy(b, 2, 1, p).wait_recv()

        @pl.when(passing)
        def _():
            for p in range(2):
                relay_copy(b, s, 1, 2 + p).start()
            msend[s] = mst[...].astype(bf16)
            m_copy(s).start()

        @pl.when(g == blocks - 1)
        def _():
            apply_fast(b, 0, tiles)

    for k, m in enumerate((0, 2)):
        for ref, state in ((w_out, wst), (m_out, mst)):
            ref[m, :unit, :] = state[outer, 0, k]
            ref[m, unit:, :] = state[inner, 1, k]
    for ref, state in ((w_out, wst), (m_out, mst)):
        ref[1, :unit, :] = swap(state[2, 0, outer])
        ref[1, unit:, :] = swap(state[2, 1, inner])

    def drain_entry(s):
        for copy in entry_copies(s):
            copy.wait_send()
        for pair in forward_copies(s):
            for copy in pair:
                copy.wait_send()
        for copy in moment_copies(s):
            copy.wait_send()

    drain_entry(0)

    @pl.when(first)
    def _():
        for s in range(1, steps):
            drain_entry(s)

    for j in range(2):
        square_copy(j).wait_send()

    @pl.when(jnp.logical_not(last))
    def _():
        for s in range(steps - 1):
            for item in range(3):
                for j in range(4):
                    relay_copy(s * blocks + blocks - 1, s, item, j).wait_send()
            m_copy(s).wait_send()

    @pl.loop(0, total)
    def _(b):
        for stage in range(3):
            for item in range(3):
                for p in range(2):
                    stage_copy(b, stage, item, p).wait_send()
        pltpu.make_async_copy(obuf.at[b], out_hbm.at[b], store_sem.at[b]).wait()


def quad_scratch(steps, blocks, rows, head):
    total = steps * blocks
    unit = head // 8
    flat = (total, rows, head)
    pair = (2, unit, head)
    dma = pltpu.SemaphoreType.DMA
    vmem = pltpu.VMEM
    return [vmem(flat, bf16)] * 4 + [
        vmem((head, rows), bf16),
        vmem((rows, head), bf16),
        vmem((head, rows), bf16),
        vmem((rows, head), bf16),
        vmem((2, rows, head), bf16),
        vmem((total + steps, 2, 2, 2, 2, unit, head), bf16),
        vmem((total + steps, 2, 2, 2, unit, head), bf16),
        vmem((total, 2, 2, 2, 2, unit, head), bf16),
        vmem((total, 2, 2, 2, unit, head), bf16),
        vmem((total, 2, 3, 2) + pair, bf16),
        vmem((total, 3, 2) + pair, bf16),
        vmem((3, 2) + pair, f32),
        vmem((3, 2) + pair, f32),
        vmem((steps, 2, 3, unit, head), bf16),
        vmem((steps, 2, 3, unit, head), bf16),
        vmem((steps, 3, 2) + pair, bf16),
        vmem((steps, 3, 2) + pair, bf16),
        vmem((3, steps, blocks, LANES), f32),
        vmem((2, steps, blocks, LANES), f32),
        dma((3, total)),
        dma((total,)),
        dma((total, 3, 3, 2)),
        dma((total, 3, 3, 2)),
        dma((steps, 2, 5)),
        dma((steps, 2, 5)),
        dma((steps, 3, 4)),
        dma((steps, 3, 4)),
        dma((steps,)),
        dma((steps,)),
        dma((steps, 2)),
        dma((steps, 2)),
        dma((2,)),
        dma((2,)),
    ]


def body(n, segs, queries, keys, values, rates, weights, momenta, fresh_w, fresh_m):
    steps, _, blocks, rows, head = queries.shape
    total = steps * blocks
    width = head // n
    tile = 256 if rows % 256 == 0 else rows
    flat = (total, rows, head)
    piece = (3, width, head)
    hbm = pl.BlockSpec(memory_space=pl.ANY)
    vmem = pl.BlockSpec(memory_space=pltpu.VMEM)
    dma = pltpu.SemaphoreType.DMA
    big = (rows, head)
    turned = (head, rows)
    if n == 4 and head % 256 == 0:
        run = functools.partial(quad_kernel, segs, steps, blocks, tile)
        scratch = quad_scratch(steps, blocks, rows, head)
    else:
        run = functools.partial(kernel, n, segs, steps, blocks, tile)
        scratch = [pltpu.VMEM(flat, bf16)] * 4 + [
            pltpu.VMEM(turned, bf16),
            pltpu.VMEM(big, bf16),
            pltpu.VMEM(turned, bf16),
            pltpu.VMEM(big, bf16),
            pltpu.VMEM(big, bf16),
            pltpu.VMEM(big, bf16),
            pltpu.VMEM((3, head, head), bf16),
            pltpu.VMEM((total, n) + piece, bf16),
            pltpu.VMEM((total + steps, 3, head, head), bf16),
            pltpu.VMEM((steps,) + piece, bf16),
            pltpu.VMEM((steps,) + piece, bf16),
            pltpu.VMEM((n, steps, blocks, LANES), f32),
            dma((3, total)),
            dma((total,)),
            dma((total, n, 3)),
            dma((total, n, 3)),
            dma((total, n, 3)),
            dma((total, n, 3)),
            dma((steps, n, 3)),
            dma((steps, n, 3)),
            dma((steps,)),
            dma((steps,)),
            dma((n,)),
            dma((n,)),
        ]
    outs = pl.pallas_call(
        run,
        out_shape=(
            jax.ShapeDtypeStruct(flat, bf16),
            jax.ShapeDtypeStruct(piece, f32),
            jax.ShapeDtypeStruct(piece, f32),
        ),
        in_specs=[hbm, hbm, hbm, vmem, vmem, vmem, vmem, vmem],
        out_specs=(hbm, vmem, vmem),
        scratch_shapes=scratch,
        compiler_params=pltpu.CompilerParams(
            collective_id=0, has_side_effects=True, vmem_limit_bytes=60 * 1024 * 1024
        ),
    )(
        keys.reshape(flat), values.reshape(flat), queries.reshape(flat), rates[:, 0],
        jnp.swapaxes(weights[0], 1, 2), jnp.swapaxes(momenta[0], 1, 2),
        jnp.swapaxes(fresh_w, 1, 2), jnp.swapaxes(fresh_m, 1, 2),
    )
    return (
        outs[0].reshape(queries.shape),
        jnp.swapaxes(outs[1], 1, 2)[None],
        jnp.swapaxes(outs[2], 1, 2)[None],
    )


def solution(mesh):
    n, segs = mesh.shape["tok"], mesh.shape["seg"]
    return jax.shard_map(
        functools.partial(body, n, segs),
        mesh=mesh,
        in_specs=(
            P(None, "seg", None, "tok", None),
            P(None, "seg", None, "tok", None),
            P(None, "seg", None, "tok", None),
            P(None, "seg", None, "tok"),
            P("seg", None, None, "tok"),
            P("seg", None, None, "tok"),
            P(None, None, "tok"),
            P(None, None, "tok"),
        ),
        out_specs=(
            P(None, "seg", None, "tok", None),
            P("seg", None, None, "tok"),
            P("seg", None, None, "tok"),
        ),
        check_vma=False,
    )
```

```python
import functools
import jax
import jax.numpy as jnp
from jax import lax
from jax.experimental import pallas as pl
from jax.experimental.pallas import tpu as pltpu
from jax.sharding import PartitionSpec as P

momentum_decay = 0.9
learn_rate = 0.05
epsilon = 1e-06
LANES = 128
UNROLL = 5
MESH = pl.DeviceIdType.MESH
f32 = jnp.float32
bf16 = jnp.bfloat16


def flip(index, mask):
    out, bit = index, 1
    while bit <= mask:
        if mask & bit:
            out = out + bit * (1 - 2 * lax.rem(index // bit, 2))
        bit *= 2
    return out


def sigmoid(x):
    return 0.5 + 0.5 * jnp.tanh(0.5 * x)


def mm(a, b):
    return jnp.dot(a, b, preferred_element_type=f32)


def mm_t(a, b):
    return lax.dot_general(a, b, (((1,), (1,)), ((), ())), preferred_element_type=f32)


def kernel(
    n, segs, steps, blocks, tile,
    k_hbm, v_hbm, q_hbm, rates, w_in, m_in, fw_in, fm_in,
    out_hbm, wstate, mstate,
    kbuf, vbuf, qbuf, obuf, kt, scaled, scaled_t, hid, bgate, bup,
    gsend, grecv, bank, msend, mrecv, sq,
    load_sem, store_sem, gs_sem, gr_sem, os_sem, or_sem, es_sem, er_sem, ms_sem, mr_sem,
    qs_sem, qr_sem,
):
    total = steps * blocks
    rows, head = kbuf.shape[1], kbuf.shape[2]
    width = head // n
    tiles = rows // tile
    order = (1, 0, 2)
    around = tuple(range(n - 1, 0, -1))
    seg = lax.axis_index("seg")
    tok = lax.axis_index("tok")
    first = seg == 0
    last = seg == segs - 1
    peers = [flip(tok, d) for d in range(n)]

    def part(p):
        return pl.ds(pl.multiple_of(p * width, width), width)

    mine = part(tok)

    def to_peer(d):
        return {"seg": seg, "tok": peers[d]}

    down = {"seg": lax.rem(seg + 1, segs), "tok": tok}
    up = {"seg": lax.rem(seg + segs - 1, segs), "tok": tok}

    def rcopy(src, dst, send, recv, device):
        return pltpu.make_async_remote_copy(
            src_ref=src, dst_ref=dst, send_sem=send, recv_sem=recv,
            device_id=device, device_id_type=MESH,
        )

    loads = [[
        pltpu.make_async_copy(src.at[b], dst.at[b], load_sem.at[j, b])
        for b in range(total)
    ] for j, (src, dst) in enumerate(((k_hbm, kbuf), (v_hbm, vbuf), (q_hbm, qbuf)))]

    barrier = pltpu.get_barrier_semaphore()
    for d in range(1, n):
        pl.semaphore_signal(barrier, inc=1, device_id=to_peer(d), device_id_type=MESH)

    @pl.when(jnp.logical_not(last))
    def _():
        pl.semaphore_signal(barrier, inc=1, device_id=down, device_id_type=MESH)

    @pl.when(jnp.logical_not(first))
    def _():
        pl.semaphore_signal(barrier, inc=1, device_id=up, device_id_type=MESH)

    for b in range(total):
        loads[0][b].start()
        loads[1][b].start()
    for b in range(total):
        loads[2][b].start()

    wstate[...] = w_in[...]
    mstate[...] = m_in[...]
    for m in range(3):
        bank[total, m, mine, :] = w_in[m].astype(bf16)
    for s in range(steps):
        drawn = rates[s]
        sums = jnp.sum(drawn * drawn, axis=1, keepdims=True)
        sq[tok, s] = jnp.broadcast_to(sums, (blocks, LANES))

    @pl.when(first)
    def _():
        for s in range(1, steps):
            for m in range(3):
                bank[total + s, m, mine, :] = fw_in[m].astype(bf16)

    neighbours = (seg + segs - 1) // segs + (2 * segs - 2 - seg) // segs
    pl.semaphore_wait(barrier, n - 1 + neighbours)

    def ent_copy(s, d, m):
        place = bank.at[total + s, m, mine, :]
        return rcopy(place, place, es_sem.at[s, d, m], er_sem.at[s, d, m], to_peer(d))

    def sq_copy(d):
        return rcopy(sq.at[tok], sq.at[tok], qs_sem.at[d], qr_sem.at[d], to_peer(d))

    for m in order:
        for d in around:
            ent_copy(0, d, m).start()
    for d in around:
        sq_copy(d).start()

    @pl.when(first)
    def _():
        for s in range(1, steps):
            for m in order:
                for d in around:
                    ent_copy(s, d, m).start()

    def g_copy(b, d, m):
        return rcopy(
            gsend.at[m, part(peers[d]), :], grecv.at[b, d, m],
            gs_sem.at[b, d, m], gr_sem.at[b, d, m], to_peer(d),
        )

    def own_copy(b, d, m):
        place = bank.at[b, m, mine, :]
        return rcopy(place, place, os_sem.at[b, d, m], or_sem.at[b, d, m], to_peer(d))

    def relay_copy(b, s, d, m):
        piece = part(peers[d])
        return rcopy(
            bank.at[b, m, piece, :], bank.at[total + s + 1, m, piece, :],
            es_sem.at[s + 1, d, m], er_sem.at[s + 1, d, m], down,
        )

    def m_copy(s):
        return rcopy(msend.at[s], mrecv.at[s], ms_sem.at[s], mr_sem.at[s], down)

    def prepare(b):
        pltpu.make_async_copy(k_hbm.at[b], kbuf.at[b], load_sem.at[0, b]).wait()
        pltpu.make_async_copy(v_hbm.at[b], vbuf.at[b], load_sem.at[1, b]).wait()
        kt[...] = kbuf[b].T
        s = b // blocks
        row = jnp.broadcast_to(rates[s, pl.ds(b - s * blocks, 1), :], (LANES, rows))
        column = jnp.concatenate([row.T] * (head // LANES), axis=1)
        product = (column * vbuf[b].astype(f32)).astype(bf16)
        scaled[...] = product
        scaled_t[...] = product.T

    def gradients(b, slot):
        w1, w2, w3 = bank[slot, 0], bank[slot, 1], bank[slot, 2]

        @pl.loop(0, tiles, unroll=UNROLL)
        def _(i):
            at = pl.ds(pl.multiple_of(i * tile, tile), tile)
            keys = kbuf[b, at, :]
            back = mm(scaled[at, :], w2)
            gate = mm_t(keys, w1)
            up_pre = mm_t(keys, w3)
            sig = sigmoid(gate)
            act = gate * sig
            slope = sig + act * (1.0 - sig)
            hid[at, :] = (act * up_pre).astype(bf16)
            bgate[at, :] = (back * up_pre * slope).astype(bf16)
            bup[at, :] = (back * act).astype(bf16)

        for m in order:
            if m == 1:
                grad = mm(scaled_t[...], hid[...])
            else:
                grad = mm(kt[...], (bgate if m == 0 else bup)[...]).T
            gsend[m] = grad.astype(bf16)
            for d in around:
                g_copy(b, d, m).start()

    def update(b, m, factor):
        grad = gsend[m, mine, :].astype(f32)
        for d in range(1, n):
            grad = grad + grecv[b, d, m].astype(f32)
        moment = momentum_decay * mstate[m] - grad * factor
        weight = wstate[m]
        stepped = weight - learn_rate * moment
        before = jnp.sum(weight * weight, axis=1, keepdims=True)
        after = jnp.sum(stepped * stepped, axis=1, keepdims=True)
        weight = stepped * jnp.sqrt(before / (after + epsilon))
        mstate[m] = moment
        wstate[m] = weight
        bank[b, m, mine, :] = weight.astype(bf16)

    def apply_fast(b):
        pltpu.make_async_copy(q_hbm.at[b], qbuf.at[b], load_sem.at[2, b]).wait()
        w1, w2, w3 = bank[b, 0], bank[b, 1], bank[b, 2]

        @pl.loop(0, tiles, unroll=UNROLL)
        def _(i):
            at = pl.ds(pl.multiple_of(i * tile, tile), tile)
            asked = qbuf[b, at, :]
            gate = mm_t(asked, w1)
            hidden = (gate * sigmoid(gate) * mm_t(asked, w3)).astype(bf16)
            obuf[b, at, :] = mm_t(hidden, w2).astype(bf16)

        pltpu.make_async_copy(obuf.at[b], out_hbm.at[b], store_sem.at[b]).start()

    prepare(0)
    for d in range(1, n):
        sq_copy(d).wait_recv()

    @pl.loop(0, total)
    def _(b):
        s = b // blocks
        g = b - s * blocks
        inner = (g + blocks - 1) // blocks
        entered = jnp.logical_and(jnp.logical_and(g == 0, s > 0), jnp.logical_not(first))

        @pl.when(g == 0)
        def _():
            for m in order:
                for d in around:
                    ent_copy(s, d, m).wait_recv()

        @pl.when(jnp.logical_and(jnp.logical_and(g == 0, s > 0), first))
        def _():
            wstate[...] = fw_in[...]
            mstate[...] = fm_in[...]

        @pl.when(entered)
        def _():
            for m in order:
                relay_copy(b - 1, s - 1, 0, m).wait_recv()
                wstate[m] = bank[total + s, m, mine, :].astype(f32)

        gradients(b, (total + s) * (1 - inner) + (b - 1) * inner)

        @pl.when(g > 0)
        def _():
            apply_fast(b - 1)

        @pl.when(entered)
        def _():
            m_copy(s - 1).wait_recv()
            mstate[...] = mrecv[s - 1].astype(f32)

        border = jnp.logical_and(g == blocks - 1, s < steps - 1)
        passing = jnp.logical_and(border, jnp.logical_not(last))
        square = sq[0, s, pl.ds(g, 1), :]
        for p in range(1, n):
            square = square + sq[p, s, pl.ds(g, 1), :]
        factor = lax.rsqrt(jnp.concatenate([square] * (head // LANES), axis=1))

        for m in order:
            for d in around:
                g_copy(b, d, m).wait_recv()
            update(b, m, factor)

            @pl.when(passing)
            def _():
                relay_copy(b, s, 0, m).start()

            for d in around:
                own_copy(b, d, m).start()

        @pl.when(passing)
        def _():
            msend[s] = mstate[...].astype(bf16)
            m_copy(s).start()

        for m in order:
            for d in around:
                g_copy(b, d, m).wait_send()

        @pl.when(b < total - 1)
        def _():
            prepare(b + 1)

        for m in order:
            for d in range(1, n):
                own_copy(b, d, m).wait_recv()

                @pl.when(passing)
                def _():
                    relay_copy(b, s, d, m).start()

        @pl.when(g == blocks - 1)
        def _():
            apply_fast(b)

        for m in order:
            for d in around:
                own_copy(b, d, m).wait_send()

        @pl.when(passing)
        def _():
            for m in order:
                for d in range(n):
                    relay_copy(b, s, d, m).wait_send()
            m_copy(s).wait_send()

    for d in around:
        sq_copy(d).wait_send()
        for m in order:
            ent_copy(0, d, m).wait_send()

    @pl.when(first)
    def _():
        for s in range(1, steps):
            for m in order:
                for d in around:
                    ent_copy(s, d, m).wait_send()

    for b in range(total):
        pltpu.make_async_copy(obuf.at[b], out_hbm.at[b], store_sem.at[b]).wait()


def quad_kernel(
    segs, steps, blocks, tile,
    k_hbm, v_hbm, q_hbm, rates_hbm, w_hbm, m_hbm, fw_hbm, fm_hbm,
    out_hbm, w_out, m_out,
    kbuf, vbuf, qbuf, obuf, kt, scaled, scaled_t, hid, bgu,
    bank, gs, got, mid, wst, mst,
    w_in, m_in, fw_in, fm_in, rates, mx, mr, msend, mrecv, sq,
    load_sem, store_sem, in_sem, st_s, st_r, en_s, en_r, rl_s, rl_r, mm_s, mm_r, mx_s, mx_r, qs, qr,
):
    total = steps * blocks
    n = 4
    rows, head = kbuf.shape[1], kbuf.shape[2]
    half = head // 2
    tiles = rows // tile
    seg = lax.axis_index("seg")
    tok = lax.axis_index("tok")
    inner = lax.rem(tok, 2)
    outer = tok // 2
    first = seg == 0
    last = seg == segs - 1
    peers = [flip(tok, d) for d in range(n)]

    def to_peer(d):
        return {"seg": seg, "tok": peers[d]}

    stage_to = ((to_peer(1), to_peer(2)), (to_peer(2), to_peer(1)))
    down = {"seg": lax.rem(seg + 1, segs), "tok": tok}
    up = {"seg": lax.rem(seg + segs - 1, segs), "tok": tok}

    def rcopy(src, dst, send, recv, device):
        return pltpu.make_async_remote_copy(
            src_ref=src, dst_ref=dst, send_sem=send, recv_sem=recv,
            device_id=device, device_id_type=MESH,
        )

    barrier = pltpu.get_barrier_semaphore()
    for d in range(1, n):
        pl.semaphore_signal(barrier, inc=1, device_id=to_peer(d), device_id_type=MESH)

    @pl.when(jnp.logical_not(last))
    def _():
        pl.semaphore_signal(barrier, inc=1, device_id=down, device_id_type=MESH)

    @pl.when(jnp.logical_not(first))
    def _():
        pl.semaphore_signal(barrier, inc=1, device_id=up, device_id_type=MESH)

    inputs = [
        pltpu.make_async_copy(src, dst, in_sem.at[j])
        for j, (src, dst) in enumerate((
            (w_hbm, w_in), (rates_hbm, rates), (m_hbm, m_in), (fw_hbm, fw_in), (fm_hbm, fm_in),
        ))
    ]
    for copy in inputs:
        copy.start()
    loads = [[
        pltpu.make_async_copy(src.at[b], dst.at[b], load_sem.at[j, b])
        for b in range(total)
    ] for j, (src, dst) in enumerate(((k_hbm, kbuf), (v_hbm, vbuf), (q_hbm, qbuf)))]
    for b in range(total):
        loads[0][b].start()
        loads[1][b].start()
    for b in range(total):
        loads[2][b].start()

    def fill_bank(e, source):
        bank[e, outer, 0, inner] = source[0].astype(bf16)
        bank[e, outer, 1, inner] = source[2].astype(bf16)
        bank[e, 2, outer, inner] = source[1].astype(bf16)

    def entry_copies(s):
        e = total + s
        pieces = (bank.at[e, outer, :, inner], bank.at[e, 2, outer, inner])
        return [
            rcopy(piece, piece, en_s.at[s, d, j], en_r.at[s, d, j], to_peer(d))
            for j, piece in enumerate(pieces) for d in (1, 2, 3)
        ]

    def moment_copies(s):
        return [
            rcopy(mx.at[s], mr.at[s, tok], mx_s.at[s, d], mx_r.at[s, d], to_peer(d))
            for d in (1, 2, 3)
        ]

    def square_copies():
        return [rcopy(sq.at[tok], sq.at[tok], qs.at[d], qr.at[d], to_peer(d)) for d in (1, 2, 3)]

    def start(copies):
        for copy in copies:
            copy.start()

    def arrive(copies):
        for copy in copies:
            copy.wait_recv()

    def take_state(s, weights, moments):
        e = total + s
        for item in range(3):
            wst[item] = bank[e, item].astype(f32)
        wst[outer, 0, inner] = weights[0]
        wst[outer, 1, inner] = weights[2]
        wst[2, outer, inner] = weights[1]
        arrive(moment_copies(s))
        for o in range(2):
            for i in range(2):
                @pl.when(tok != 2 * o + i)
                def _():
                    mst[o, 0, i] = mr[s, 2 * o + i, 0].astype(f32)
                    mst[o, 1, i] = mr[s, 2 * o + i, 2].astype(f32)
                    mst[2, o, i] = mr[s, 2 * o + i, 1].astype(f32)
        mst[outer, 0, inner] = moments[0]
        mst[outer, 1, inner] = moments[2]
        mst[2, outer, inner] = moments[1]

    inputs[0].wait()
    fill_bank(total, w_in)
    neighbours = (seg + segs - 1) // segs + (2 * segs - 2 - seg) // segs
    pl.semaphore_wait(barrier, n - 1 + neighbours)
    start(entry_copies(0))
    inputs[1].wait()
    for s in range(steps):
        drawn = rates[s]
        sums = jnp.sum(drawn * drawn, axis=1, keepdims=True)
        sq[tok, s] = jnp.broadcast_to(sums, (blocks, LANES))
    start(square_copies())
    inputs[2].wait()
    mx[0] = m_in[...].astype(bf16)
    start(moment_copies(0))
    inputs[3].wait()
    inputs[4].wait()

    def prepare_keys(b):
        pltpu.make_async_copy(k_hbm.at[b], kbuf.at[b], load_sem.at[0, b]).wait()
        kt[...] = kbuf[b].T

    def prepare_values(b):
        pltpu.make_async_copy(v_hbm.at[b], vbuf.at[b], load_sem.at[1, b]).wait()
        s = b // blocks
        row = jnp.broadcast_to(rates[s, pl.ds(b - s * blocks, 1), :], (LANES, rows))
        column = jnp.concatenate([row.T] * (head // LANES), axis=1)
        product = (column * vbuf[b].astype(f32)).astype(bf16)
        scaled[...] = product
        scaled_t[...] = product.T

    def stage_copy(b, stage, item, p):
        src = (gs, mid)[stage].at[b, item, p]
        return rcopy(
            src, got.at[b, stage, item, p],
            st_s.at[b, stage, item, p], st_r.at[b, stage, item, p], stage_to[stage][p],
        )

    def relay_copy(b, s, item):
        return rcopy(
            bank.at[b, item], bank.at[total + s + 1, item],
            rl_s.at[s, item], rl_r.at[s, item], down,
        )

    def m_copy(s, item):
        return rcopy(msend.at[s, item], mrecv.at[s, item], mm_s.at[s, item], mm_r.at[s, item], down)

    def matrix(slot, item):
        return bank[slot, item].reshape(head, head)

    def flow(b, slot, c):
        w13 = matrix(slot, c)
        w2 = matrix(slot, 2)[:, c * half:(c + 1) * half]

        @pl.loop(0, tiles, unroll=UNROLL)
        def _(i):
            at = pl.ds(pl.multiple_of(i * tile, tile), tile)
            both = mm_t(kbuf[b, at, :], w13)
            back = mm(scaled[at, :], w2)
            gate, up_pre = both[:, :half], both[:, half:]
            sig = sigmoid(gate)
            act = gate * sig
            slope = sig + act * (1.0 - sig)
            hid[at, c * half:(c + 1) * half] = (act * up_pre).astype(bf16)
            bgu[c, at, :half] = (back * up_pre * slope).astype(bf16)
            bgu[c, at, half:] = (back * act).astype(bf16)

    def send_grads(b, item):
        if item < 2:
            grad = mm(kt[...], bgu[item]).T
        else:
            grad = mm(scaled_t[...], hid[...])
        for p in range(2):
            gs[b, item, p] = grad[p * half:(p + 1) * half].astype(bf16).reshape(gs.shape[3:])
            stage_copy(b, 0, item, p).start()

    def pair_sum(b, item):
        for p in range(2):
            stage_copy(b, 0, item, p).wait_recv()
            mid[b, item, p] = (gs[b, item, p].astype(f32) + got[b, 0, item, p].astype(f32)).astype(bf16)
            stage_copy(b, 1, item, p).start()

    def update(b, item, factor):
        for p in range(2):
            stage_copy(b, 1, item, p).wait_recv()
            grad = mid[b, item, p].astype(f32) + got[b, 1, item, p].astype(f32)
            moment = momentum_decay * mst[item, p] - grad * factor
            weight = wst[item, p]
            stepped = weight - learn_rate * moment
            before = jnp.sum(weight * weight, axis=2, keepdims=True)
            after = jnp.sum(stepped * stepped, axis=2, keepdims=True)
            weight = stepped * jnp.sqrt(before / (after + epsilon))
            mst[item, p] = moment
            wst[item, p] = weight
            bank[b, item, p] = weight.astype(bf16)

    def apply_fast(b, begin, stop):
        if begin == 0:
            pltpu.make_async_copy(q_hbm.at[b], qbuf.at[b], load_sem.at[2, b]).wait()
        wa, wb, w2 = matrix(b, 0), matrix(b, 1), matrix(b, 2)

        @pl.loop(begin, stop, unroll=min(UNROLL, stop - begin))
        def _(i):
            at = pl.ds(pl.multiple_of(i * tile, tile), tile)
            asked = qbuf[b, at, :]
            parts = []
            for w13 in (wa, wb):
                both = mm_t(asked, w13)
                gate = both[:, :half]
                parts.append((gate * sigmoid(gate) * both[:, half:]).astype(bf16))
            obuf[b, at, :] = mm_t(jnp.concatenate(parts, axis=1), w2).astype(bf16)

        if stop == tiles:
            pltpu.make_async_copy(obuf.at[b], out_hbm.at[b], store_sem.at[b]).start()

    prepare_keys(0)
    prepare_values(0)
    arrive(entry_copies(0))

    @pl.when(first)
    def _():
        for s in range(1, steps):
            fill_bank(total + s, fw_in)
            mx[s] = fm_in[...].astype(bf16)
            start(entry_copies(s))
            start(moment_copies(s))

    cut = (tiles + 1) // 2

    @pl.loop(0, total)
    def _(b):
        s = b // blocks
        g = b - s * blocks
        inside = (g + blocks - 1) // blocks
        slot = (total + s) * (1 - inside) + (b - 1) * inside
        entered = jnp.logical_and(jnp.logical_and(g == 0, s > 0), jnp.logical_not(first))
        renewed = jnp.logical_and(jnp.logical_and(g == 0, s > 0), first)
        border = jnp.logical_and(g == blocks - 1, s < steps - 1)
        passing = jnp.logical_and(border, jnp.logical_not(last))

        @pl.when(renewed)
        def _():
            arrive(entry_copies(s))

        @pl.when(entered)
        def _():
            for item in (0, 2):
                relay_copy(b - 1, s - 1, item).wait_recv()

        flow(b, slot, 0)
        send_grads(b, 0)

        @pl.when(entered)
        def _():
            relay_copy(b - 1, s - 1, 1).wait_recv()

        flow(b, slot, 1)
        send_grads(b, 2)
        send_grads(b, 1)

        @pl.when(jnp.logical_and(g == 0, s == 0))
        def _():
            arrive(square_copies())
            take_state(0, w_in, m_in)

        @pl.when(renewed)
        def _():
            take_state(s, fw_in, fm_in)

        @pl.when(entered)
        def _():
            for item in range(3):
                wst[item] = bank[total + s, item].astype(f32)

        square = sq[0, s, pl.ds(g, 1), :]
        for p in range(1, n):
            square = square + sq[p, s, pl.ds(g, 1), :]
        factor = lax.rsqrt(jnp.concatenate([square] * (head // LANES), axis=1))

        @pl.when(g > 0)
        def _():
            apply_fast(b - 1, 0, cut)

        @pl.when(b < total - 1)
        def _():
            prepare_keys(b + 1)

        pair_sum(b, 0)

        @pl.when(g > 0)
        def _():
            apply_fast(b - 1, cut, tiles)

        pair_sum(b, 2)

        @pl.when(b < total - 1)
        def _():
            prepare_values(b + 1)

        pair_sum(b, 1)

        @pl.when(entered)
        def _():
            for item in range(3):
                m_copy(s - 1, item).wait_recv()
                mst[item] = mrecv[s - 1, item].astype(f32)

        for item in (0, 2, 1):
            update(b, item, factor)

            @pl.when(passing)
            def _():
                relay_copy(b, s, item).start()

        @pl.when(passing)
        def _():
            for item in (0, 2, 1):
                msend[s, item] = mst[item].astype(bf16)
                m_copy(s, item).start()

        @pl.when(g == blocks - 1)
        def _():
            apply_fast(b, 0, tiles)

    for ref, state in ((w_out, wst), (m_out, mst)):
        ref[0] = state[outer, 0, inner]
        ref[2] = state[outer, 1, inner]
        ref[1] = state[2, outer, inner]

    def drain_entry(s):
        for copy in entry_copies(s) + moment_copies(s):
            copy.wait_send()

    drain_entry(0)

    @pl.when(first)
    def _():
        for s in range(1, steps):
            drain_entry(s)

    for copy in square_copies():
        copy.wait_send()

    @pl.when(jnp.logical_not(last))
    def _():
        for s in range(steps - 1):
            for item in range(3):
                relay_copy(s * blocks + blocks - 1, s, item).wait_send()
                m_copy(s, item).wait_send()

    @pl.loop(0, total)
    def _(b):
        for stage in range(2):
            for item in range(3):
                for p in range(2):
                    stage_copy(b, stage, item, p).wait_send()
        pltpu.make_async_copy(obuf.at[b], out_hbm.at[b], store_sem.at[b]).wait()


def quad_scratch(steps, blocks, rows, head):
    total = steps * blocks
    quarter = head // 4
    flat = (total, rows, head)
    whole = (2, 2, quarter, head)
    piece = (3, quarter, head)
    dma = pltpu.SemaphoreType.DMA
    vmem = pltpu.VMEM
    return [vmem(flat, bf16)] * 4 + [
        vmem((head, rows), bf16),
        vmem((rows, head), bf16),
        vmem((head, rows), bf16),
        vmem((rows, head), bf16),
        vmem((2, rows, head), bf16),
        vmem((total + steps, 3) + whole, bf16),
        vmem((total, 3) + whole, bf16),
        vmem((total, 2, 3) + whole, bf16),
        vmem((total, 3) + whole, bf16),
        vmem((3,) + whole, f32),
        vmem((3,) + whole, f32),
        vmem(piece, f32),
        vmem(piece, f32),
        vmem(piece, f32),
        vmem(piece, f32),
        vmem((steps, blocks, rows), f32),
        vmem((steps,) + piece, bf16),
        vmem((steps, 4) + piece, bf16),
        vmem((steps, 3) + whole, bf16),
        vmem((steps, 3) + whole, bf16),
        vmem((4, steps, blocks, LANES), f32),
        dma((3, total)),
        dma((total,)),
        dma((5,)),
        dma((total, 2, 3, 2)),
        dma((total, 2, 3, 2)),
        dma((steps, 4, 2)),
        dma((steps, 4, 2)),
        dma((steps, 3)),
        dma((steps, 3)),
        dma((steps, 3)),
        dma((steps, 3)),
        dma((steps, 4)),
        dma((steps, 4)),
        dma((4,)),
        dma((4,)),
    ]


def body(n, segs, queries, keys, values, rates, weights, momenta, fresh_w, fresh_m):
    steps, _, blocks, rows, head = queries.shape
    total = steps * blocks
    width = head // n
    tile = 256 if rows % 256 == 0 else rows
    flat = (total, rows, head)
    piece = (3, width, head)
    hbm = pl.BlockSpec(memory_space=pl.ANY)
    vmem = pl.BlockSpec(memory_space=pltpu.VMEM)
    dma = pltpu.SemaphoreType.DMA
    big = (rows, head)
    turned = (head, rows)
    if n == 4 and head % 256 == 0:
        run = functools.partial(quad_kernel, segs, steps, blocks, tile)
        scratch = quad_scratch(steps, blocks, rows, head)
        in_specs = [hbm] * 8
    else:
        run = functools.partial(kernel, n, segs, steps, blocks, tile)
        scratch = [pltpu.VMEM(flat, bf16)] * 4 + [
            pltpu.VMEM(turned, bf16),
            pltpu.VMEM(big, bf16),
            pltpu.VMEM(turned, bf16),
            pltpu.VMEM(big, bf16),
            pltpu.VMEM(big, bf16),
            pltpu.VMEM(big, bf16),
            pltpu.VMEM((3, head, head), bf16),
            pltpu.VMEM((total, n) + piece, bf16),
            pltpu.VMEM((total + steps, 3, head, head), bf16),
            pltpu.VMEM((steps,) + piece, bf16),
            pltpu.VMEM((steps,) + piece, bf16),
            pltpu.VMEM((n, steps, blocks, LANES), f32),
            dma((3, total)),
            dma((total,)),
            dma((total, n, 3)),
            dma((total, n, 3)),
            dma((total, n, 3)),
            dma((total, n, 3)),
            dma((steps, n, 3)),
            dma((steps, n, 3)),
            dma((steps,)),
            dma((steps,)),
            dma((n,)),
            dma((n,)),
        ]
        in_specs = [hbm, hbm, hbm, vmem, vmem, vmem, vmem, vmem]
    outs = pl.pallas_call(
        run,
        out_shape=(
            jax.ShapeDtypeStruct(flat, bf16),
            jax.ShapeDtypeStruct(piece, f32),
            jax.ShapeDtypeStruct(piece, f32),
        ),
        in_specs=in_specs,
        out_specs=(hbm, vmem, vmem),
        scratch_shapes=scratch,
        compiler_params=pltpu.CompilerParams(
            collective_id=0, has_side_effects=True, vmem_limit_bytes=60 * 1024 * 1024
        ),
    )(
        keys.reshape(flat), values.reshape(flat), queries.reshape(flat), rates[:, 0],
        jnp.swapaxes(weights[0], 1, 2), jnp.swapaxes(momenta[0], 1, 2),
        jnp.swapaxes(fresh_w, 1, 2), jnp.swapaxes(fresh_m, 1, 2),
    )
    return (
        outs[0].reshape(queries.shape),
        jnp.swapaxes(outs[1], 1, 2)[None],
        jnp.swapaxes(outs[2], 1, 2)[None],
    )


def solution(mesh):
    n, segs = mesh.shape["tok"], mesh.shape["seg"]
    return jax.shard_map(
        functools.partial(body, n, segs),
        mesh=mesh,
        in_specs=(
            P(None, "seg", None, "tok", None),
            P(None, "seg", None, "tok", None),
            P(None, "seg", None, "tok", None),
            P(None, "seg", None, "tok"),
            P("seg", None, None, "tok"),
            P("seg", None, None, "tok"),
            P(None, None, "tok"),
            P(None, None, "tok"),
        ),
        out_specs=(
            P(None, "seg", None, "tok", None),
            P("seg", None, None, "tok"),
            P("seg", None, None, "tok"),
        ),
        check_vma=False,
    )
```

```python
import functools
import jax
import jax.numpy as jnp
from jax import lax
from jax.experimental import pallas as pl
from jax.experimental.pallas import tpu as pltpu
from jax.sharding import PartitionSpec as P

momentum_decay = 0.9
learn_rate = 0.05
epsilon = 1e-06
LANES = 128
UNROLL = 5
MESH = pl.DeviceIdType.MESH
f32 = jnp.float32
bf16 = jnp.bfloat16


def flip(index, mask):
    out, bit = index, 1
    while bit <= mask:
        if mask & bit:
            out = out + bit * (1 - 2 * lax.rem(index // bit, 2))
        bit *= 2
    return out


def sigmoid(x):
    return 0.5 + 0.5 * jnp.tanh(0.5 * x)


def mm(a, b):
    return jnp.dot(a, b, preferred_element_type=f32)


def mm_t(a, b):
    return lax.dot_general(a, b, (((1,), (1,)), ((), ())), preferred_element_type=f32)


def kernel(
    n, segs, steps, blocks, tile,
    k_hbm, v_hbm, q_hbm, rates, w_in, m_in, fw_in, fm_in,
    out_hbm, wstate, mstate,
    kbuf, vbuf, qbuf, obuf, kt, scaled, scaled_t, hid, bgate, bup,
    gsend, grecv, bank, msend, mrecv, sq,
    load_sem, store_sem, gs_sem, gr_sem, os_sem, or_sem, es_sem, er_sem, ms_sem, mr_sem,
    qs_sem, qr_sem,
):
    total = steps * blocks
    rows, head = kbuf.shape[1], kbuf.shape[2]
    width = head // n
    tiles = rows // tile
    order = (1, 0, 2)
    around = tuple(range(n - 1, 0, -1))
    seg = lax.axis_index("seg")
    tok = lax.axis_index("tok")
    first = seg == 0
    last = seg == segs - 1
    peers = [flip(tok, d) for d in range(n)]

    def part(p):
        return pl.ds(pl.multiple_of(p * width, width), width)

    mine = part(tok)

    def to_peer(d):
        return {"seg": seg, "tok": peers[d]}

    down = {"seg": lax.rem(seg + 1, segs), "tok": tok}
    up = {"seg": lax.rem(seg + segs - 1, segs), "tok": tok}

    def rcopy(src, dst, send, recv, device):
        return pltpu.make_async_remote_copy(
            src_ref=src, dst_ref=dst, send_sem=send, recv_sem=recv,
            device_id=device, device_id_type=MESH,
        )

    loads = [[
        pltpu.make_async_copy(src.at[b], dst.at[b], load_sem.at[j, b])
        for b in range(total)
    ] for j, (src, dst) in enumerate(((k_hbm, kbuf), (v_hbm, vbuf), (q_hbm, qbuf)))]

    barrier = pltpu.get_barrier_semaphore()
    for d in range(1, n):
        pl.semaphore_signal(barrier, inc=1, device_id=to_peer(d), device_id_type=MESH)

    @pl.when(jnp.logical_not(last))
    def _():
        pl.semaphore_signal(barrier, inc=1, device_id=down, device_id_type=MESH)

    @pl.when(jnp.logical_not(first))
    def _():
        pl.semaphore_signal(barrier, inc=1, device_id=up, device_id_type=MESH)

    for b in range(total):
        loads[0][b].start()
        loads[1][b].start()
    for b in range(total):
        loads[2][b].start()

    wstate[...] = w_in[...]
    mstate[...] = m_in[...]
    for m in range(3):
        bank[total, m, mine, :] = w_in[m].astype(bf16)
    for s in range(steps):
        drawn = rates[s]
        sums = jnp.sum(drawn * drawn, axis=1, keepdims=True)
        sq[tok, s] = jnp.broadcast_to(sums, (blocks, LANES))

    @pl.when(first)
    def _():
        for s in range(1, steps):
            for m in range(3):
                bank[total + s, m, mine, :] = fw_in[m].astype(bf16)

    neighbours = (seg + segs - 1) // segs + (2 * segs - 2 - seg) // segs
    pl.semaphore_wait(barrier, n - 1 + neighbours)

    def ent_copy(s, d, m):
        place = bank.at[total + s, m, mine, :]
        return rcopy(place, place, es_sem.at[s, d, m], er_sem.at[s, d, m], to_peer(d))

    def sq_copy(d):
        return rcopy(sq.at[tok], sq.at[tok], qs_sem.at[d], qr_sem.at[d], to_peer(d))

    for m in order:
        for d in around:
            ent_copy(0, d, m).start()
    for d in around:
        sq_copy(d).start()

    @pl.when(first)
    def _():
        for s in range(1, steps):
            for m in order:
                for d in around:
                    ent_copy(s, d, m).start()

    def g_copy(b, d, m):
        return rcopy(
            gsend.at[m, part(peers[d]), :], grecv.at[b, d, m],
            gs_sem.at[b, d, m], gr_sem.at[b, d, m], to_peer(d),
        )

    def own_copy(b, d, m):
        place = bank.at[b, m, mine, :]
        return rcopy(place, place, os_sem.at[b, d, m], or_sem.at[b, d, m], to_peer(d))

    def relay_copy(b, s, d, m):
        piece = part(peers[d])
        return rcopy(
            bank.at[b, m, piece, :], bank.at[total + s + 1, m, piece, :],
            es_sem.at[s + 1, d, m], er_sem.at[s + 1, d, m], down,
        )

    def m_copy(s):
        return rcopy(msend.at[s], mrecv.at[s], ms_sem.at[s], mr_sem.at[s], down)

    def prepare(b):
        pltpu.make_async_copy(k_hbm.at[b], kbuf.at[b], load_sem.at[0, b]).wait()
        pltpu.make_async_copy(v_hbm.at[b], vbuf.at[b], load_sem.at[1, b]).wait()
        kt[...] = kbuf[b].T
        s = b // blocks
        row = jnp.broadcast_to(rates[s, pl.ds(b - s * blocks, 1), :], (LANES, rows))
        column = jnp.concatenate([row.T] * (head // LANES), axis=1)
        product = (column * vbuf[b].astype(f32)).astype(bf16)
        scaled[...] = product
        scaled_t[...] = product.T

    def gradients(b, slot):
        w1, w2, w3 = bank[slot, 0], bank[slot, 1], bank[slot, 2]

        @pl.loop(0, tiles, unroll=UNROLL)
        def _(i):
            at = pl.ds(pl.multiple_of(i * tile, tile), tile)
            keys = kbuf[b, at, :]
            back = mm(scaled[at, :], w2)
            gate = mm_t(keys, w1)
            up_pre = mm_t(keys, w3)
            sig = sigmoid(gate)
            act = gate * sig
            slope = sig + act * (1.0 - sig)
            hid[at, :] = (act * up_pre).astype(bf16)
            bgate[at, :] = (back * up_pre * slope).astype(bf16)
            bup[at, :] = (back * act).astype(bf16)

        for m in order:
            if m == 1:
                grad = mm(scaled_t[...], hid[...])
            else:
                grad = mm(kt[...], (bgate if m == 0 else bup)[...]).T
            gsend[m] = grad.astype(bf16)
            for d in around:
                g_copy(b, d, m).start()

    def update(b, m, factor):
        grad = gsend[m, mine, :].astype(f32)
        for d in range(1, n):
            grad = grad + grecv[b, d, m].astype(f32)
        moment = momentum_decay * mstate[m] - grad * factor
        weight = wstate[m]
        stepped = weight - learn_rate * moment
        before = jnp.sum(weight * weight, axis=1, keepdims=True)
        after = jnp.sum(stepped * stepped, axis=1, keepdims=True)
        weight = stepped * jnp.sqrt(before / (after + epsilon))
        mstate[m] = moment
        wstate[m] = weight
        bank[b, m, mine, :] = weight.astype(bf16)

    def apply_fast(b):
        pltpu.make_async_copy(q_hbm.at[b], qbuf.at[b], load_sem.at[2, b]).wait()
        w1, w2, w3 = bank[b, 0], bank[b, 1], bank[b, 2]

        @pl.loop(0, tiles, unroll=UNROLL)
        def _(i):
            at = pl.ds(pl.multiple_of(i * tile, tile), tile)
            asked = qbuf[b, at, :]
            gate = mm_t(asked, w1)
            hidden = (gate * sigmoid(gate) * mm_t(asked, w3)).astype(bf16)
            obuf[b, at, :] = mm_t(hidden, w2).astype(bf16)

        pltpu.make_async_copy(obuf.at[b], out_hbm.at[b], store_sem.at[b]).start()

    prepare(0)
    for d in range(1, n):
        sq_copy(d).wait_recv()

    @pl.loop(0, total)
    def _(b):
        s = b // blocks
        g = b - s * blocks
        inner = (g + blocks - 1) // blocks
        entered = jnp.logical_and(jnp.logical_and(g == 0, s > 0), jnp.logical_not(first))

        @pl.when(g == 0)
        def _():
            for m in order:
                for d in around:
                    ent_copy(s, d, m).wait_recv()

        @pl.when(jnp.logical_and(jnp.logical_and(g == 0, s > 0), first))
        def _():
            wstate[...] = fw_in[...]
            mstate[...] = fm_in[...]

        @pl.when(entered)
        def _():
            for m in order:
                relay_copy(b - 1, s - 1, 0, m).wait_recv()
                wstate[m] = bank[total + s, m, mine, :].astype(f32)

        gradients(b, (total + s) * (1 - inner) + (b - 1) * inner)

        @pl.when(g > 0)
        def _():
            apply_fast(b - 1)

        @pl.when(entered)
        def _():
            m_copy(s - 1).wait_recv()
            mstate[...] = mrecv[s - 1].astype(f32)

        border = jnp.logical_and(g == blocks - 1, s < steps - 1)
        passing = jnp.logical_and(border, jnp.logical_not(last))
        square = sq[0, s, pl.ds(g, 1), :]
        for p in range(1, n):
            square = square + sq[p, s, pl.ds(g, 1), :]
        factor = lax.rsqrt(jnp.concatenate([square] * (head // LANES), axis=1))

        for m in order:
            for d in around:
                g_copy(b, d, m).wait_recv()
            update(b, m, factor)

            @pl.when(passing)
            def _():
                relay_copy(b, s, 0, m).start()

            for d in around:
                own_copy(b, d, m).start()

        @pl.when(passing)
        def _():
            msend[s] = mstate[...].astype(bf16)
            m_copy(s).start()

        for m in order:
            for d in around:
                g_copy(b, d, m).wait_send()

        @pl.when(b < total - 1)
        def _():
            prepare(b + 1)

        for m in order:
            for d in range(1, n):
                own_copy(b, d, m).wait_recv()

                @pl.when(passing)
                def _():
                    relay_copy(b, s, d, m).start()

        @pl.when(g == blocks - 1)
        def _():
            apply_fast(b)

        for m in order:
            for d in around:
                own_copy(b, d, m).wait_send()

        @pl.when(passing)
        def _():
            for m in order:
                for d in range(n):
                    relay_copy(b, s, d, m).wait_send()
            m_copy(s).wait_send()

    for d in around:
        sq_copy(d).wait_send()
        for m in order:
            ent_copy(0, d, m).wait_send()

    @pl.when(first)
    def _():
        for s in range(1, steps):
            for m in order:
                for d in around:
                    ent_copy(s, d, m).wait_send()

    for b in range(total):
        pltpu.make_async_copy(obuf.at[b], out_hbm.at[b], store_sem.at[b]).wait()


def quad_kernel(
    segs, steps, blocks, tile,
    k_hbm, v_hbm, q_hbm, rates_hbm, w_hbm, m_hbm, fw_hbm, fm_hbm,
    out_hbm, w_out, m_out,
    kbuf, vbuf, qbuf, obuf, kt, scaled, scaled_t, hid, bgu,
    bank, gs, got, mid, tot, wst, mst,
    w_in, m_in, fw_in, fm_in, rates, mx, mr, msend, mrecv, sq,
    load_sem, store_sem, in_sem, st_s, st_r, en_s, en_r, rl_s, rl_r, mm_s, mm_r, mx_s, mx_r, qs, qr,
):
    total = steps * blocks
    n = 4
    rows, head = kbuf.shape[1], kbuf.shape[2]
    half = head // 2
    tiles = rows // tile
    seg = lax.axis_index("seg")
    tok = lax.axis_index("tok")
    inner = lax.rem(tok, 2)
    outer = tok // 2
    first = seg == 0
    last = seg == segs - 1
    peers = [flip(tok, d) for d in range(n)]

    def to_peer(d):
        return {"seg": seg, "tok": peers[d]}

    gather_to = (to_peer(1), to_peer(2))
    cross_to = (to_peer(2), to_peer(1))
    own = (inner, outer)
    far = (1 - inner, 1 - outer)
    odd = lax.rem(seg, 2) == 1
    even = jnp.logical_not(odd)
    down = {"seg": lax.rem(seg + 1, segs), "tok": tok}
    up = {"seg": lax.rem(seg + segs - 1, segs), "tok": tok}

    def rcopy(src, dst, send, recv, device):
        return pltpu.make_async_remote_copy(
            src_ref=src, dst_ref=dst, send_sem=send, recv_sem=recv,
            device_id=device, device_id_type=MESH,
        )

    barrier = pltpu.get_barrier_semaphore()
    for d in range(1, n):
        pl.semaphore_signal(barrier, inc=1, device_id=to_peer(d), device_id_type=MESH)

    @pl.when(jnp.logical_not(last))
    def _():
        pl.semaphore_signal(barrier, inc=1, device_id=down, device_id_type=MESH)

    @pl.when(jnp.logical_not(first))
    def _():
        pl.semaphore_signal(barrier, inc=1, device_id=up, device_id_type=MESH)

    inputs = [
        pltpu.make_async_copy(src, dst, in_sem.at[j])
        for j, (src, dst) in enumerate((
            (w_hbm, w_in), (m_hbm, m_in), (rates_hbm, rates), (fw_hbm, fw_in), (fm_hbm, fm_in),
        ))
    ]
    loads = [[
        pltpu.make_async_copy(src.at[b], dst.at[b], load_sem.at[j, b])
        for b in range(total)
    ] for j, (src, dst) in enumerate(((k_hbm, kbuf), (v_hbm, vbuf), (q_hbm, qbuf)))]
    for copy in (*inputs[:3], loads[0][0], loads[1][0]):
        copy.start()

    def fill_bank(e, source):
        bank[e, outer, 0, inner] = source[0].astype(bf16)
        bank[e, outer, 1, inner] = source[2].astype(bf16)
        bank[e, 2, outer, inner] = source[1].astype(bf16)

    def entry_copies(s):
        e = total + s
        pieces = (bank.at[e, outer, :, inner], bank.at[e, 2, outer, inner])
        return [
            rcopy(piece, piece, en_s.at[s, d, j], en_r.at[s, d, j], to_peer(d))
            for j, piece in enumerate(pieces) for d in (1, 2, 3)
        ]

    def moment_copies(s):
        return [
            rcopy(mx.at[s], mr.at[s, tok], mx_s.at[s, d], mx_r.at[s, d], to_peer(d))
            for d in (1, 2, 3)
        ]

    def square_copies():
        return [rcopy(sq.at[tok], sq.at[tok], qs.at[d], qr.at[d], to_peer(d)) for d in (1, 2, 3)]

    def start(copies):
        for copy in copies:
            copy.start()

    def arrive(copies):
        for copy in copies:
            copy.wait_recv()

    def take_weights(s, weights):
        e = total + s
        for item in range(3):
            wst[item] = bank[e, item].astype(f32)
        wst[outer, 0, inner] = weights[0]
        wst[outer, 1, inner] = weights[2]
        wst[2, outer, inner] = weights[1]

    def take_moments(s, moments):
        arrive(moment_copies(s))
        for o in range(2):
            for i in range(2):
                @pl.when(tok != 2 * o + i)
                def _():
                    mst[o, 0, i] = mr[s, 2 * o + i, 0].astype(f32)
                    mst[o, 1, i] = mr[s, 2 * o + i, 2].astype(f32)
                    mst[2, o, i] = mr[s, 2 * o + i, 1].astype(f32)
        mst[outer, 0, inner] = moments[0]
        mst[outer, 1, inner] = moments[2]
        mst[2, outer, inner] = moments[1]

    inputs[0].wait()
    fill_bank(total, w_in)
    neighbours = (seg + segs - 1) // segs + (2 * segs - 2 - seg) // segs
    pl.semaphore_wait(barrier, n - 1 + neighbours)
    start(entry_copies(0))
    for b in range(1, total):
        loads[0][b].start()
        loads[1][b].start()
    for b in range(total):
        loads[2][b].start()
    for copy in inputs[3:]:
        copy.start()
    inputs[1].wait()
    mx[0] = m_in[...].astype(bf16)
    inputs[2].wait()
    for s in range(steps):
        drawn = rates[s]
        sums = jnp.sum(drawn * drawn, axis=1, keepdims=True)
        sq[tok, s] = jnp.broadcast_to(sums, (blocks, LANES))
    start(square_copies())

    def prepare_keys(b):
        pltpu.make_async_copy(k_hbm.at[b], kbuf.at[b], load_sem.at[0, b]).wait()
        kt[...] = kbuf[b].T

    def prepare_values(b):
        pltpu.make_async_copy(v_hbm.at[b], vbuf.at[b], load_sem.at[1, b]).wait()
        s = b // blocks
        row = jnp.broadcast_to(rates[s, pl.ds(b - s * blocks, 1), :], (LANES, rows))
        column = jnp.concatenate([row.T] * (head // LANES), axis=1)
        product = (column * vbuf[b].astype(f32)).astype(bf16)
        scaled[...] = product
        scaled_t[...] = product.T

    def pair_copy(b, stage, item, p):
        return rcopy(
            (gs, mid)[stage].at[b, item, p], got.at[b, stage, item, p],
            st_s.at[b, stage, item, p], st_r.at[b, stage, item, p], (gather_to, cross_to)[stage][p],
        )

    def trio_copy(b, stage, item, p):
        if stage == 0:
            src, dst, peer = gs.at[b, item, p, far[p]], got.at[b, 0, item, p, 0], gather_to[p]
        elif stage == 1:
            src, dst, peer = mid.at[b, item, p, 0], got.at[b, 1, item, p, 0], cross_to[p]
        else:
            src, peer = tot.at[b, item, p, own[p]], gather_to[p]
            dst = src
        return rcopy(src, dst, st_s.at[b, stage, item, p], st_r.at[b, stage, item, p], peer)

    def relay_copy(b, s, item):
        return rcopy(
            bank.at[b, item], bank.at[total + s + 1, item],
            rl_s.at[s, item], rl_r.at[s, item], down,
        )

    def m_copy(s, item):
        return rcopy(msend.at[s, item], mrecv.at[s, item], mm_s.at[s, item], mm_r.at[s, item], down)

    def matrix(slot, item):
        return bank[slot, item].reshape(head, head)

    def flow(b, slot, c):
        w13 = matrix(slot, c)
        w2 = matrix(slot, 2)[:, c * half:(c + 1) * half]

        @pl.loop(0, tiles, unroll=UNROLL)
        def _(i):
            at = pl.ds(pl.multiple_of(i * tile, tile), tile)
            both = mm_t(kbuf[b, at, :], w13)
            back = mm(scaled[at, :], w2)
            gate, up_pre = both[:, :half], both[:, half:]
            sig = sigmoid(gate)
            act = gate * sig
            slope = sig + act * (1.0 - sig)
            hid[at, c * half:(c + 1) * half] = (act * up_pre).astype(bf16)
            bgu[c, at, :half] = (back * up_pre * slope).astype(bf16)
            bgu[c, at, half:] = (back * act).astype(bf16)

    def send_grads(b, item):
        if item < 2:
            grad = mm(kt[...], bgu[item]).T
        else:
            grad = mm(scaled_t[...], hid[...])
        for p in range(2):
            gs[b, item, p] = grad[p * half:(p + 1) * half].astype(bf16).reshape(gs.shape[3:])

            @pl.when(even)
            def _():
                pair_copy(b, 0, item, p).start()

            @pl.when(odd)
            def _():
                trio_copy(b, 0, item, p).start()

    def pair_sum(b, item):
        for p in range(2):
            pair_copy(b, 0, item, p).wait_recv()
            mid[b, item, p] = (gs[b, item, p].astype(f32) + got[b, 0, item, p].astype(f32)).astype(bf16)
            pair_copy(b, 1, item, p).start()

    def trio_sum(b, item):
        for p in range(2):
            trio_copy(b, 0, item, p).wait_recv()
            mine = gs[b, item, p, own[p]].astype(f32)
            mid[b, item, p, 0] = (mine + got[b, 0, item, p, 0].astype(f32)).astype(bf16)
            trio_copy(b, 1, item, p).start()

    def trio_cross(b, item):
        for p in range(2):
            trio_copy(b, 1, item, p).wait_recv()
            both = mid[b, item, p, 0].astype(f32) + got[b, 1, item, p, 0].astype(f32)
            tot[b, item, p, own[p]] = both.astype(bf16)
            trio_copy(b, 2, item, p).start()

    def step_half(b, item, p, factor, grad):
        moment = momentum_decay * mst[item, p] - grad * factor
        weight = wst[item, p]
        stepped = weight - learn_rate * moment
        before = jnp.sum(weight * weight, axis=2, keepdims=True)
        after = jnp.sum(stepped * stepped, axis=2, keepdims=True)
        weight = stepped * jnp.sqrt(before / (after + epsilon))
        mst[item, p] = moment
        wst[item, p] = weight
        bank[b, item, p] = weight.astype(bf16)

    def update(b, item):
        s = b // blocks
        g = b - s * blocks
        square = sq[0, s, pl.ds(g, 1), :]
        for p in range(1, n):
            square = square + sq[p, s, pl.ds(g, 1), :]
        factor = lax.rsqrt(jnp.concatenate([square] * (head // LANES), axis=1))

        @pl.when(even)
        def _():
            for p in range(2):
                pair_copy(b, 1, item, p).wait_recv()
                grad = mid[b, item, p].astype(f32) + got[b, 1, item, p].astype(f32)
                step_half(b, item, p, factor, grad)

        @pl.when(odd)
        def _():
            for p in range(2):
                trio_copy(b, 2, item, p).wait_recv()
                step_half(b, item, p, factor, tot[b, item, p].astype(f32))

    def apply_fast(b, begin, stop):
        if begin == 0:
            pltpu.make_async_copy(q_hbm.at[b], qbuf.at[b], load_sem.at[2, b]).wait()
        wa, wb, w2 = matrix(b, 0), matrix(b, 1), matrix(b, 2)

        @pl.loop(begin, stop, unroll=min(UNROLL, stop - begin))
        def _(i):
            at = pl.ds(pl.multiple_of(i * tile, tile), tile)
            asked = qbuf[b, at, :]
            parts = []
            for w13 in (wa, wb):
                both = mm_t(asked, w13)
                gate = both[:, :half]
                parts.append((gate * sigmoid(gate) * both[:, half:]).astype(bf16))
            obuf[b, at, :] = mm_t(jnp.concatenate(parts, axis=1), w2).astype(bf16)

        if stop == tiles:
            pltpu.make_async_copy(obuf.at[b], out_hbm.at[b], store_sem.at[b]).start()

    prepare_keys(0)
    prepare_values(0)
    for copy in entry_copies(0):
        copy.wait_send()
    start(moment_copies(0))
    arrive(entry_copies(0))
    for copy in inputs[3:]:
        copy.wait()
    cut = (tiles + 1) // 2

    @pl.loop(0, total)
    def _(b):
        s = b // blocks
        g = b - s * blocks
        inside = (g + blocks - 1) // blocks
        slot = (total + s) * (1 - inside) + (b - 1) * inside
        entered = jnp.logical_and(jnp.logical_and(g == 0, s > 0), jnp.logical_not(first))
        renewed = jnp.logical_and(jnp.logical_and(g == 0, s > 0), first)
        border = jnp.logical_and(g == blocks - 1, s < steps - 1)
        passing = jnp.logical_and(border, jnp.logical_not(last))

        @pl.when(renewed)
        def _():
            arrive(entry_copies(s))

        @pl.when(entered)
        def _():
            for item in (0, 2):
                relay_copy(b - 1, s - 1, item).wait_recv()

        flow(b, slot, 0)
        send_grads(b, 0)

        @pl.when(g > 0)
        def _():
            update(b - 1, 1)

        @pl.when(entered)
        def _():
            relay_copy(b - 1, s - 1, 1).wait_recv()

        flow(b, slot, 1)
        send_grads(b, 2)
        send_grads(b, 1)

        @pl.when(b < total - 1)
        def _():
            prepare_keys(b + 1)

        @pl.when(odd)
        def _():
            trio_sum(b, 0)

        @pl.when(b > 0)
        def _():
            apply_fast(b - 1, 0, cut)

        @pl.when(even)
        def _():
            pair_sum(b, 0)

        @pl.when(odd)
        def _():
            trio_sum(b, 2)
            trio_cross(b, 0)

        @pl.when(b > 0)
        def _():
            apply_fast(b - 1, cut, tiles)

        @pl.when(even)
        def _():
            pair_sum(b, 2)

        @pl.when(odd)
        def _():
            trio_sum(b, 1)
            trio_cross(b, 2)

        @pl.when(b < total - 1)
        def _():
            prepare_values(b + 1)

        @pl.when(even)
        def _():
            pair_sum(b, 1)

        @pl.when(odd)
        def _():
            trio_cross(b, 1)

        for step in range(1, steps):
            @pl.when(jnp.logical_and(first, b == 0))
            def _():
                fill_bank(total + step, fw_in)
                start(entry_copies(step))

            @pl.when(jnp.logical_and(first, b == step * blocks - 1))
            def _():
                mx[step] = fm_in[...].astype(bf16)
                start(moment_copies(step))

        @pl.when(b == 0)
        def _():
            arrive(square_copies())
            take_weights(0, w_in)
            take_moments(0, m_in)

        @pl.when(renewed)
        def _():
            take_weights(s, fw_in)
            take_moments(s, fm_in)

        @pl.when(entered)
        def _():
            for item in range(3):
                wst[item] = bank[total + s, item].astype(f32)
            for item in range(3):
                m_copy(s - 1, item).wait_recv()
                mst[item] = mrecv[s - 1, item].astype(f32)

        def finish(item):
            update(b, item)

            @pl.when(passing)
            def _():
                relay_copy(b, s, item).start()

        finish(0)
        finish(2)

        @pl.when(g == blocks - 1)
        def _():
            finish(1)

        @pl.when(passing)
        def _():
            for item in (0, 2, 1):
                msend[s, item] = mst[item].astype(bf16)
                m_copy(s, item).start()

    apply_fast(total - 1, 0, tiles)

    for ref, state in ((w_out, wst), (m_out, mst)):
        ref[0] = state[outer, 0, inner]
        ref[2] = state[outer, 1, inner]
        ref[1] = state[2, outer, inner]

    def drain_entry(s):
        for copy in entry_copies(s) + moment_copies(s):
            copy.wait_send()

    for copy in moment_copies(0):
        copy.wait_send()

    @pl.when(first)
    def _():
        for s in range(1, steps):
            drain_entry(s)

    for copy in square_copies():
        copy.wait_send()

    @pl.when(jnp.logical_not(last))
    def _():
        for s in range(steps - 1):
            for item in range(3):
                relay_copy(s * blocks + blocks - 1, s, item).wait_send()
                m_copy(s, item).wait_send()

    @pl.loop(0, total)
    def _(b):
        @pl.when(even)
        def _():
            for stage in range(2):
                for item in range(3):
                    for p in range(2):
                        pair_copy(b, stage, item, p).wait_send()

        @pl.when(odd)
        def _():
            for stage in range(3):
                for item in range(3):
                    for p in range(2):
                        trio_copy(b, stage, item, p).wait_send()

        pltpu.make_async_copy(obuf.at[b], out_hbm.at[b], store_sem.at[b]).wait()


def quad_scratch(steps, blocks, rows, head):
    total = steps * blocks
    quarter = head // 4
    flat = (total, rows, head)
    whole = (2, 2, quarter, head)
    piece = (3, quarter, head)
    dma = pltpu.SemaphoreType.DMA
    vmem = pltpu.VMEM
    return [vmem(flat, bf16)] * 4 + [
        vmem((head, rows), bf16),
        vmem((rows, head), bf16),
        vmem((head, rows), bf16),
        vmem((rows, head), bf16),
        vmem((2, rows, head), bf16),
        vmem((total + steps, 3) + whole, bf16),
        vmem((total, 3) + whole, bf16),
        vmem((total, 2, 3) + whole, bf16),
        vmem((total, 3) + whole, bf16),
        vmem((total, 3) + whole, bf16),
        vmem((3,) + whole, f32),
        vmem((3,) + whole, f32),
        vmem(piece, f32),
        vmem(piece, f32),
        vmem(piece, f32),
        vmem(piece, f32),
        vmem((steps, blocks, rows), f32),
        vmem((steps,) + piece, bf16),
        vmem((steps, 4) + piece, bf16),
        vmem((steps, 3) + whole, bf16),
        vmem((steps, 3) + whole, bf16),
        vmem((4, steps, blocks, LANES), f32),
        dma((3, total)),
        dma((total,)),
        dma((5,)),
        dma((total, 3, 3, 2)),
        dma((total, 3, 3, 2)),
        dma((steps, 4, 2)),
        dma((steps, 4, 2)),
        dma((steps, 3)),
        dma((steps, 3)),
        dma((steps, 3)),
        dma((steps, 3)),
        dma((steps, 4)),
        dma((steps, 4)),
        dma((4,)),
        dma((4,)),
    ]


def body(n, segs, queries, keys, values, rates, weights, momenta, fresh_w, fresh_m):
    steps, _, blocks, rows, head = queries.shape
    total = steps * blocks
    width = head // n
    tile = 256 if rows % 256 == 0 else rows
    flat = (total, rows, head)
    piece = (3, width, head)
    hbm = pl.BlockSpec(memory_space=pl.ANY)
    vmem = pl.BlockSpec(memory_space=pltpu.VMEM)
    dma = pltpu.SemaphoreType.DMA
    big = (rows, head)
    turned = (head, rows)
    if n == 4 and head % 256 == 0:
        run = functools.partial(quad_kernel, segs, steps, blocks, tile)
        scratch = quad_scratch(steps, blocks, rows, head)
        in_specs = [hbm] * 8
    else:
        run = functools.partial(kernel, n, segs, steps, blocks, tile)
        scratch = [pltpu.VMEM(flat, bf16)] * 4 + [
            pltpu.VMEM(turned, bf16),
            pltpu.VMEM(big, bf16),
            pltpu.VMEM(turned, bf16),
            pltpu.VMEM(big, bf16),
            pltpu.VMEM(big, bf16),
            pltpu.VMEM(big, bf16),
            pltpu.VMEM((3, head, head), bf16),
            pltpu.VMEM((total, n) + piece, bf16),
            pltpu.VMEM((total + steps, 3, head, head), bf16),
            pltpu.VMEM((steps,) + piece, bf16),
            pltpu.VMEM((steps,) + piece, bf16),
            pltpu.VMEM((n, steps, blocks, LANES), f32),
            dma((3, total)),
            dma((total,)),
            dma((total, n, 3)),
            dma((total, n, 3)),
            dma((total, n, 3)),
            dma((total, n, 3)),
            dma((steps, n, 3)),
            dma((steps, n, 3)),
            dma((steps,)),
            dma((steps,)),
            dma((n,)),
            dma((n,)),
        ]
        in_specs = [hbm, hbm, hbm, vmem, vmem, vmem, vmem, vmem]
    outs = pl.pallas_call(
        run,
        out_shape=(
            jax.ShapeDtypeStruct(flat, bf16),
            jax.ShapeDtypeStruct(piece, f32),
            jax.ShapeDtypeStruct(piece, f32),
        ),
        in_specs=in_specs,
        out_specs=(hbm, vmem, vmem),
        scratch_shapes=scratch,
        compiler_params=pltpu.CompilerParams(
            collective_id=0, has_side_effects=True, vmem_limit_bytes=60 * 1024 * 1024
        ),
    )(
        keys.reshape(flat), values.reshape(flat), queries.reshape(flat), rates[:, 0],
        jnp.swapaxes(weights[0], 1, 2), jnp.swapaxes(momenta[0], 1, 2),
        jnp.swapaxes(fresh_w, 1, 2), jnp.swapaxes(fresh_m, 1, 2),
    )
    return (
        outs[0].reshape(queries.shape),
        jnp.swapaxes(outs[1], 1, 2)[None],
        jnp.swapaxes(outs[2], 1, 2)[None],
    )


def solution(mesh):
    n, segs = mesh.shape["tok"], mesh.shape["seg"]
    return jax.shard_map(
        functools.partial(body, n, segs),
        mesh=mesh,
        in_specs=(
            P(None, "seg", None, "tok", None),
            P(None, "seg", None, "tok", None),
            P(None, "seg", None, "tok", None),
            P(None, "seg", None, "tok"),
            P("seg", None, None, "tok"),
            P("seg", None, None, "tok"),
            P(None, None, "tok"),
            P(None, None, "tok"),
        ),
        out_specs=(
            P(None, "seg", None, "tok", None),
            P("seg", None, None, "tok"),
            P("seg", None, None, "tok"),
        ),
        check_vma=False,
    )
```

```python
import functools
import jax
import jax.numpy as jnp
from jax import lax
from jax.experimental import pallas as pl
from jax.experimental.pallas import tpu as pltpu
from jax.sharding import PartitionSpec as P

momentum_decay = 0.9
learn_rate = 0.05
epsilon = 1e-06
LANES = 128
UNROLL = 5
QUAD_VMEM = 40 * 1024 * 1024
MESH = pl.DeviceIdType.MESH
f32 = jnp.float32
bf16 = jnp.bfloat16


def flip(index, mask):
    out, bit = index, 1
    while bit <= mask:
        if mask & bit:
            out = out + bit * (1 - 2 * lax.rem(index // bit, 2))
        bit *= 2
    return out


def sigmoid(x):
    return 0.5 + 0.5 * jnp.tanh(0.5 * x)


def mm(a, b):
    return jnp.dot(a, b, preferred_element_type=f32)


def mm_t(a, b):
    return lax.dot_general(a, b, (((1,), (1,)), ((), ())), preferred_element_type=f32)


def kernel(
    n, segs, steps, blocks, tile,
    k_hbm, v_hbm, q_hbm, rates, w_in, m_in, fw_in, fm_in,
    out_hbm, wstate, mstate,
    kbuf, vbuf, qbuf, obuf, kt, scaled, scaled_t, hid, bgate, bup,
    gsend, grecv, bank, msend, mrecv, sq,
    load_sem, store_sem, gs_sem, gr_sem, os_sem, or_sem, es_sem, er_sem, ms_sem, mr_sem,
    qs_sem, qr_sem,
):
    total = steps * blocks
    rows, head = kbuf.shape[1], kbuf.shape[2]
    width = head // n
    tiles = rows // tile
    order = (1, 0, 2)
    around = tuple(range(n - 1, 0, -1))
    seg = lax.axis_index("seg")
    tok = lax.axis_index("tok")
    first = seg == 0
    last = seg == segs - 1
    peers = [flip(tok, d) for d in range(n)]

    def part(p):
        return pl.ds(pl.multiple_of(p * width, width), width)

    mine = part(tok)

    def to_peer(d):
        return {"seg": seg, "tok": peers[d]}

    down = {"seg": lax.rem(seg + 1, segs), "tok": tok}
    up = {"seg": lax.rem(seg + segs - 1, segs), "tok": tok}

    def rcopy(src, dst, send, recv, device):
        return pltpu.make_async_remote_copy(
            src_ref=src, dst_ref=dst, send_sem=send, recv_sem=recv,
            device_id=device, device_id_type=MESH,
        )

    loads = [[
        pltpu.make_async_copy(src.at[b], dst.at[b], load_sem.at[j, b])
        for b in range(total)
    ] for j, (src, dst) in enumerate(((k_hbm, kbuf), (v_hbm, vbuf), (q_hbm, qbuf)))]

    barrier = pltpu.get_barrier_semaphore()
    for d in range(1, n):
        pl.semaphore_signal(barrier, inc=1, device_id=to_peer(d), device_id_type=MESH)

    @pl.when(jnp.logical_not(last))
    def _():
        pl.semaphore_signal(barrier, inc=1, device_id=down, device_id_type=MESH)

    @pl.when(jnp.logical_not(first))
    def _():
        pl.semaphore_signal(barrier, inc=1, device_id=up, device_id_type=MESH)

    for b in range(total):
        loads[0][b].start()
        loads[1][b].start()
    for b in range(total):
        loads[2][b].start()

    wstate[...] = w_in[...]
    mstate[...] = m_in[...]
    for m in range(3):
        bank[total, m, mine, :] = w_in[m].astype(bf16)
    for s in range(steps):
        drawn = rates[s]
        sums = jnp.sum(drawn * drawn, axis=1, keepdims=True)
        sq[tok, s] = jnp.broadcast_to(sums, (blocks, LANES))

    @pl.when(first)
    def _():
        for s in range(1, steps):
            for m in range(3):
                bank[total + s, m, mine, :] = fw_in[m].astype(bf16)

    neighbours = (seg + segs - 1) // segs + (2 * segs - 2 - seg) // segs
    pl.semaphore_wait(barrier, n - 1 + neighbours)

    def ent_copy(s, d, m):
        place = bank.at[total + s, m, mine, :]
        return rcopy(place, place, es_sem.at[s, d, m], er_sem.at[s, d, m], to_peer(d))

    def sq_copy(d):
        return rcopy(sq.at[tok], sq.at[tok], qs_sem.at[d], qr_sem.at[d], to_peer(d))

    for m in order:
        for d in around:
            ent_copy(0, d, m).start()
    for d in around:
        sq_copy(d).start()

    @pl.when(first)
    def _():
        for s in range(1, steps):
            for m in order:
                for d in around:
                    ent_copy(s, d, m).start()

    def g_copy(b, d, m):
        return rcopy(
            gsend.at[m, part(peers[d]), :], grecv.at[b, d, m],
            gs_sem.at[b, d, m], gr_sem.at[b, d, m], to_peer(d),
        )

    def own_copy(b, d, m):
        place = bank.at[b, m, mine, :]
        return rcopy(place, place, os_sem.at[b, d, m], or_sem.at[b, d, m], to_peer(d))

    def relay_copy(b, s, d, m):
        piece = part(peers[d])
        return rcopy(
            bank.at[b, m, piece, :], bank.at[total + s + 1, m, piece, :],
            es_sem.at[s + 1, d, m], er_sem.at[s + 1, d, m], down,
        )

    def m_copy(s):
        return rcopy(msend.at[s], mrecv.at[s], ms_sem.at[s], mr_sem.at[s], down)

    def prepare(b):
        pltpu.make_async_copy(k_hbm.at[b], kbuf.at[b], load_sem.at[0, b]).wait()
        pltpu.make_async_copy(v_hbm.at[b], vbuf.at[b], load_sem.at[1, b]).wait()
        kt[...] = kbuf[b].T
        s = b // blocks
        row = jnp.broadcast_to(rates[s, pl.ds(b - s * blocks, 1), :], (LANES, rows))
        column = jnp.concatenate([row.T] * (head // LANES), axis=1)
        product = (column * vbuf[b].astype(f32)).astype(bf16)
        scaled[...] = product
        scaled_t[...] = product.T

    def gradients(b, slot):
        w1, w2, w3 = bank[slot, 0], bank[slot, 1], bank[slot, 2]

        @pl.loop(0, tiles, unroll=UNROLL)
        def _(i):
            at = pl.ds(pl.multiple_of(i * tile, tile), tile)
            keys = kbuf[b, at, :]
            back = mm(scaled[at, :], w2)
            gate = mm_t(keys, w1)
            up_pre = mm_t(keys, w3)
            sig = sigmoid(gate)
            act = gate * sig
            slope = sig + act * (1.0 - sig)
            hid[at, :] = (act * up_pre).astype(bf16)
            bgate[at, :] = (back * up_pre * slope).astype(bf16)
            bup[at, :] = (back * act).astype(bf16)

        for m in order:
            if m == 1:
                grad = mm(scaled_t[...], hid[...])
            else:
                grad = mm(kt[...], (bgate if m == 0 else bup)[...]).T
            gsend[m] = grad.astype(bf16)
            for d in around:
                g_copy(b, d, m).start()

    def update(b, m, factor):
        grad = gsend[m, mine, :].astype(f32)
        for d in range(1, n):
            grad = grad + grecv[b, d, m].astype(f32)
        moment = momentum_decay * mstate[m] - grad * factor
        weight = wstate[m]
        stepped = weight - learn_rate * moment
        before = jnp.sum(weight * weight, axis=1, keepdims=True)
        after = jnp.sum(stepped * stepped, axis=1, keepdims=True)
        weight = stepped * jnp.sqrt(before / (after + epsilon))
        mstate[m] = moment
        wstate[m] = weight
        bank[b, m, mine, :] = weight.astype(bf16)

    def apply_fast(b):
        pltpu.make_async_copy(q_hbm.at[b], qbuf.at[b], load_sem.at[2, b]).wait()
        w1, w2, w3 = bank[b, 0], bank[b, 1], bank[b, 2]

        @pl.loop(0, tiles, unroll=UNROLL)
        def _(i):
            at = pl.ds(pl.multiple_of(i * tile, tile), tile)
            asked = qbuf[b, at, :]
            gate = mm_t(asked, w1)
            hidden = (gate * sigmoid(gate) * mm_t(asked, w3)).astype(bf16)
            obuf[b, at, :] = mm_t(hidden, w2).astype(bf16)

        pltpu.make_async_copy(obuf.at[b], out_hbm.at[b], store_sem.at[b]).start()

    prepare(0)
    for d in range(1, n):
        sq_copy(d).wait_recv()

    @pl.loop(0, total)
    def _(b):
        s = b // blocks
        g = b - s * blocks
        inner = (g + blocks - 1) // blocks
        entered = jnp.logical_and(jnp.logical_and(g == 0, s > 0), jnp.logical_not(first))

        @pl.when(g == 0)
        def _():
            for m in order:
                for d in around:
                    ent_copy(s, d, m).wait_recv()

        @pl.when(jnp.logical_and(jnp.logical_and(g == 0, s > 0), first))
        def _():
            wstate[...] = fw_in[...]
            mstate[...] = fm_in[...]

        @pl.when(entered)
        def _():
            for m in order:
                relay_copy(b - 1, s - 1, 0, m).wait_recv()
                wstate[m] = bank[total + s, m, mine, :].astype(f32)

        gradients(b, (total + s) * (1 - inner) + (b - 1) * inner)

        @pl.when(g > 0)
        def _():
            apply_fast(b - 1)

        @pl.when(entered)
        def _():
            m_copy(s - 1).wait_recv()
            mstate[...] = mrecv[s - 1].astype(f32)

        border = jnp.logical_and(g == blocks - 1, s < steps - 1)
        passing = jnp.logical_and(border, jnp.logical_not(last))
        square = sq[0, s, pl.ds(g, 1), :]
        for p in range(1, n):
            square = square + sq[p, s, pl.ds(g, 1), :]
        factor = lax.rsqrt(jnp.concatenate([square] * (head // LANES), axis=1))

        for m in order:
            for d in around:
                g_copy(b, d, m).wait_recv()
            update(b, m, factor)

            @pl.when(passing)
            def _():
                relay_copy(b, s, 0, m).start()

            for d in around:
                own_copy(b, d, m).start()

        @pl.when(passing)
        def _():
            msend[s] = mstate[...].astype(bf16)
            m_copy(s).start()

        for m in order:
            for d in around:
                g_copy(b, d, m).wait_send()

        @pl.when(b < total - 1)
        def _():
            prepare(b + 1)

        for m in order:
            for d in range(1, n):
                own_copy(b, d, m).wait_recv()

                @pl.when(passing)
                def _():
                    relay_copy(b, s, d, m).start()

        @pl.when(g == blocks - 1)
        def _():
            apply_fast(b)

        for m in order:
            for d in around:
                own_copy(b, d, m).wait_send()

        @pl.when(passing)
        def _():
            for m in order:
                for d in range(n):
                    relay_copy(b, s, d, m).wait_send()
            m_copy(s).wait_send()

    for d in around:
        sq_copy(d).wait_send()
        for m in order:
            ent_copy(0, d, m).wait_send()

    @pl.when(first)
    def _():
        for s in range(1, steps):
            for m in order:
                for d in around:
                    ent_copy(s, d, m).wait_send()

    for b in range(total):
        pltpu.make_async_copy(obuf.at[b], out_hbm.at[b], store_sem.at[b]).wait()


def apply_tiles(begin, stop, tile, weights, asked_ref, out_ref):
    half = asked_ref.shape[-1] // 2

    @pl.loop(begin, stop, unroll=min(UNROLL, stop - begin))
    def _(i):
        at = pl.ds(pl.multiple_of(i * tile, tile), tile)
        asked = asked_ref[at, :]
        parts = []
        for w13 in weights[:2]:
            both = mm_t(asked, w13)
            gate = both[:, :half]
            parts.append((gate * sigmoid(gate) * both[:, half:]).astype(bf16))
        out_ref[at, :] = mm_t(jnp.concatenate(parts, axis=1), weights[2]).astype(bf16)


def quad_kernel(
    segs, steps, blocks, tile,
    k_hbm, v_hbm, q_hbm, rates_hbm, w_hbm, m_hbm, fw_hbm, fm_hbm,
    obuf, usable, asked_last, w_out, m_out,
    kbuf, vbuf, qbuf, kt, scaled, scaled_t, hid, bgu,
    bank, gs, got, mid, tot, wst, mst,
    w_in, m_in, fw_in, fm_in, rates, mx, mr, msend, mrecv, sq,
    load_sem, in_sem, st_s, st_r, en_s, en_r, rl_s, rl_r, mm_s, mm_r, mx_s, mx_r, qs, qr,
):
    total = steps * blocks
    n = 4
    rows, head = kbuf.shape[1], kbuf.shape[2]
    half = head // 2
    tiles = rows // tile
    seg = lax.axis_index("seg")
    tok = lax.axis_index("tok")
    inner = lax.rem(tok, 2)
    outer = tok // 2
    first = seg == 0
    last = seg == segs - 1
    peers = [flip(tok, d) for d in range(n)]

    def to_peer(d):
        return {"seg": seg, "tok": peers[d]}

    gather_to = (to_peer(1), to_peer(2))
    cross_to = (to_peer(2), to_peer(1))
    own = (inner, outer)
    far = (1 - inner, 1 - outer)
    odd = lax.rem(seg, 2) == 1
    even = jnp.logical_not(odd)
    down = {"seg": lax.rem(seg + 1, segs), "tok": tok}
    up = {"seg": lax.rem(seg + segs - 1, segs), "tok": tok}

    def rcopy(src, dst, send, recv, device):
        return pltpu.make_async_remote_copy(
            src_ref=src, dst_ref=dst, send_sem=send, recv_sem=recv,
            device_id=device, device_id_type=MESH,
        )

    barrier = pltpu.get_barrier_semaphore()
    for d in range(1, n):
        pl.semaphore_signal(barrier, inc=1, device_id=to_peer(d), device_id_type=MESH)

    @pl.when(jnp.logical_not(last))
    def _():
        pl.semaphore_signal(barrier, inc=1, device_id=down, device_id_type=MESH)

    @pl.when(jnp.logical_not(first))
    def _():
        pl.semaphore_signal(barrier, inc=1, device_id=up, device_id_type=MESH)

    inputs = [
        pltpu.make_async_copy(src, dst, in_sem.at[j])
        for j, (src, dst) in enumerate((
            (w_hbm, w_in), (m_hbm, m_in), (rates_hbm, rates), (fw_hbm, fw_in), (fm_hbm, fm_in),
        ))
    ]
    loads = [[
        pltpu.make_async_copy(src.at[b], dst.at[b], load_sem.at[j, b])
        for b in range(total - (j == 2))
    ] for j, (src, dst) in enumerate(((k_hbm, kbuf), (v_hbm, vbuf), (q_hbm, qbuf)))]
    late = pltpu.make_async_copy(q_hbm.at[total - 1], asked_last, load_sem.at[2, total - 1])
    for copy in (*inputs[:3], loads[0][0], loads[1][0]):
        copy.start()

    def fill_bank(e, source):
        bank[e, outer, 0, inner] = source[0].astype(bf16)
        bank[e, outer, 1, inner] = source[2].astype(bf16)
        bank[e, 2, outer, inner] = source[1].astype(bf16)

    def entry_copies(s):
        e = total + s
        pieces = (bank.at[e, outer, :, inner], bank.at[e, 2, outer, inner])
        return [
            rcopy(piece, piece, en_s.at[s, d, j], en_r.at[s, d, j], to_peer(d))
            for j, piece in enumerate(pieces) for d in (1, 2, 3)
        ]

    def moment_copies(s):
        return [
            rcopy(mx.at[s], mr.at[s, tok], mx_s.at[s, d], mx_r.at[s, d], to_peer(d))
            for d in (1, 2, 3)
        ]

    def square_copies():
        return [rcopy(sq.at[tok], sq.at[tok], qs.at[d], qr.at[d], to_peer(d)) for d in (1, 2, 3)]

    def start(copies):
        for copy in copies:
            copy.start()

    def arrive(copies):
        for copy in copies:
            copy.wait_recv()

    def take_weights(s, weights):
        e = total + s
        for item in range(3):
            wst[item] = bank[e, item].astype(f32)
        wst[outer, 0, inner] = weights[0]
        wst[outer, 1, inner] = weights[2]
        wst[2, outer, inner] = weights[1]

    def take_moments(s, moments):
        arrive(moment_copies(s))
        for o in range(2):
            for i in range(2):
                @pl.when(tok != 2 * o + i)
                def _():
                    mst[o, 0, i] = mr[s, 2 * o + i, 0].astype(f32)
                    mst[o, 1, i] = mr[s, 2 * o + i, 2].astype(f32)
                    mst[2, o, i] = mr[s, 2 * o + i, 1].astype(f32)
        mst[outer, 0, inner] = moments[0]
        mst[outer, 1, inner] = moments[2]
        mst[2, outer, inner] = moments[1]

    inputs[0].wait()
    fill_bank(total, w_in)
    neighbours = (seg + segs - 1) // segs + (2 * segs - 2 - seg) // segs
    pl.semaphore_wait(barrier, n - 1 + neighbours)
    start(entry_copies(0))
    for b in range(1, total):
        loads[0][b].start()
        loads[1][b].start()
    for copy in loads[2]:
        copy.start()
    late.start()
    for copy in inputs[3:]:
        copy.start()
    inputs[1].wait()
    mx[0] = m_in[...].astype(bf16)
    inputs[2].wait()
    for s in range(steps):
        drawn = rates[s]
        sums = jnp.sum(drawn * drawn, axis=1, keepdims=True)
        sq[tok, s] = jnp.broadcast_to(sums, (blocks, LANES))
    start(square_copies())

    def prepare_keys(b):
        pltpu.make_async_copy(k_hbm.at[b], kbuf.at[b], load_sem.at[0, b]).wait()
        kt[...] = kbuf[b].T

    def prepare_values(b):
        pltpu.make_async_copy(v_hbm.at[b], vbuf.at[b], load_sem.at[1, b]).wait()
        s = b // blocks
        row = jnp.broadcast_to(rates[s, pl.ds(b - s * blocks, 1), :], (LANES, rows))
        column = jnp.concatenate([row.T] * (head // LANES), axis=1)
        product = (column * vbuf[b].astype(f32)).astype(bf16)
        scaled[...] = product
        scaled_t[...] = product.T

    def pair_copy(b, stage, item, p):
        return rcopy(
            (gs, mid)[stage].at[b, item, p], got.at[b, stage, item, p],
            st_s.at[b, stage, item, p], st_r.at[b, stage, item, p], (gather_to, cross_to)[stage][p],
        )

    def trio_copy(b, stage, item, p):
        if stage == 0:
            src, dst, peer = gs.at[b, item, p, far[p]], got.at[b, 0, item, p, 0], gather_to[p]
        elif stage == 1:
            src, dst, peer = mid.at[b, item, p, 0], got.at[b, 1, item, p, 0], cross_to[p]
        else:
            src, peer = tot.at[b, item, p, own[p]], gather_to[p]
            dst = src
        return rcopy(src, dst, st_s.at[b, stage, item, p], st_r.at[b, stage, item, p], peer)

    def relay_copy(b, s, item):
        return rcopy(
            bank.at[b, item], bank.at[total + s + 1, item],
            rl_s.at[s, item], rl_r.at[s, item], down,
        )

    def m_copy(s, item):
        return rcopy(msend.at[s, item], mrecv.at[s, item], mm_s.at[s, item], mm_r.at[s, item], down)

    def matrix(slot, item):
        return bank[slot, item].reshape(head, head)

    def flow(b, slot, c):
        w13 = matrix(slot, c)
        w2 = matrix(slot, 2)[:, c * half:(c + 1) * half]

        @pl.loop(0, tiles, unroll=UNROLL)
        def _(i):
            at = pl.ds(pl.multiple_of(i * tile, tile), tile)
            both = mm_t(kbuf[b, at, :], w13)
            back = mm(scaled[at, :], w2)
            gate, up_pre = both[:, :half], both[:, half:]
            sig = sigmoid(gate)
            act = gate * sig
            slope = sig + act * (1.0 - sig)
            hid[at, c * half:(c + 1) * half] = (act * up_pre).astype(bf16)
            bgu[c, at, :half] = (back * up_pre * slope).astype(bf16)
            bgu[c, at, half:] = (back * act).astype(bf16)

    def send_grads(b, item):
        if item < 2:
            grad = mm(kt[...], bgu[item]).T
        else:
            grad = mm(scaled_t[...], hid[...])
        for p in range(2):
            gs[b, item, p] = grad[p * half:(p + 1) * half].astype(bf16).reshape(gs.shape[3:])

            @pl.when(even)
            def _():
                pair_copy(b, 0, item, p).start()

            @pl.when(odd)
            def _():
                trio_copy(b, 0, item, p).start()

    def pair_sum(b, item):
        for p in range(2):
            pair_copy(b, 0, item, p).wait_recv()
            mid[b, item, p] = (gs[b, item, p].astype(f32) + got[b, 0, item, p].astype(f32)).astype(bf16)
            pair_copy(b, 1, item, p).start()

    def trio_sum(b, item):
        for p in range(2):
            trio_copy(b, 0, item, p).wait_recv()
            mine = gs[b, item, p, own[p]].astype(f32)
            mid[b, item, p, 0] = (mine + got[b, 0, item, p, 0].astype(f32)).astype(bf16)
            trio_copy(b, 1, item, p).start()

    def trio_cross(b, item):
        for p in range(2):
            trio_copy(b, 1, item, p).wait_recv()
            both = mid[b, item, p, 0].astype(f32) + got[b, 1, item, p, 0].astype(f32)
            tot[b, item, p, own[p]] = both.astype(bf16)
            trio_copy(b, 2, item, p).start()

    def step_half(b, item, p, factor, grad):
        moment = momentum_decay * mst[item, p] - grad * factor
        weight = wst[item, p]
        stepped = weight - learn_rate * moment
        before = jnp.sum(weight * weight, axis=2, keepdims=True)
        after = jnp.sum(stepped * stepped, axis=2, keepdims=True)
        weight = stepped * jnp.sqrt(before / (after + epsilon))
        mst[item, p] = moment
        wst[item, p] = weight
        bank[b, item, p] = weight.astype(bf16)

    def update(b, item):
        s = b // blocks
        g = b - s * blocks
        square = sq[0, s, pl.ds(g, 1), :]
        for p in range(1, n):
            square = square + sq[p, s, pl.ds(g, 1), :]
        factor = lax.rsqrt(jnp.concatenate([square] * (head // LANES), axis=1))

        @pl.when(even)
        def _():
            for p in range(2):
                pair_copy(b, 1, item, p).wait_recv()
                grad = mid[b, item, p].astype(f32) + got[b, 1, item, p].astype(f32)
                step_half(b, item, p, factor, grad)

        @pl.when(odd)
        def _():
            for p in range(2):
                trio_copy(b, 2, item, p).wait_recv()
                step_half(b, item, p, factor, tot[b, item, p].astype(f32))

    def apply_fast(b, begin, stop):
        if begin == 0:
            pltpu.make_async_copy(q_hbm.at[b], qbuf.at[b], load_sem.at[2, b]).wait()
        apply_tiles(begin, stop, tile, [matrix(b, item) for item in range(3)], qbuf.at[b], obuf.at[b])

    prepare_keys(0)
    prepare_values(0)
    for copy in entry_copies(0):
        copy.wait_send()
    start(moment_copies(0))
    arrive(entry_copies(0))
    for copy in inputs[3:]:
        copy.wait()
    cut = (tiles + 1) // 2

    @pl.loop(0, total)
    def _(b):
        s = b // blocks
        g = b - s * blocks
        inside = (g + blocks - 1) // blocks
        slot = (total + s) * (1 - inside) + (b - 1) * inside
        entered = jnp.logical_and(jnp.logical_and(g == 0, s > 0), jnp.logical_not(first))
        renewed = jnp.logical_and(jnp.logical_and(g == 0, s > 0), first)
        border = jnp.logical_and(g == blocks - 1, s < steps - 1)
        passing = jnp.logical_and(border, jnp.logical_not(last))

        @pl.when(renewed)
        def _():
            arrive(entry_copies(s))

        @pl.when(entered)
        def _():
            for item in (0, 2):
                relay_copy(b - 1, s - 1, item).wait_recv()

        flow(b, slot, 0)
        send_grads(b, 0)

        @pl.when(g > 0)
        def _():
            update(b - 1, 1)

        @pl.when(entered)
        def _():
            relay_copy(b - 1, s - 1, 1).wait_recv()

        flow(b, slot, 1)
        send_grads(b, 2)
        send_grads(b, 1)

        @pl.when(b < total - 1)
        def _():
            prepare_keys(b + 1)

        @pl.when(odd)
        def _():
            trio_sum(b, 0)

        @pl.when(b > 0)
        def _():
            apply_fast(b - 1, 0, cut)

        @pl.when(even)
        def _():
            pair_sum(b, 0)

        @pl.when(odd)
        def _():
            trio_sum(b, 2)
            trio_cross(b, 0)

        @pl.when(b > 0)
        def _():
            apply_fast(b - 1, cut, tiles)

        @pl.when(even)
        def _():
            pair_sum(b, 2)

        @pl.when(odd)
        def _():
            trio_sum(b, 1)
            trio_cross(b, 2)

        @pl.when(b < total - 1)
        def _():
            prepare_values(b + 1)

        @pl.when(even)
        def _():
            pair_sum(b, 1)

        @pl.when(odd)
        def _():
            trio_cross(b, 1)

        for step in range(1, steps):
            @pl.when(jnp.logical_and(first, b == 0))
            def _():
                fill_bank(total + step, fw_in)
                start(entry_copies(step))

            @pl.when(jnp.logical_and(first, b == step * blocks - 1))
            def _():
                mx[step] = fm_in[...].astype(bf16)
                start(moment_copies(step))

        @pl.when(b == 0)
        def _():
            arrive(square_copies())
            take_weights(0, w_in)
            take_moments(0, m_in)

        @pl.when(renewed)
        def _():
            take_weights(s, fw_in)
            take_moments(s, fm_in)

        @pl.when(entered)
        def _():
            for item in range(3):
                wst[item] = bank[total + s, item].astype(f32)
            for item in range(3):
                m_copy(s - 1, item).wait_recv()
                mst[item] = mrecv[s - 1, item].astype(f32)

        def finish(item):
            update(b, item)

            @pl.when(passing)
            def _():
                relay_copy(b, s, item).start()

        finish(0)
        finish(2)

        @pl.when(g == blocks - 1)
        def _():
            finish(1)

        @pl.when(passing)
        def _():
            for item in (0, 2, 1):
                msend[s, item] = mst[item].astype(bf16)
                m_copy(s, item).start()

    usable[...] = bank[total - 1]
    late.wait()
    for ref, state in ((w_out, wst), (m_out, mst)):
        ref[0] = state[outer, 0, inner]
        ref[2] = state[outer, 1, inner]
        ref[1] = state[2, outer, inner]

    def drain_entry(s):
        for copy in entry_copies(s) + moment_copies(s):
            copy.wait_send()

    for copy in moment_copies(0):
        copy.wait_send()

    @pl.when(first)
    def _():
        for s in range(1, steps):
            drain_entry(s)

    for copy in square_copies():
        copy.wait_send()

    @pl.when(jnp.logical_not(last))
    def _():
        for s in range(steps - 1):
            for item in range(3):
                relay_copy(s * blocks + blocks - 1, s, item).wait_send()
                m_copy(s, item).wait_send()

    @pl.loop(0, total)
    def _(b):
        @pl.when(even)
        def _():
            for stage in range(2):
                for item in range(3):
                    for p in range(2):
                        pair_copy(b, stage, item, p).wait_send()

        @pl.when(odd)
        def _():
            for stage in range(3):
                for item in range(3):
                    for p in range(2):
                        trio_copy(b, stage, item, p).wait_send()


def tail_kernel(
    tile, done, usable, asked, w_ready, m_ready, out_hbm, w_hbm, m_hbm, obuf, sem,
):
    count = done.shape[0]
    rows, head = asked.shape
    copies = [
        pltpu.make_async_copy(src, dst, sem.at[j])
        for j, (src, dst) in enumerate(
            [(w_ready, w_hbm), (m_ready, m_hbm)] + [(done.at[b], out_hbm.at[b]) for b in range(count)]
        )
    ]
    for copy in copies:
        copy.start()
    weights = [usable[item].reshape(head, head) for item in range(3)]
    for i in range(rows // tile):
        apply_tiles(i, i + 1, tile, weights, asked, obuf)
        at = pl.ds(i * tile, tile)
        copy = pltpu.make_async_copy(obuf.at[at], out_hbm.at[count, at], sem.at[count + 2 + i])
        copy.start()
        copies.append(copy)
    for copy in copies:
        copy.wait()


def quad_scratch(steps, blocks, rows, head):
    total = steps * blocks
    quarter = head // 4
    flat = (total, rows, head)
    whole = (2, 2, quarter, head)
    piece = (3, quarter, head)
    dma = pltpu.SemaphoreType.DMA
    vmem = pltpu.VMEM
    return [vmem(flat, bf16)] * 2 + [
        vmem((total - 1, rows, head), bf16),
        vmem((head, rows), bf16),
        vmem((rows, head), bf16),
        vmem((head, rows), bf16),
        vmem((rows, head), bf16),
        vmem((2, rows, head), bf16),
        vmem((total + steps, 3) + whole, bf16),
        vmem((total, 3) + whole, bf16),
        vmem((total, 2, 3) + whole, bf16),
        vmem((total, 3) + whole, bf16),
        vmem((total, 3) + whole, bf16),
        vmem((3,) + whole, f32),
        vmem((3,) + whole, f32),
        vmem(piece, f32),
        vmem(piece, f32),
        vmem(piece, f32),
        vmem(piece, f32),
        vmem((steps, blocks, rows), f32),
        vmem((steps,) + piece, bf16),
        vmem((steps, 4) + piece, bf16),
        vmem((steps, 3) + whole, bf16),
        vmem((steps, 3) + whole, bf16),
        vmem((4, steps, blocks, LANES), f32),
        dma((3, total)),
        dma((5,)),
        dma((total, 3, 3, 2)),
        dma((total, 3, 3, 2)),
        dma((steps, 4, 2)),
        dma((steps, 4, 2)),
        dma((steps, 3)),
        dma((steps, 3)),
        dma((steps, 3)),
        dma((steps, 3)),
        dma((steps, 4)),
        dma((steps, 4)),
        dma((4,)),
        dma((4,)),
    ]


def body(n, segs, queries, keys, values, rates, weights, momenta, fresh_w, fresh_m):
    steps, _, blocks, rows, head = queries.shape
    total = steps * blocks
    width = head // n
    tile = 256 if rows % 256 == 0 else rows
    flat = (total, rows, head)
    piece = (3, width, head)
    hbm = pl.BlockSpec(memory_space=pl.ANY)
    vmem = pl.BlockSpec(memory_space=pltpu.VMEM)
    dma = pltpu.SemaphoreType.DMA
    big = (rows, head)
    turned = (head, rows)
    operands = (
        keys.reshape(flat), values.reshape(flat), queries.reshape(flat), rates[:, 0],
        jnp.swapaxes(weights[0], 1, 2), jnp.swapaxes(momenta[0], 1, 2),
        jnp.swapaxes(fresh_w, 1, 2), jnp.swapaxes(fresh_m, 1, 2),
    )
    results = (
        jax.ShapeDtypeStruct(flat, bf16),
        jax.ShapeDtypeStruct(piece, f32),
        jax.ShapeDtypeStruct(piece, f32),
    )
    if n == 4 and head % 256 == 0:
        ready = pl.pallas_call(
            functools.partial(quad_kernel, segs, steps, blocks, tile),
            out_shape=(
                jax.ShapeDtypeStruct((total - 1, rows, head), bf16),
                jax.ShapeDtypeStruct((3, 2, 2, head // 4, head), bf16),
                jax.ShapeDtypeStruct(big, bf16),
                *results[1:],
            ),
            in_specs=[pl.BlockSpec(memory_space=pltpu.HBM)] * 8,
            out_specs=(vmem,) * 5,
            scratch_shapes=quad_scratch(steps, blocks, rows, head),
            compiler_params=pltpu.CompilerParams(
                collective_id=0, has_side_effects=True, vmem_limit_bytes=QUAD_VMEM
            ),
        )(*(pltpu.with_memory_space_constraint(x, pltpu.HBM) for x in operands))
        outs = pl.pallas_call(
            functools.partial(tail_kernel, tile),
            out_shape=results,
            in_specs=[vmem] * 5,
            out_specs=(hbm,) * 3,
            scratch_shapes=[pltpu.VMEM(big, bf16), dma((total + 1 + rows // tile,))],
            compiler_params=pltpu.CompilerParams(vmem_limit_bytes=16 * 1024 * 1024),
        )(*ready)
    else:
        outs = pl.pallas_call(
            functools.partial(kernel, n, segs, steps, blocks, tile),
            out_shape=results,
            in_specs=[hbm, hbm, hbm, vmem, vmem, vmem, vmem, vmem],
            out_specs=(hbm, vmem, vmem),
            scratch_shapes=[pltpu.VMEM(flat, bf16)] * 4 + [
                pltpu.VMEM(turned, bf16),
                pltpu.VMEM(big, bf16),
                pltpu.VMEM(turned, bf16),
                pltpu.VMEM(big, bf16),
                pltpu.VMEM(big, bf16),
                pltpu.VMEM(big, bf16),
                pltpu.VMEM((3, head, head), bf16),
                pltpu.VMEM((total, n) + piece, bf16),
                pltpu.VMEM((total + steps, 3, head, head), bf16),
                pltpu.VMEM((steps,) + piece, bf16),
                pltpu.VMEM((steps,) + piece, bf16),
                pltpu.VMEM((n, steps, blocks, LANES), f32),
                dma((3, total)),
                dma((total,)),
                dma((total, n, 3)),
                dma((total, n, 3)),
                dma((total, n, 3)),
                dma((total, n, 3)),
                dma((steps, n, 3)),
                dma((steps, n, 3)),
                dma((steps,)),
                dma((steps,)),
                dma((n,)),
                dma((n,)),
        ],
            compiler_params=pltpu.CompilerParams(
                collective_id=0, has_side_effects=True, vmem_limit_bytes=60 * 1024 * 1024
            ),
        )(*operands)
    return (
        outs[0].reshape(queries.shape),
        jnp.swapaxes(outs[1], 1, 2)[None],
        jnp.swapaxes(outs[2], 1, 2)[None],
    )


def solution(mesh):
    n, segs = mesh.shape["tok"], mesh.shape["seg"]
    return jax.shard_map(
        functools.partial(body, n, segs),
        mesh=mesh,
        in_specs=(
            P(None, "seg", None, "tok", None),
            P(None, "seg", None, "tok", None),
            P(None, "seg", None, "tok", None),
            P(None, "seg", None, "tok"),
            P("seg", None, None, "tok"),
            P("seg", None, None, "tok"),
            P(None, None, "tok"),
            P(None, None, "tok"),
        ),
        out_specs=(
            P(None, "seg", None, "tok", None),
            P("seg", None, None, "tok"),
            P("seg", None, None, "tok"),
        ),
        check_vma=False,
    )
```

```python
import functools
import jax
import jax.numpy as jnp
from jax import lax
from jax.experimental import pallas as pl
from jax.experimental.pallas import tpu as pltpu
from jax.sharding import PartitionSpec as P

momentum_decay = 0.9
learn_rate = 0.05
epsilon = 1e-06
LANES = 128
UNROLL = 5
QUAD_VMEM = 40 * 1024 * 1024
MESH = pl.DeviceIdType.MESH
f32 = jnp.float32
bf16 = jnp.bfloat16


def flip(index, mask):
    out, bit = index, 1
    while bit <= mask:
        if mask & bit:
            out = out + bit * (1 - 2 * lax.rem(index // bit, 2))
        bit *= 2
    return out


def sigmoid(x):
    return 0.5 + 0.5 * jnp.tanh(0.5 * x)


def mm(a, b):
    return jnp.dot(a, b, preferred_element_type=f32)


def mm_t(a, b):
    return lax.dot_general(a, b, (((1,), (1,)), ((), ())), preferred_element_type=f32)


def kernel(
    n, segs, steps, blocks, tile,
    k_hbm, v_hbm, q_hbm, rates, w_in, m_in, fw_in, fm_in,
    out_hbm, wstate, mstate,
    kbuf, vbuf, qbuf, obuf, kt, scaled, scaled_t, hid, bgate, bup,
    gsend, grecv, bank, msend, mrecv, sq,
    load_sem, store_sem, gs_sem, gr_sem, os_sem, or_sem, es_sem, er_sem, ms_sem, mr_sem,
    qs_sem, qr_sem,
):
    total = steps * blocks
    rows, head = kbuf.shape[1], kbuf.shape[2]
    width = head // n
    tiles = rows // tile
    order = (1, 0, 2)
    around = tuple(range(n - 1, 0, -1))
    seg = lax.axis_index("seg")
    tok = lax.axis_index("tok")
    first = seg == 0
    last = seg == segs - 1
    peers = [flip(tok, d) for d in range(n)]

    def part(p):
        return pl.ds(pl.multiple_of(p * width, width), width)

    mine = part(tok)

    def to_peer(d):
        return {"seg": seg, "tok": peers[d]}

    down = {"seg": lax.rem(seg + 1, segs), "tok": tok}
    up = {"seg": lax.rem(seg + segs - 1, segs), "tok": tok}

    def rcopy(src, dst, send, recv, device):
        return pltpu.make_async_remote_copy(
            src_ref=src, dst_ref=dst, send_sem=send, recv_sem=recv,
            device_id=device, device_id_type=MESH,
        )

    loads = [[
        pltpu.make_async_copy(src.at[b], dst.at[b], load_sem.at[j, b])
        for b in range(total)
    ] for j, (src, dst) in enumerate(((k_hbm, kbuf), (v_hbm, vbuf), (q_hbm, qbuf)))]

    barrier = pltpu.get_barrier_semaphore()
    for d in range(1, n):
        pl.semaphore_signal(barrier, inc=1, device_id=to_peer(d), device_id_type=MESH)

    @pl.when(jnp.logical_not(last))
    def _():
        pl.semaphore_signal(barrier, inc=1, device_id=down, device_id_type=MESH)

    @pl.when(jnp.logical_not(first))
    def _():
        pl.semaphore_signal(barrier, inc=1, device_id=up, device_id_type=MESH)

    for b in range(total):
        loads[0][b].start()
        loads[1][b].start()
    for b in range(total):
        loads[2][b].start()

    wstate[...] = w_in[...]
    mstate[...] = m_in[...]
    for m in range(3):
        bank[total, m, mine, :] = w_in[m].astype(bf16)
    for s in range(steps):
        drawn = rates[s]
        sums = jnp.sum(drawn * drawn, axis=1, keepdims=True)
        sq[tok, s] = jnp.broadcast_to(sums, (blocks, LANES))

    @pl.when(first)
    def _():
        for s in range(1, steps):
            for m in range(3):
                bank[total + s, m, mine, :] = fw_in[m].astype(bf16)

    neighbours = (seg + segs - 1) // segs + (2 * segs - 2 - seg) // segs
    pl.semaphore_wait(barrier, n - 1 + neighbours)

    def ent_copy(s, d, m):
        place = bank.at[total + s, m, mine, :]
        return rcopy(place, place, es_sem.at[s, d, m], er_sem.at[s, d, m], to_peer(d))

    def sq_copy(d):
        return rcopy(sq.at[tok], sq.at[tok], qs_sem.at[d], qr_sem.at[d], to_peer(d))

    for m in order:
        for d in around:
            ent_copy(0, d, m).start()
    for d in around:
        sq_copy(d).start()

    @pl.when(first)
    def _():
        for s in range(1, steps):
            for m in order:
                for d in around:
                    ent_copy(s, d, m).start()

    def g_copy(b, d, m):
        return rcopy(
            gsend.at[m, part(peers[d]), :], grecv.at[b, d, m],
            gs_sem.at[b, d, m], gr_sem.at[b, d, m], to_peer(d),
        )

    def own_copy(b, d, m):
        place = bank.at[b, m, mine, :]
        return rcopy(place, place, os_sem.at[b, d, m], or_sem.at[b, d, m], to_peer(d))

    def relay_copy(b, s, d, m):
        piece = part(peers[d])
        return rcopy(
            bank.at[b, m, piece, :], bank.at[total + s + 1, m, piece, :],
            es_sem.at[s + 1, d, m], er_sem.at[s + 1, d, m], down,
        )

    def m_copy(s):
        return rcopy(msend.at[s], mrecv.at[s], ms_sem.at[s], mr_sem.at[s], down)

    def prepare(b):
        pltpu.make_async_copy(k_hbm.at[b], kbuf.at[b], load_sem.at[0, b]).wait()
        pltpu.make_async_copy(v_hbm.at[b], vbuf.at[b], load_sem.at[1, b]).wait()
        kt[...] = kbuf[b].T
        s = b // blocks
        row = jnp.broadcast_to(rates[s, pl.ds(b - s * blocks, 1), :], (LANES, rows))
        column = jnp.concatenate([row.T] * (head // LANES), axis=1)
        product = (column * vbuf[b].astype(f32)).astype(bf16)
        scaled[...] = product
        scaled_t[...] = product.T

    def gradients(b, slot):
        w1, w2, w3 = bank[slot, 0], bank[slot, 1], bank[slot, 2]

        @pl.loop(0, tiles, unroll=UNROLL)
        def _(i):
            at = pl.ds(pl.multiple_of(i * tile, tile), tile)
            keys = kbuf[b, at, :]
            back = mm(scaled[at, :], w2)
            gate = mm_t(keys, w1)
            up_pre = mm_t(keys, w3)
            sig = sigmoid(gate)
            act = gate * sig
            slope = sig + act * (1.0 - sig)
            hid[at, :] = (act * up_pre).astype(bf16)
            bgate[at, :] = (back * up_pre * slope).astype(bf16)
            bup[at, :] = (back * act).astype(bf16)

        for m in order:
            if m == 1:
                grad = mm(scaled_t[...], hid[...])
            else:
                grad = mm(kt[...], (bgate if m == 0 else bup)[...]).T
            gsend[m] = grad.astype(bf16)
            for d in around:
                g_copy(b, d, m).start()

    def update(b, m, factor):
        grad = gsend[m, mine, :].astype(f32)
        for d in range(1, n):
            grad = grad + grecv[b, d, m].astype(f32)
        moment = momentum_decay * mstate[m] - grad * factor
        weight = wstate[m]
        stepped = weight - learn_rate * moment
        before = jnp.sum(weight * weight, axis=1, keepdims=True)
        after = jnp.sum(stepped * stepped, axis=1, keepdims=True)
        weight = stepped * jnp.sqrt(before / (after + epsilon))
        mstate[m] = moment
        wstate[m] = weight
        bank[b, m, mine, :] = weight.astype(bf16)

    def apply_fast(b):
        pltpu.make_async_copy(q_hbm.at[b], qbuf.at[b], load_sem.at[2, b]).wait()
        w1, w2, w3 = bank[b, 0], bank[b, 1], bank[b, 2]

        @pl.loop(0, tiles, unroll=UNROLL)
        def _(i):
            at = pl.ds(pl.multiple_of(i * tile, tile), tile)
            asked = qbuf[b, at, :]
            gate = mm_t(asked, w1)
            hidden = (gate * sigmoid(gate) * mm_t(asked, w3)).astype(bf16)
            obuf[b, at, :] = mm_t(hidden, w2).astype(bf16)

        pltpu.make_async_copy(obuf.at[b], out_hbm.at[b], store_sem.at[b]).start()

    prepare(0)
    for d in range(1, n):
        sq_copy(d).wait_recv()

    @pl.loop(0, total)
    def _(b):
        s = b // blocks
        g = b - s * blocks
        inner = (g + blocks - 1) // blocks
        entered = jnp.logical_and(jnp.logical_and(g == 0, s > 0), jnp.logical_not(first))

        @pl.when(g == 0)
        def _():
            for m in order:
                for d in around:
                    ent_copy(s, d, m).wait_recv()

        @pl.when(jnp.logical_and(jnp.logical_and(g == 0, s > 0), first))
        def _():
            wstate[...] = fw_in[...]
            mstate[...] = fm_in[...]

        @pl.when(entered)
        def _():
            for m in order:
                relay_copy(b - 1, s - 1, 0, m).wait_recv()
                wstate[m] = bank[total + s, m, mine, :].astype(f32)

        gradients(b, (total + s) * (1 - inner) + (b - 1) * inner)

        @pl.when(g > 0)
        def _():
            apply_fast(b - 1)

        @pl.when(entered)
        def _():
            m_copy(s - 1).wait_recv()
            mstate[...] = mrecv[s - 1].astype(f32)

        border = jnp.logical_and(g == blocks - 1, s < steps - 1)
        passing = jnp.logical_and(border, jnp.logical_not(last))
        square = sq[0, s, pl.ds(g, 1), :]
        for p in range(1, n):
            square = square + sq[p, s, pl.ds(g, 1), :]
        factor = lax.rsqrt(jnp.concatenate([square] * (head // LANES), axis=1))

        for m in order:
            for d in around:
                g_copy(b, d, m).wait_recv()
            update(b, m, factor)

            @pl.when(passing)
            def _():
                relay_copy(b, s, 0, m).start()

            for d in around:
                own_copy(b, d, m).start()

        @pl.when(passing)
        def _():
            msend[s] = mstate[...].astype(bf16)
            m_copy(s).start()

        for m in order:
            for d in around:
                g_copy(b, d, m).wait_send()

        @pl.when(b < total - 1)
        def _():
            prepare(b + 1)

        for m in order:
            for d in range(1, n):
                own_copy(b, d, m).wait_recv()

                @pl.when(passing)
                def _():
                    relay_copy(b, s, d, m).start()

        @pl.when(g == blocks - 1)
        def _():
            apply_fast(b)

        for m in order:
            for d in around:
                own_copy(b, d, m).wait_send()

        @pl.when(passing)
        def _():
            for m in order:
                for d in range(n):
                    relay_copy(b, s, d, m).wait_send()
            m_copy(s).wait_send()

    for d in around:
        sq_copy(d).wait_send()
        for m in order:
            ent_copy(0, d, m).wait_send()

    @pl.when(first)
    def _():
        for s in range(1, steps):
            for m in order:
                for d in around:
                    ent_copy(s, d, m).wait_send()

    for b in range(total):
        pltpu.make_async_copy(obuf.at[b], out_hbm.at[b], store_sem.at[b]).wait()


def apply_tiles(begin, stop, tile, weights, asked_ref, out_ref):
    half = asked_ref.shape[-1] // 2

    @pl.loop(begin, stop, unroll=min(UNROLL, stop - begin))
    def _(i):
        at = pl.ds(pl.multiple_of(i * tile, tile), tile)
        asked = asked_ref[at, :]
        parts = []
        for w13 in weights[:2]:
            both = mm_t(asked, w13)
            gate = both[:, :half]
            parts.append((gate * sigmoid(gate) * both[:, half:]).astype(bf16))
        out_ref[at, :] = mm_t(jnp.concatenate(parts, axis=1), weights[2]).astype(bf16)


def quad_kernel(
    segs, steps, blocks, tile,
    k_hbm, v_hbm, q_hbm, rates_hbm, w_hbm, m_hbm, fw_hbm, fm_hbm,
    obuf, usable, asked_last, w_out, m_out,
    kbuf, vbuf, qbuf, kt, scaled, scaled_t, hid, bgu,
    bank, gs, got, mid, tot, wst, mst,
    w_in, m_in, fw_in, fm_in, rates, mx, mr, msend, mrecv, sq,
    load_sem, in_sem, st_s, st_r, en_s, en_r, rl_s, rl_r, mm_s, mm_r, mx_s, mx_r, qs, qr,
):
    total = steps * blocks
    n = 4
    rows, head = kbuf.shape[1], kbuf.shape[2]
    half = head // 2
    tiles = rows // tile
    seg = lax.axis_index("seg")
    tok = lax.axis_index("tok")
    inner = lax.rem(tok, 2)
    outer = tok // 2
    first = seg == 0
    last = seg == segs - 1
    peers = [flip(tok, d) for d in range(n)]

    def to_peer(d):
        return {"seg": seg, "tok": peers[d]}

    gather_to = (to_peer(1), to_peer(2))
    cross_to = (to_peer(2), to_peer(1))
    own = (inner, outer)
    far = (1 - inner, 1 - outer)
    odd = lax.rem(seg, 2) == 1
    even = jnp.logical_not(odd)
    down = {"seg": lax.rem(seg + 1, segs), "tok": tok}
    up = {"seg": lax.rem(seg + segs - 1, segs), "tok": tok}

    def rcopy(src, dst, send, recv, device):
        return pltpu.make_async_remote_copy(
            src_ref=src, dst_ref=dst, send_sem=send, recv_sem=recv,
            device_id=device, device_id_type=MESH,
        )

    barrier = pltpu.get_barrier_semaphore()
    for d in range(1, n):
        pl.semaphore_signal(barrier, inc=1, device_id=to_peer(d), device_id_type=MESH)

    @pl.when(jnp.logical_not(last))
    def _():
        pl.semaphore_signal(barrier, inc=1, device_id=down, device_id_type=MESH)

    @pl.when(jnp.logical_not(first))
    def _():
        pl.semaphore_signal(barrier, inc=1, device_id=up, device_id_type=MESH)

    inputs = [
        pltpu.make_async_copy(src, dst, in_sem.at[j])
        for j, (src, dst) in enumerate((
            (w_hbm, w_in), (m_hbm, m_in), (rates_hbm, rates), (fw_hbm, fw_in), (fm_hbm, fm_in),
        ))
    ]
    early = [
        pltpu.make_async_copy(src.at[0], dst.at[0], load_sem.at[j])
        for j, (src, dst) in enumerate(((k_hbm, kbuf), (v_hbm, vbuf)))
    ]
    rest = pl.ds(1, total - 1)
    later = [
        pltpu.make_async_copy(k_hbm.at[rest], kbuf.at[rest], load_sem.at[2]),
        pltpu.make_async_copy(v_hbm.at[rest], vbuf.at[rest], load_sem.at[3]),
        pltpu.make_async_copy(q_hbm.at[pl.ds(0, total - 1)], qbuf, load_sem.at[4]),
        pltpu.make_async_copy(q_hbm.at[total - 1], asked_last, load_sem.at[5]),
    ]
    for copy in (*inputs[:3], *early):
        copy.start()

    def fill_bank(e, source):
        bank[e, outer, 0, inner] = source[0].astype(bf16)
        bank[e, outer, 1, inner] = source[2].astype(bf16)
        bank[e, 2, outer, inner] = source[1].astype(bf16)

    def entry_copy(s, j, d):
        e = total + s
        piece = bank.at[e, 2, outer, inner] if j else bank.at[e, outer, :, inner]
        return rcopy(piece, piece, en_s.at[d - 1, j], en_r.at[s, d - 1, j], to_peer(d))

    def start_entry(s):
        @pl.when(outer == 0)
        def _():
            for j in (0, 1):
                for d in (3, 1, 2):
                    entry_copy(s, j, d).start()

        @pl.when(outer == 1)
        def _():
            for j in (1, 0):
                for d in (3, 1, 2):
                    entry_copy(s, j, d).start()

    def arrive_entry(s, c):
        @pl.when(outer == c)
        def _():
            entry_copy(s, 0, 1).wait_recv()

        @pl.when(outer != c)
        def _():
            for d in (2, 3):
                entry_copy(s, 0, d).wait_recv()

    def moment_copies(s):
        return [
            rcopy(mx.at[s], mr.at[s, tok], mx_s.at[d - 1], mx_r.at[s, d - 1], to_peer(d))
            for d in (1, 2, 3)
        ]

    def square_copies():
        return [
            rcopy(sq.at[tok], sq.at[tok], qs.at[d - 1], qr.at[d - 1], to_peer(d)) for d in (1, 2, 3)
        ]

    def start(copies):
        for copy in copies:
            copy.start()

    def arrive(copies):
        for copy in copies:
            copy.wait_recv()

    def take_weights(s, weights):
        e = total + s
        for item in range(3):
            wst[item] = bank[e, item].astype(f32)
        wst[outer, 0, inner] = weights[0]
        wst[outer, 1, inner] = weights[2]
        wst[2, outer, inner] = weights[1]

    def take_moments(s, moments):
        arrive(moment_copies(s))
        for o in range(2):
            for i in range(2):
                @pl.when(tok != 2 * o + i)
                def _():
                    mst[o, 0, i] = mr[s, 2 * o + i, 0].astype(f32)
                    mst[o, 1, i] = mr[s, 2 * o + i, 2].astype(f32)
                    mst[2, o, i] = mr[s, 2 * o + i, 1].astype(f32)
        mst[outer, 0, inner] = moments[0]
        mst[outer, 1, inner] = moments[2]
        mst[2, outer, inner] = moments[1]

    inputs[0].wait()
    fill_bank(total, w_in)
    neighbours = (seg + segs - 1) // segs + (2 * segs - 2 - seg) // segs
    pl.semaphore_wait(barrier, n - 1 + neighbours)
    start_entry(0)
    for copy in later:
        copy.start()
    for copy in inputs[3:]:
        copy.start()
    inputs[1].wait()
    mx[0] = m_in[...].astype(bf16)
    inputs[2].wait()
    for s in range(steps):
        drawn = rates[s]
        sums = jnp.sum(drawn * drawn, axis=1, keepdims=True)
        sq[tok, s] = jnp.broadcast_to(sums, (blocks, LANES))
    start(square_copies())

    def prepare_keys(b):
        kt[...] = kbuf[b].T

    def prepare_values(b):
        s = b // blocks
        row = jnp.broadcast_to(rates[s, pl.ds(b - s * blocks, 1), :], (LANES, rows))
        column = jnp.concatenate([row.T] * (head // LANES), axis=1)
        product = (column * vbuf[b].astype(f32)).astype(bf16)
        scaled[...] = product
        scaled_t[...] = product.T

    def pair_copy(b, stage, item, p):
        return rcopy(
            (gs, mid)[stage].at[b, item, p], got.at[b, stage, item, p],
            st_s.at[item, p], st_r.at[lax.rem(b, 2), stage, item, p], (gather_to, cross_to)[stage][p],
        )

    def trio_copy(b, stage, item, p):
        if stage == 0:
            src, dst, peer = gs.at[b, item, p, far[p]], got.at[b, 0, item, p, 0], gather_to[p]
        elif stage == 1:
            src, dst, peer = mid.at[b, item, p, 0], got.at[b, 1, item, p, 0], cross_to[p]
        else:
            src, peer = tot.at[b, item, p, own[p]], gather_to[p]
            dst = src
        return rcopy(src, dst, st_s.at[item, p], st_r.at[lax.rem(b, 2), stage, item, p], peer)

    def relay_copy(b, s, item):
        return rcopy(
            bank.at[b, item], bank.at[total + s + 1, item],
            rl_s.at[s, item], rl_r.at[s, item], down,
        )

    def m_copy(s, item):
        return rcopy(msend.at[s, item], mrecv.at[s, item], mm_s.at[s, item], mm_r.at[s, item], down)

    def matrix(slot, item):
        return bank[slot, item].reshape(head, head)

    def flow(b, slot, c):
        w13 = matrix(slot, c)
        w2 = matrix(slot, 2)[:, c * half:(c + 1) * half]

        @pl.loop(0, tiles, unroll=UNROLL)
        def _(i):
            at = pl.ds(pl.multiple_of(i * tile, tile), tile)
            both = mm_t(kbuf[b, at, :], w13)
            back = mm(scaled[at, :], w2)
            gate, up_pre = both[:, :half], both[:, half:]
            sig = sigmoid(gate)
            act = gate * sig
            slope = sig + act * (1.0 - sig)
            hid[at, c * half:(c + 1) * half] = (act * up_pre).astype(bf16)
            bgu[c, at, :half] = (back * up_pre * slope).astype(bf16)
            bgu[c, at, half:] = (back * act).astype(bf16)

    def send_grads(b, item):
        if item < 2:
            grad = mm(kt[...], bgu[item]).astype(bf16).T
        else:
            grad = mm(scaled_t[...], hid[...]).astype(bf16)
        for p in range(2):
            gs[b, item, p] = grad[p * half:(p + 1) * half].reshape(gs.shape[3:])

            @pl.when(jnp.logical_and(even, b > 0))
            def _():
                pair_copy(b - 1, 1, item, p).wait_send()

            @pl.when(jnp.logical_and(odd, b > 0))
            def _():
                trio_copy(b - 1, 2, item, p).wait_send()

            @pl.when(even)
            def _():
                pair_copy(b, 0, item, p).start()

            @pl.when(odd)
            def _():
                trio_copy(b, 0, item, p).start()

    def pair_sum(b, item):
        for p in range(2):
            pair_copy(b, 0, item, p).wait_recv()
            mid[b, item, p] = (gs[b, item, p].astype(f32) + got[b, 0, item, p].astype(f32)).astype(bf16)
            pair_copy(b, 0, item, p).wait_send()
            pair_copy(b, 1, item, p).start()

    def trio_sum(b, item):
        for p in range(2):
            trio_copy(b, 0, item, p).wait_recv()
            mine = gs[b, item, p, own[p]].astype(f32)
            mid[b, item, p, 0] = (mine + got[b, 0, item, p, 0].astype(f32)).astype(bf16)
            trio_copy(b, 0, item, p).wait_send()
            trio_copy(b, 1, item, p).start()

    def trio_cross(b, item):
        for p in range(2):
            trio_copy(b, 1, item, p).wait_recv()
            both = mid[b, item, p, 0].astype(f32) + got[b, 1, item, p, 0].astype(f32)
            tot[b, item, p, own[p]] = both.astype(bf16)
            trio_copy(b, 1, item, p).wait_send()
            trio_copy(b, 2, item, p).start()

    def step_half(b, item, p, factor, grad):
        moment = momentum_decay * mst[item, p] - grad * factor
        weight = wst[item, p]
        stepped = weight - learn_rate * moment
        before = jnp.sum(weight * weight, axis=2, keepdims=True)
        after = jnp.sum(stepped * stepped, axis=2, keepdims=True)
        weight = stepped * jnp.sqrt(before / (after + epsilon))
        mst[item, p] = moment
        wst[item, p] = weight
        bank[b, item, p] = weight.astype(bf16)

    def update(b, item):
        s = b // blocks
        g = b - s * blocks
        square = sq[0, s, pl.ds(g, 1), :]
        for p in range(1, n):
            square = square + sq[p, s, pl.ds(g, 1), :]
        factor = lax.rsqrt(jnp.concatenate([square] * (head // LANES), axis=1))

        @pl.when(even)
        def _():
            for p in range(2):
                pair_copy(b, 1, item, p).wait_recv()
                grad = mid[b, item, p].astype(f32) + got[b, 1, item, p].astype(f32)
                step_half(b, item, p, factor, grad)

        @pl.when(odd)
        def _():
            for p in range(2):
                trio_copy(b, 2, item, p).wait_recv()
                step_half(b, item, p, factor, tot[b, item, p].astype(f32))

    def apply_fast(b, begin, stop):
        apply_tiles(begin, stop, tile, [matrix(b, item) for item in range(3)], qbuf.at[b], obuf.at[b])

    early[0].wait()
    prepare_keys(0)
    early[1].wait()
    prepare_values(0)
    for j in range(2):
        entry_copy(0, j, 3).wait_send()
    start(moment_copies(0))
    for copy in inputs[3:]:
        copy.wait()
    cut = (tiles + 1) // 2

    @pl.loop(0, total)
    def _(b):
        s = b // blocks
        g = b - s * blocks
        inside = (g + blocks - 1) // blocks
        slot = (total + s) * (1 - inside) + (b - 1) * inside
        entered = jnp.logical_and(jnp.logical_and(g == 0, s > 0), jnp.logical_not(first))
        renewed = jnp.logical_and(jnp.logical_and(g == 0, s > 0), first)
        border = jnp.logical_and(g == blocks - 1, s < steps - 1)
        passing = jnp.logical_and(border, jnp.logical_not(last))

        newly = jnp.logical_and(g == 0, jnp.logical_or(first, s == 0))

        @pl.when(newly)
        def _():
            for d in (1, 2, 3):
                entry_copy(s, 1, d).wait_recv()
            arrive_entry(s, 0)

        @pl.when(entered)
        def _():
            for item in (0, 2):
                relay_copy(b - 1, s - 1, item).wait_recv()

        flow(b, slot, 0)
        send_grads(b, 0)

        @pl.when(g > 0)
        def _():
            update(b - 1, 1)

        @pl.when(newly)
        def _():
            arrive_entry(s, 1)

        @pl.when(entered)
        def _():
            relay_copy(b - 1, s - 1, 1).wait_recv()

        flow(b, slot, 1)
        send_grads(b, 2)
        send_grads(b, 1)

        @pl.when(b == 0)
        def _():
            for copy in later[:3]:
                copy.wait()

        @pl.when(b < total - 1)
        def _():
            prepare_keys(b + 1)

        @pl.when(odd)
        def _():
            trio_sum(b, 0)

        @pl.when(b > 0)
        def _():
            apply_fast(b - 1, 0, cut)

        @pl.when(even)
        def _():
            pair_sum(b, 0)

        @pl.when(odd)
        def _():
            trio_sum(b, 2)
            trio_cross(b, 0)

        @pl.when(b > 0)
        def _():
            apply_fast(b - 1, cut, tiles)

        @pl.when(even)
        def _():
            pair_sum(b, 2)

        @pl.when(odd)
        def _():
            trio_sum(b, 1)
            trio_cross(b, 2)

        @pl.when(b < total - 1)
        def _():
            prepare_values(b + 1)

        @pl.when(even)
        def _():
            pair_sum(b, 1)

        for step in range(1, steps):
            @pl.when(jnp.logical_and(first, b == 0))
            def _():
                fill_bank(total + step, fw_in)
                for j in range(2):
                    for d in (1, 2) if step == 1 else (1, 2, 3):
                        entry_copy(step - 1, j, d).wait_send()
                start_entry(step)

            @pl.when(jnp.logical_and(first, b == step * blocks - 1))
            def _():
                for copy in moment_copies(step - 1):
                    copy.wait_send()
                mx[step] = fm_in[...].astype(bf16)
                start(moment_copies(step))

        @pl.when(b == 0)
        def _():
            arrive(square_copies())
            take_weights(0, w_in)
            take_moments(0, m_in)

        @pl.when(renewed)
        def _():
            take_weights(s, fw_in)
            take_moments(s, fm_in)

        @pl.when(entered)
        def _():
            for item in range(3):
                wst[item] = bank[total + s, item].astype(f32)
            for item in range(3):
                m_copy(s - 1, item).wait_recv()
                mst[item] = mrecv[s - 1, item].astype(f32)

        def finish(item):
            update(b, item)

            @pl.when(passing)
            def _():
                relay_copy(b, s, item).start()

        finish(0)

        @pl.when(odd)
        def _():
            trio_cross(b, 1)

        finish(2)

        @pl.when(g == blocks - 1)
        def _():
            finish(1)

        @pl.when(passing)
        def _():
            for item in (0, 2, 1):
                msend[s, item] = mst[item].astype(bf16)
                m_copy(s, item).start()

    usable[...] = bank[total - 1]
    later[3].wait()
    for ref, state in ((w_out, wst), (m_out, mst)):
        ref[0] = state[outer, 0, inner]
        ref[2] = state[outer, 1, inner]
        ref[1] = state[2, outer, inner]

    def drain_entry(peers_left):
        for j in range(2):
            for d in peers_left:
                entry_copy(0, j, d).wait_send()
        for copy in moment_copies(0):
            copy.wait_send()

    if steps > 1:
        @pl.when(first)
        def _():
            drain_entry((1, 2, 3))

        @pl.when(jnp.logical_not(first))
        def _():
            drain_entry((1, 2))
    else:
        drain_entry((1, 2))

    for copy in square_copies():
        copy.wait_send()

    @pl.when(jnp.logical_not(last))
    def _():
        for s in range(steps - 1):
            for item in range(3):
                relay_copy(s * blocks + blocks - 1, s, item).wait_send()
                m_copy(s, item).wait_send()

    for item in range(3):
        for p in range(2):
            @pl.when(even)
            def _():
                pair_copy(total - 1, 1, item, p).wait_send()

            @pl.when(odd)
            def _():
                trio_copy(total - 1, 2, item, p).wait_send()


def tail_kernel(
    tile, done, usable, asked, w_ready, m_ready, out_hbm, w_hbm, m_hbm, obuf, sem,
):
    count = done.shape[0]
    rows, head = asked.shape
    copies = [
        pltpu.make_async_copy(src, dst, sem.at[j])
        for j, (src, dst) in enumerate(
            [(w_ready, w_hbm), (m_ready, m_hbm)] + [(done.at[b], out_hbm.at[b]) for b in range(count)]
        )
    ]
    for copy in copies:
        copy.start()
    weights = [usable[item].reshape(head, head) for item in range(3)]
    for i in range(rows // tile):
        apply_tiles(i, i + 1, tile, weights, asked, obuf)
        at = pl.ds(i * tile, tile)
        copy = pltpu.make_async_copy(obuf.at[at], out_hbm.at[count, at], sem.at[count + 2 + i])
        copy.start()
        copies.append(copy)
    for copy in copies:
        copy.wait()


def quad_scratch(steps, blocks, rows, head):
    total = steps * blocks
    quarter = head // 4
    flat = (total, rows, head)
    whole = (2, 2, quarter, head)
    piece = (3, quarter, head)
    dma = pltpu.SemaphoreType.DMA
    vmem = pltpu.VMEM
    return [vmem(flat, bf16)] * 2 + [
        vmem((total - 1, rows, head), bf16),
        vmem((head, rows), bf16),
        vmem((rows, head), bf16),
        vmem((head, rows), bf16),
        vmem((rows, head), bf16),
        vmem((2, rows, head), bf16),
        vmem((total + steps, 3) + whole, bf16),
        vmem((total, 3) + whole, bf16),
        vmem((total, 2, 3) + whole, bf16),
        vmem((total, 3) + whole, bf16),
        vmem((total, 3) + whole, bf16),
        vmem((3,) + whole, f32),
        vmem((3,) + whole, f32),
        vmem(piece, f32),
        vmem(piece, f32),
        vmem(piece, f32),
        vmem(piece, f32),
        vmem((steps, blocks, rows), f32),
        vmem((steps,) + piece, bf16),
        vmem((steps, 4) + piece, bf16),
        vmem((steps, 3) + whole, bf16),
        vmem((steps, 3) + whole, bf16),
        vmem((4, steps, blocks, LANES), f32),
        dma((6,)),
        dma((5,)),
        dma((3, 2)),
        dma((2, 3, 3, 2)),
        dma((3, 2)),
        dma((steps, 3, 2)),
        dma((steps - 1, 3)),
        dma((steps - 1, 3)),
        dma((steps - 1, 3)),
        dma((steps - 1, 3)),
        dma((3,)),
        dma((steps, 3)),
        dma((3,)),
        dma((3,)),
    ]


def body(n, segs, queries, keys, values, rates, weights, momenta, fresh_w, fresh_m):
    steps, _, blocks, rows, head = queries.shape
    total = steps * blocks
    width = head // n
    tile = 256 if rows % 256 == 0 else rows
    flat = (total, rows, head)
    piece = (3, width, head)
    hbm = pl.BlockSpec(memory_space=pl.ANY)
    vmem = pl.BlockSpec(memory_space=pltpu.VMEM)
    dma = pltpu.SemaphoreType.DMA
    big = (rows, head)
    turned = (head, rows)
    operands = (
        keys.reshape(flat), values.reshape(flat), queries.reshape(flat), rates[:, 0],
        jnp.swapaxes(weights[0], 1, 2), jnp.swapaxes(momenta[0], 1, 2),
        jnp.swapaxes(fresh_w, 1, 2), jnp.swapaxes(fresh_m, 1, 2),
    )
    results = (
        jax.ShapeDtypeStruct(flat, bf16),
        jax.ShapeDtypeStruct(piece, f32),
        jax.ShapeDtypeStruct(piece, f32),
    )
    if n == 4 and head % 256 == 0 and min(steps, blocks) > 1:
        ready = pl.pallas_call(
            functools.partial(quad_kernel, segs, steps, blocks, tile),
            out_shape=(
                jax.ShapeDtypeStruct((total - 1, rows, head), bf16),
                jax.ShapeDtypeStruct((3, 2, 2, head // 4, head), bf16),
                jax.ShapeDtypeStruct(big, bf16),
                *results[1:],
            ),
            in_specs=[pl.BlockSpec(memory_space=pltpu.HBM)] * 8,
            out_specs=(vmem,) * 5,
            scratch_shapes=quad_scratch(steps, blocks, rows, head),
            compiler_params=pltpu.CompilerParams(
                collective_id=0, has_side_effects=True, vmem_limit_bytes=QUAD_VMEM
            ),
        )(*(pltpu.with_memory_space_constraint(x, pltpu.HBM) for x in operands))
        outs = pl.pallas_call(
            functools.partial(tail_kernel, tile),
            out_shape=results,
            in_specs=[vmem] * 5,
            out_specs=(hbm,) * 3,
            scratch_shapes=[pltpu.VMEM(big, bf16), dma((total + 1 + rows // tile,))],
            compiler_params=pltpu.CompilerParams(vmem_limit_bytes=16 * 1024 * 1024),
        )(*ready)
    else:
        outs = pl.pallas_call(
            functools.partial(kernel, n, segs, steps, blocks, tile),
            out_shape=results,
            in_specs=[hbm, hbm, hbm, vmem, vmem, vmem, vmem, vmem],
            out_specs=(hbm, vmem, vmem),
            scratch_shapes=[pltpu.VMEM(flat, bf16)] * 4 + [
                pltpu.VMEM(turned, bf16),
                pltpu.VMEM(big, bf16),
                pltpu.VMEM(turned, bf16),
                pltpu.VMEM(big, bf16),
                pltpu.VMEM(big, bf16),
                pltpu.VMEM(big, bf16),
                pltpu.VMEM((3, head, head), bf16),
                pltpu.VMEM((total, n) + piece, bf16),
                pltpu.VMEM((total + steps, 3, head, head), bf16),
                pltpu.VMEM((steps,) + piece, bf16),
                pltpu.VMEM((steps,) + piece, bf16),
                pltpu.VMEM((n, steps, blocks, LANES), f32),
                dma((3, total)),
                dma((total,)),
                dma((total, n, 3)),
                dma((total, n, 3)),
                dma((total, n, 3)),
                dma((total, n, 3)),
                dma((steps, n, 3)),
                dma((steps, n, 3)),
                dma((steps,)),
                dma((steps,)),
                dma((n,)),
                dma((n,)),
        ],
            compiler_params=pltpu.CompilerParams(
                collective_id=0, has_side_effects=True, vmem_limit_bytes=60 * 1024 * 1024
            ),
        )(*operands)
    return (
        outs[0].reshape(queries.shape),
        jnp.swapaxes(outs[1], 1, 2)[None],
        jnp.swapaxes(outs[2], 1, 2)[None],
    )


def solution(mesh):
    n, segs = mesh.shape["tok"], mesh.shape["seg"]
    return jax.shard_map(
        functools.partial(body, n, segs),
        mesh=mesh,
        in_specs=(
            P(None, "seg", None, "tok", None),
            P(None, "seg", None, "tok", None),
            P(None, "seg", None, "tok", None),
            P(None, "seg", None, "tok"),
            P("seg", None, None, "tok"),
            P("seg", None, None, "tok"),
            P(None, None, "tok"),
            P(None, None, "tok"),
        ),
        out_specs=(
            P(None, "seg", None, "tok", None),
            P("seg", None, None, "tok"),
            P("seg", None, None, "tok"),
        ),
        check_vma=False,
    )
```

```python
import functools
import jax
import jax.numpy as jnp
from jax import lax
from jax.experimental import pallas as pl
from jax.experimental.pallas import tpu as pltpu
from jax.sharding import PartitionSpec as P

momentum_decay = 0.9
learn_rate = 0.05
epsilon = 1e-06
LANES = 128
UNROLL = 5
QUAD_VMEM = 40 * 1024 * 1024
MESH = pl.DeviceIdType.MESH
f32 = jnp.float32
bf16 = jnp.bfloat16


def flip(index, mask):
    out, bit = index, 1
    while bit <= mask:
        if mask & bit:
            out = out + bit * (1 - 2 * lax.rem(index // bit, 2))
        bit *= 2
    return out


def sigmoid(x):
    return 0.5 + 0.5 * jnp.tanh(0.5 * x)


def mm(a, b):
    return jnp.dot(a, b, preferred_element_type=f32)


def mm_t(a, b):
    return lax.dot_general(a, b, (((1,), (1,)), ((), ())), preferred_element_type=f32)


def kernel(
    n, segs, steps, blocks, tile,
    k_hbm, v_hbm, q_hbm, rates, w_in, m_in, fw_in, fm_in,
    out_hbm, wstate, mstate,
    kbuf, vbuf, qbuf, obuf, kt, scaled, scaled_t, hid, bgate, bup,
    gsend, grecv, bank, msend, mrecv, sq,
    load_sem, store_sem, gs_sem, gr_sem, os_sem, or_sem, es_sem, er_sem, ms_sem, mr_sem,
    qs_sem, qr_sem,
):
    total = steps * blocks
    rows, head = kbuf.shape[1], kbuf.shape[2]
    width = head // n
    tiles = rows // tile
    order = (1, 0, 2)
    around = tuple(range(n - 1, 0, -1))
    seg = lax.axis_index("seg")
    tok = lax.axis_index("tok")
    first = seg == 0
    last = seg == segs - 1
    peers = [flip(tok, d) for d in range(n)]

    def part(p):
        return pl.ds(pl.multiple_of(p * width, width), width)

    mine = part(tok)

    def to_peer(d):
        return {"seg": seg, "tok": peers[d]}

    down = {"seg": lax.rem(seg + 1, segs), "tok": tok}
    up = {"seg": lax.rem(seg + segs - 1, segs), "tok": tok}

    def rcopy(src, dst, send, recv, device):
        return pltpu.make_async_remote_copy(
            src_ref=src, dst_ref=dst, send_sem=send, recv_sem=recv,
            device_id=device, device_id_type=MESH,
        )

    loads = [[
        pltpu.make_async_copy(src.at[b], dst.at[b], load_sem.at[j, b])
        for b in range(total)
    ] for j, (src, dst) in enumerate(((k_hbm, kbuf), (v_hbm, vbuf), (q_hbm, qbuf)))]

    barrier = pltpu.get_barrier_semaphore()
    for d in range(1, n):
        pl.semaphore_signal(barrier, inc=1, device_id=to_peer(d), device_id_type=MESH)

    @pl.when(jnp.logical_not(last))
    def _():
        pl.semaphore_signal(barrier, inc=1, device_id=down, device_id_type=MESH)

    @pl.when(jnp.logical_not(first))
    def _():
        pl.semaphore_signal(barrier, inc=1, device_id=up, device_id_type=MESH)

    for b in range(total):
        loads[0][b].start()
        loads[1][b].start()
    for b in range(total):
        loads[2][b].start()

    wstate[...] = w_in[...]
    mstate[...] = m_in[...]
    for m in range(3):
        bank[total, m, mine, :] = w_in[m].astype(bf16)
    for s in range(steps):
        drawn = rates[s]
        sums = jnp.sum(drawn * drawn, axis=1, keepdims=True)
        sq[tok, s] = jnp.broadcast_to(sums, (blocks, LANES))

    @pl.when(first)
    def _():
        for s in range(1, steps):
            for m in range(3):
                bank[total + s, m, mine, :] = fw_in[m].astype(bf16)

    neighbours = (seg + segs - 1) // segs + (2 * segs - 2 - seg) // segs
    pl.semaphore_wait(barrier, n - 1 + neighbours)

    def ent_copy(s, d, m):
        place = bank.at[total + s, m, mine, :]
        return rcopy(place, place, es_sem.at[s, d, m], er_sem.at[s, d, m], to_peer(d))

    def sq_copy(d):
        return rcopy(sq.at[tok], sq.at[tok], qs_sem.at[d], qr_sem.at[d], to_peer(d))

    for m in order:
        for d in around:
            ent_copy(0, d, m).start()
    for d in around:
        sq_copy(d).start()

    @pl.when(first)
    def _():
        for s in range(1, steps):
            for m in order:
                for d in around:
                    ent_copy(s, d, m).start()

    def g_copy(b, d, m):
        return rcopy(
            gsend.at[m, part(peers[d]), :], grecv.at[b, d, m],
            gs_sem.at[b, d, m], gr_sem.at[b, d, m], to_peer(d),
        )

    def own_copy(b, d, m):
        place = bank.at[b, m, mine, :]
        return rcopy(place, place, os_sem.at[b, d, m], or_sem.at[b, d, m], to_peer(d))

    def relay_copy(b, s, d, m):
        piece = part(peers[d])
        return rcopy(
            bank.at[b, m, piece, :], bank.at[total + s + 1, m, piece, :],
            es_sem.at[s + 1, d, m], er_sem.at[s + 1, d, m], down,
        )

    def m_copy(s):
        return rcopy(msend.at[s], mrecv.at[s], ms_sem.at[s], mr_sem.at[s], down)

    def prepare(b):
        pltpu.make_async_copy(k_hbm.at[b], kbuf.at[b], load_sem.at[0, b]).wait()
        pltpu.make_async_copy(v_hbm.at[b], vbuf.at[b], load_sem.at[1, b]).wait()
        kt[...] = kbuf[b].T
        s = b // blocks
        row = jnp.broadcast_to(rates[s, pl.ds(b - s * blocks, 1), :], (LANES, rows))
        column = jnp.concatenate([row.T] * (head // LANES), axis=1)
        product = (column * vbuf[b].astype(f32)).astype(bf16)
        scaled[...] = product
        scaled_t[...] = product.T

    def gradients(b, slot):
        w1, w2, w3 = bank[slot, 0], bank[slot, 1], bank[slot, 2]

        @pl.loop(0, tiles, unroll=UNROLL)
        def _(i):
            at = pl.ds(pl.multiple_of(i * tile, tile), tile)
            keys = kbuf[b, at, :]
            back = mm(scaled[at, :], w2)
            gate = mm_t(keys, w1)
            up_pre = mm_t(keys, w3)
            sig = sigmoid(gate)
            act = gate * sig
            slope = sig + act * (1.0 - sig)
            hid[at, :] = (act * up_pre).astype(bf16)
            bgate[at, :] = (back * up_pre * slope).astype(bf16)
            bup[at, :] = (back * act).astype(bf16)

        for m in order:
            if m == 1:
                grad = mm(scaled_t[...], hid[...])
            else:
                grad = mm(kt[...], (bgate if m == 0 else bup)[...]).T
            gsend[m] = grad.astype(bf16)
            for d in around:
                g_copy(b, d, m).start()

    def update(b, m, factor):
        grad = gsend[m, mine, :].astype(f32)
        for d in range(1, n):
            grad = grad + grecv[b, d, m].astype(f32)
        moment = momentum_decay * mstate[m] - grad * factor
        weight = wstate[m]
        stepped = weight - learn_rate * moment
        before = jnp.sum(weight * weight, axis=1, keepdims=True)
        after = jnp.sum(stepped * stepped, axis=1, keepdims=True)
        weight = stepped * jnp.sqrt(before / (after + epsilon))
        mstate[m] = moment
        wstate[m] = weight
        bank[b, m, mine, :] = weight.astype(bf16)

    def apply_fast(b):
        pltpu.make_async_copy(q_hbm.at[b], qbuf.at[b], load_sem.at[2, b]).wait()
        w1, w2, w3 = bank[b, 0], bank[b, 1], bank[b, 2]

        @pl.loop(0, tiles, unroll=UNROLL)
        def _(i):
            at = pl.ds(pl.multiple_of(i * tile, tile), tile)
            asked = qbuf[b, at, :]
            gate = mm_t(asked, w1)
            hidden = (gate * sigmoid(gate) * mm_t(asked, w3)).astype(bf16)
            obuf[b, at, :] = mm_t(hidden, w2).astype(bf16)

        pltpu.make_async_copy(obuf.at[b], out_hbm.at[b], store_sem.at[b]).start()

    prepare(0)
    for d in range(1, n):
        sq_copy(d).wait_recv()

    @pl.loop(0, total)
    def _(b):
        s = b // blocks
        g = b - s * blocks
        inner = (g + blocks - 1) // blocks
        entered = jnp.logical_and(jnp.logical_and(g == 0, s > 0), jnp.logical_not(first))

        @pl.when(g == 0)
        def _():
            for m in order:
                for d in around:
                    ent_copy(s, d, m).wait_recv()

        @pl.when(jnp.logical_and(jnp.logical_and(g == 0, s > 0), first))
        def _():
            wstate[...] = fw_in[...]
            mstate[...] = fm_in[...]

        @pl.when(entered)
        def _():
            for m in order:
                relay_copy(b - 1, s - 1, 0, m).wait_recv()
                wstate[m] = bank[total + s, m, mine, :].astype(f32)

        gradients(b, (total + s) * (1 - inner) + (b - 1) * inner)

        @pl.when(g > 0)
        def _():
            apply_fast(b - 1)

        @pl.when(entered)
        def _():
            m_copy(s - 1).wait_recv()
            mstate[...] = mrecv[s - 1].astype(f32)

        border = jnp.logical_and(g == blocks - 1, s < steps - 1)
        passing = jnp.logical_and(border, jnp.logical_not(last))
        square = sq[0, s, pl.ds(g, 1), :]
        for p in range(1, n):
            square = square + sq[p, s, pl.ds(g, 1), :]
        factor = lax.rsqrt(jnp.concatenate([square] * (head // LANES), axis=1))

        for m in order:
            for d in around:
                g_copy(b, d, m).wait_recv()
            update(b, m, factor)

            @pl.when(passing)
            def _():
                relay_copy(b, s, 0, m).start()

            for d in around:
                own_copy(b, d, m).start()

        @pl.when(passing)
        def _():
            msend[s] = mstate[...].astype(bf16)
            m_copy(s).start()

        for m in order:
            for d in around:
                g_copy(b, d, m).wait_send()

        @pl.when(b < total - 1)
        def _():
            prepare(b + 1)

        for m in order:
            for d in range(1, n):
                own_copy(b, d, m).wait_recv()

                @pl.when(passing)
                def _():
                    relay_copy(b, s, d, m).start()

        @pl.when(g == blocks - 1)
        def _():
            apply_fast(b)

        for m in order:
            for d in around:
                own_copy(b, d, m).wait_send()

        @pl.when(passing)
        def _():
            for m in order:
                for d in range(n):
                    relay_copy(b, s, d, m).wait_send()
            m_copy(s).wait_send()

    for d in around:
        sq_copy(d).wait_send()
        for m in order:
            ent_copy(0, d, m).wait_send()

    @pl.when(first)
    def _():
        for s in range(1, steps):
            for m in order:
                for d in around:
                    ent_copy(s, d, m).wait_send()

    for b in range(total):
        pltpu.make_async_copy(obuf.at[b], out_hbm.at[b], store_sem.at[b]).wait()


def apply_tiles(begin, stop, tile, weights, asked_ref, out_ref):
    half = asked_ref.shape[-1] // 2

    @pl.loop(begin, stop, unroll=min(UNROLL, stop - begin))
    def _(i):
        at = pl.ds(pl.multiple_of(i * tile, tile), tile)
        asked = asked_ref[at, :]
        parts = []
        for w13 in weights[:2]:
            both = mm_t(asked, w13)
            gate = both[:, :half]
            parts.append((gate * sigmoid(gate) * both[:, half:]).astype(bf16))
        out_ref[at, :] = mm_t(jnp.concatenate(parts, axis=1), weights[2]).astype(bf16)


def quad_kernel(
    segs, steps, blocks, tile,
    k_hbm, v_hbm, q_hbm, rates_hbm, w_hbm, m_hbm, fw_hbm, fm_hbm,
    obuf, usable, asked_last, w_out, m_out,
    kbuf, vbuf, qbuf, kt, scaled, scaled_t, hid, bgu,
    bank, gs, got, mid, wst, mst,
    w_in, m_in, fw_in, fm_in, rates, mx, mr, msend, mrecv, sq,
    load_sem, in_sem, st_s, st_r, en_s, en_r, rl_s, rl_r, mm_s, mm_r, mx_s, mx_r, qs, qr,
):
    total = steps * blocks
    n = 4
    rows, head = kbuf.shape[1], kbuf.shape[2]
    half = head // 2
    tiles = rows // tile
    seg = lax.axis_index("seg")
    tok = lax.axis_index("tok")
    inner = lax.rem(tok, 2)
    outer = tok // 2
    first = seg == 0
    last = seg == segs - 1
    peers = [flip(tok, d) for d in range(n)]

    def to_peer(d):
        return {"seg": seg, "tok": peers[d]}

    gather_to = (to_peer(1), to_peer(2))
    cross_to = (to_peer(2), to_peer(1))
    down = {"seg": lax.rem(seg + 1, segs), "tok": tok}
    up = {"seg": lax.rem(seg + segs - 1, segs), "tok": tok}

    def rcopy(src, dst, send, recv, device):
        return pltpu.make_async_remote_copy(
            src_ref=src, dst_ref=dst, send_sem=send, recv_sem=recv,
            device_id=device, device_id_type=MESH,
        )

    barrier = pltpu.get_barrier_semaphore()
    for d in range(1, n):
        pl.semaphore_signal(barrier, inc=1, device_id=to_peer(d), device_id_type=MESH)

    @pl.when(jnp.logical_not(last))
    def _():
        pl.semaphore_signal(barrier, inc=1, device_id=down, device_id_type=MESH)

    @pl.when(jnp.logical_not(first))
    def _():
        pl.semaphore_signal(barrier, inc=1, device_id=up, device_id_type=MESH)

    inputs = [
        pltpu.make_async_copy(src, dst, in_sem.at[j])
        for j, (src, dst) in enumerate((
            (w_hbm, w_in), (m_hbm, m_in), (rates_hbm, rates), (fw_hbm, fw_in), (fm_hbm, fm_in),
        ))
    ]
    early = [
        pltpu.make_async_copy(src.at[0], dst.at[0], load_sem.at[j])
        for j, (src, dst) in enumerate(((k_hbm, kbuf), (v_hbm, vbuf)))
    ]
    rest = pl.ds(1, total - 1)
    later = [
        pltpu.make_async_copy(k_hbm.at[rest], kbuf.at[rest], load_sem.at[2]),
        pltpu.make_async_copy(v_hbm.at[rest], vbuf.at[rest], load_sem.at[3]),
        pltpu.make_async_copy(q_hbm.at[pl.ds(0, total - 1)], qbuf, load_sem.at[4]),
        pltpu.make_async_copy(q_hbm.at[total - 1], asked_last, load_sem.at[5]),
    ]
    for copy in (*inputs[:3], *early):
        copy.start()

    def fill_bank(e, source):
        bank[e, outer, 0, inner] = source[0].astype(bf16)
        bank[e, outer, 1, inner] = source[2].astype(bf16)
        bank[e, 2, outer, inner] = source[1].astype(bf16)

    def entry_copy(s, j, d):
        e = total + s
        piece = bank.at[e, 2, outer, inner] if j else bank.at[e, outer, :, inner]
        return rcopy(piece, piece, en_s.at[d - 1, j], en_r.at[s, d - 1, j], to_peer(d))

    def start_entry(s):
        @pl.when(outer == 0)
        def _():
            for j in (0, 1):
                for d in (3, 1, 2):
                    entry_copy(s, j, d).start()

        @pl.when(outer == 1)
        def _():
            for j in (1, 0):
                for d in (3, 1, 2):
                    entry_copy(s, j, d).start()

    def arrive_entry(s, c):
        @pl.when(outer == c)
        def _():
            entry_copy(s, 0, 1).wait_recv()

        @pl.when(outer != c)
        def _():
            for d in (2, 3):
                entry_copy(s, 0, d).wait_recv()

    def moment_copies(s, targets):
        return [
            rcopy(mx.at[s], mr.at[s, tok], mx_s.at[d - 1], mx_r.at[s, d - 1], to_peer(d))
            for d in targets
        ]

    def passed_moments(s):
        strip = head // 8
        copies = []
        for d in (1, 2):
            piece = mr.at[s, peers[3 - d], :, pl.ds((d - 1) * strip, strip), :]
            copies.append(rcopy(piece, piece, mx_s.at[1 + d], mx_r.at[s, 1 + d], to_peer(d)))
        return copies

    def square_copies():
        return [
            rcopy(sq.at[tok], sq.at[tok], qs.at[d - 1], qr.at[d - 1], to_peer(d)) for d in (1, 2, 3)
        ]

    def start(copies):
        for copy in copies:
            copy.start()

    def arrive(copies):
        for copy in copies:
            copy.wait_recv()

    def take_weights(s, weights):
        e = total + s
        for item in range(3):
            wst[item] = bank[e, item].astype(f32)
        wst[outer, 0, inner] = weights[0]
        wst[outer, 1, inner] = weights[2]
        wst[2, outer, inner] = weights[1]

    def take_moments(s, moments):
        for o in range(2):
            for i in range(2):
                @pl.when(tok != 2 * o + i)
                def _():
                    mst[o, 0, i] = mr[s, 2 * o + i, 0].astype(f32)
                    mst[o, 1, i] = mr[s, 2 * o + i, 2].astype(f32)
                    mst[2, o, i] = mr[s, 2 * o + i, 1].astype(f32)
        mst[outer, 0, inner] = moments[0]
        mst[outer, 1, inner] = moments[2]
        mst[2, outer, inner] = moments[1]

    inputs[0].wait()
    fill_bank(total, w_in)
    neighbours = (seg + segs - 1) // segs + (2 * segs - 2 - seg) // segs
    pl.semaphore_wait(barrier, n - 1 + neighbours)
    start_entry(0)
    for copy in later:
        copy.start()
    for copy in inputs[3:]:
        copy.start()
    inputs[1].wait()
    mx[0] = m_in[...].astype(bf16)
    inputs[2].wait()
    for s in range(steps):
        drawn = rates[s]
        sums = jnp.sum(drawn * drawn, axis=1, keepdims=True)
        sq[tok, s] = jnp.broadcast_to(sums, (blocks, LANES))
    start(square_copies())

    def prepare_keys(b):
        kt[...] = kbuf[b].T

    def prepare_values(b):
        s = b // blocks
        row = jnp.broadcast_to(rates[s, pl.ds(b - s * blocks, 1), :], (LANES, rows))
        column = jnp.concatenate([row.T] * (head // LANES), axis=1)
        product = (column * vbuf[b].astype(f32)).astype(bf16)
        scaled[...] = product
        scaled_t[...] = product.T

    def pair_copy(b, stage, item, p):
        return rcopy(
            (gs, mid)[stage].at[b, item, p], got.at[b, stage, item, p],
            st_s.at[item, p], st_r.at[lax.rem(b, 2), stage, item, p], (gather_to, cross_to)[stage][p],
        )

    def relay_copy(b, s, item):
        return rcopy(
            bank.at[b, item], bank.at[total + s + 1, item],
            rl_s.at[s, item], rl_r.at[s, item], down,
        )

    def m_copy(s, item):
        return rcopy(msend.at[s, item], mrecv.at[s, item], mm_s.at[s, item], mm_r.at[s, item], down)

    def matrix(slot, item):
        return bank[slot, item].reshape(head, head)

    def flow(b, slot, c):
        w13 = matrix(slot, c)
        w2 = matrix(slot, 2)[:, c * half:(c + 1) * half]

        @pl.loop(0, tiles, unroll=UNROLL)
        def _(i):
            at = pl.ds(pl.multiple_of(i * tile, tile), tile)
            both = mm_t(kbuf[b, at, :], w13)
            back = mm(scaled[at, :], w2)
            gate, up_pre = both[:, :half], both[:, half:]
            sig = sigmoid(gate)
            act = gate * sig
            slope = sig + act * (1.0 - sig)
            hid[at, c * half:(c + 1) * half] = (act * up_pre).astype(bf16)
            bgu[c, at, :half] = (back * up_pre * slope).astype(bf16)
            bgu[c, at, half:] = (back * act).astype(bf16)

    def gradient(b, item):
        if item < 2:
            grad = mm(kt[...], bgu[item]).astype(bf16).T
        else:
            grad = mm(scaled_t[...], hid[...]).astype(bf16)
        gs[b, item] = grad.reshape(gs.shape[2:])

    def launch(b, item):
        for p in range(2):
            pair_copy(b, 0, item, p).start()

    def pair_sum(b, item):
        for p in range(2):
            pair_copy(b, 0, item, p).wait_recv()
            mid[b, item, p] = (gs[b, item, p].astype(f32) + got[b, 0, item, p].astype(f32)).astype(bf16)
            pair_copy(b, 0, item, p).wait_send()
            pair_copy(b, 1, item, p).start()

    def step_half(b, item, p, factor, grad):
        moment = momentum_decay * mst[item, p] - grad * factor
        weight = wst[item, p]
        stepped = weight - learn_rate * moment
        before = jnp.sum(weight * weight, axis=2, keepdims=True)
        after = jnp.sum(stepped * stepped, axis=2, keepdims=True)
        weight = stepped * jnp.sqrt(before / (after + epsilon))
        mst[item, p] = moment
        wst[item, p] = weight
        bank[b, item, p] = weight.astype(bf16)

    def update(b, item):
        s = b // blocks
        g = b - s * blocks
        square = sq[0, s, pl.ds(g, 1), :]
        for p in range(1, n):
            square = square + sq[p, s, pl.ds(g, 1), :]
        factor = lax.rsqrt(jnp.concatenate([square] * (head // LANES), axis=1))

        for p in range(2):
            pair_copy(b, 1, item, p).wait_recv()
            pair_copy(b, 1, item, p).wait_send()
            grad = mid[b, item, p].astype(f32) + got[b, 1, item, p].astype(f32)
            step_half(b, item, p, factor, grad)

    def apply_fast(b, begin, stop):
        apply_tiles(begin, stop, tile, [matrix(b, item) for item in range(3)], qbuf.at[b], obuf.at[b])

    early[0].wait()
    prepare_keys(0)
    early[1].wait()
    prepare_values(0)
    for j in range(2):
        entry_copy(0, j, 3).wait_send()
    start(moment_copies(0, (1, 2)))
    for copy in inputs[3:]:
        copy.wait()
    cut = (tiles + 1) // 2

    @pl.loop(0, total)
    def _(b):
        s = b // blocks
        g = b - s * blocks
        inside = (g + blocks - 1) // blocks
        slot = (total + s) * (1 - inside) + (b - 1) * inside
        entered = jnp.logical_and(jnp.logical_and(g == 0, s > 0), jnp.logical_not(first))
        renewed = jnp.logical_and(jnp.logical_and(g == 0, s > 0), first)
        border = jnp.logical_and(g == blocks - 1, s < steps - 1)
        passing = jnp.logical_and(border, jnp.logical_not(last))

        newly = jnp.logical_and(g == 0, jnp.logical_or(first, s == 0))

        @pl.when(newly)
        def _():
            for d in (1, 2, 3):
                entry_copy(s, 1, d).wait_recv()
            arrive_entry(s, 0)

        @pl.when(entered)
        def _():
            for item in (0, 2):
                relay_copy(b - 1, s - 1, item).wait_recv()

        flow(b, slot, 0)
        gradient(b, 0)
        launch(b, 0)

        @pl.when(g > 0)
        def _():
            update(b - 1, 1)

        @pl.when(newly)
        def _():
            arrive_entry(s, 1)

        @pl.when(entered)
        def _():
            relay_copy(b - 1, s - 1, 1).wait_recv()

        flow(b, slot, 1)
        gradient(b, 2)
        launch(b, 2)
        gradient(b, 1)
        launch(b, 1)

        @pl.when(b == 0)
        def _():
            for copy in later[:3]:
                copy.wait()

        @pl.when(b < total - 1)
        def _():
            prepare_keys(b + 1)

        @pl.when(b == 0)
        def _():
            arrive(moment_copies(0, (1, 2)))
            start(passed_moments(0))

        @pl.when(b > 0)
        def _():
            apply_fast(b - 1, 0, cut)

        pair_sum(b, 0)

        @pl.when(b > 0)
        def _():
            apply_fast(b - 1, cut, tiles)

        pair_sum(b, 2)

        @pl.when(b < total - 1)
        def _():
            prepare_values(b + 1)

        pair_sum(b, 1)

        for step in range(1, steps):
            @pl.when(jnp.logical_and(first, b == 0))
            def _():
                fill_bank(total + step, fw_in)
                for j in range(2):
                    for d in (1, 2) if step == 1 else (1, 2, 3):
                        entry_copy(step - 1, j, d).wait_send()
                start_entry(step)

            @pl.when(jnp.logical_and(first, b == step * blocks - 1))
            def _():
                sent = moment_copies(0, (1, 2)) + passed_moments(0)
                for copy in sent if step == 1 else moment_copies(step - 1, (1, 2, 3)):
                    copy.wait_send()
                mx[step] = fm_in[...].astype(bf16)
                start(moment_copies(step, (1, 2, 3)))

        @pl.when(b == 0)
        def _():
            arrive(square_copies())
            take_weights(0, w_in)
            arrive(passed_moments(0))
            take_moments(0, m_in)

        @pl.when(renewed)
        def _():
            take_weights(s, fw_in)
            arrive(moment_copies(s, (1, 2, 3)))
            take_moments(s, fm_in)

        @pl.when(entered)
        def _():
            for item in range(3):
                wst[item] = bank[total + s, item].astype(f32)
            for item in range(3):
                m_copy(s - 1, item).wait_recv()
                mst[item] = mrecv[s - 1, item].astype(f32)

        def finish(item):
            update(b, item)

            @pl.when(passing)
            def _():
                relay_copy(b, s, item).start()

        finish(0)

        finish(2)

        @pl.when(g == blocks - 1)
        def _():
            finish(1)

        @pl.when(passing)
        def _():
            for item in (0, 2, 1):
                msend[s, item] = mst[item].astype(bf16)
                m_copy(s, item).start()

    usable[...] = bank[total - 1]
    later[3].wait()
    for ref, state in ((w_out, wst), (m_out, mst)):
        ref[0] = state[outer, 0, inner]
        ref[2] = state[outer, 1, inner]
        ref[1] = state[2, outer, inner]

    def drain_entry(peers_left, sent):
        for j in range(2):
            for d in peers_left:
                entry_copy(0, j, d).wait_send()
        for copy in sent:
            copy.wait_send()

    @pl.when(first)
    def _():
        drain_entry((1, 2, 3), moment_copies(steps - 1, (1, 2, 3)))

    @pl.when(jnp.logical_not(first))
    def _():
        drain_entry((1, 2), moment_copies(0, (1, 2)) + passed_moments(0))

    for copy in square_copies():
        copy.wait_send()

    @pl.when(jnp.logical_not(last))
    def _():
        for s in range(steps - 1):
            for item in range(3):
                relay_copy(s * blocks + blocks - 1, s, item).wait_send()
                m_copy(s, item).wait_send()


def tail_kernel(
    tile, done, usable, asked, w_ready, m_ready, out_hbm, w_hbm, m_hbm, obuf, sem,
):
    count = done.shape[0]
    rows, head = asked.shape
    copies = [
        pltpu.make_async_copy(src, dst, sem.at[j])
        for j, (src, dst) in enumerate(
            [(w_ready, w_hbm), (m_ready, m_hbm)] + [(done.at[b], out_hbm.at[b]) for b in range(count)]
        )
    ]
    for copy in copies:
        copy.start()
    weights = [usable[item].reshape(head, head) for item in range(3)]
    for i in range(rows // tile):
        apply_tiles(i, i + 1, tile, weights, asked, obuf)
        at = pl.ds(i * tile, tile)
        copy = pltpu.make_async_copy(obuf.at[at], out_hbm.at[count, at], sem.at[count + 2 + i])
        copy.start()
        copies.append(copy)
    for copy in copies:
        copy.wait()


def quad_scratch(steps, blocks, rows, head):
    total = steps * blocks
    quarter = head // 4
    flat = (total, rows, head)
    whole = (2, 2, quarter, head)
    piece = (3, quarter, head)
    dma = pltpu.SemaphoreType.DMA
    vmem = pltpu.VMEM
    return [vmem(flat, bf16)] * 2 + [
        vmem((total - 1, rows, head), bf16),
        vmem((head, rows), bf16),
        vmem((rows, head), bf16),
        vmem((head, rows), bf16),
        vmem((rows, head), bf16),
        vmem((2, rows, head), bf16),
        vmem((total + steps, 3) + whole, bf16),
        vmem((total, 3) + whole, bf16),
        vmem((total, 2, 3) + whole, bf16),
        vmem((total, 3) + whole, bf16),
        vmem((3,) + whole, f32),
        vmem((3,) + whole, f32),
        vmem(piece, f32),
        vmem(piece, f32),
        vmem(piece, f32),
        vmem(piece, f32),
        vmem((steps, blocks, rows), f32),
        vmem((steps,) + piece, bf16),
        vmem((steps, 4) + piece, bf16),
        vmem((steps, 3) + whole, bf16),
        vmem((steps, 3) + whole, bf16),
        vmem((4, steps, blocks, LANES), f32),
        dma((6,)),
        dma((5,)),
        dma((3, 2)),
        dma((2, 2, 3, 2)),
        dma((3, 2)),
        dma((steps, 3, 2)),
        dma((steps - 1, 3)),
        dma((steps - 1, 3)),
        dma((steps - 1, 3)),
        dma((steps - 1, 3)),
        dma((4,)),
        dma((steps, 4)),
        dma((3,)),
        dma((3,)),
    ]


def body(n, segs, queries, keys, values, rates, weights, momenta, fresh_w, fresh_m):
    steps, _, blocks, rows, head = queries.shape
    total = steps * blocks
    width = head // n
    tile = 256 if rows % 256 == 0 else rows
    flat = (total, rows, head)
    piece = (3, width, head)
    hbm = pl.BlockSpec(memory_space=pl.ANY)
    vmem = pl.BlockSpec(memory_space=pltpu.VMEM)
    dma = pltpu.SemaphoreType.DMA
    big = (rows, head)
    turned = (head, rows)
    operands = (
        keys.reshape(flat), values.reshape(flat), queries.reshape(flat), rates[:, 0],
        jnp.swapaxes(weights[0], 1, 2), jnp.swapaxes(momenta[0], 1, 2),
        jnp.swapaxes(fresh_w, 1, 2), jnp.swapaxes(fresh_m, 1, 2),
    )
    results = (
        jax.ShapeDtypeStruct(flat, bf16),
        jax.ShapeDtypeStruct(piece, f32),
        jax.ShapeDtypeStruct(piece, f32),
    )
    if n == 4 and head % 256 == 0 and min(steps, blocks) > 1:
        ready = pl.pallas_call(
            functools.partial(quad_kernel, segs, steps, blocks, tile),
            out_shape=(
                jax.ShapeDtypeStruct((total - 1, rows, head), bf16),
                jax.ShapeDtypeStruct((3, 2, 2, head // 4, head), bf16),
                jax.ShapeDtypeStruct(big, bf16),
                *results[1:],
            ),
            in_specs=[pl.BlockSpec(memory_space=pltpu.HBM)] * 8,
            out_specs=(vmem,) * 5,
            scratch_shapes=quad_scratch(steps, blocks, rows, head),
            compiler_params=pltpu.CompilerParams(
                collective_id=0, has_side_effects=True, vmem_limit_bytes=QUAD_VMEM
            ),
        )(*(pltpu.with_memory_space_constraint(x, pltpu.HBM) for x in operands))
        outs = pl.pallas_call(
            functools.partial(tail_kernel, tile),
            out_shape=results,
            in_specs=[vmem] * 5,
            out_specs=(hbm,) * 3,
            scratch_shapes=[pltpu.VMEM(big, bf16), dma((total + 1 + rows // tile,))],
            compiler_params=pltpu.CompilerParams(vmem_limit_bytes=16 * 1024 * 1024),
        )(*ready)
    else:
        outs = pl.pallas_call(
            functools.partial(kernel, n, segs, steps, blocks, tile),
            out_shape=results,
            in_specs=[hbm, hbm, hbm, vmem, vmem, vmem, vmem, vmem],
            out_specs=(hbm, vmem, vmem),
            scratch_shapes=[pltpu.VMEM(flat, bf16)] * 4 + [
                pltpu.VMEM(turned, bf16),
                pltpu.VMEM(big, bf16),
                pltpu.VMEM(turned, bf16),
                pltpu.VMEM(big, bf16),
                pltpu.VMEM(big, bf16),
                pltpu.VMEM(big, bf16),
                pltpu.VMEM((3, head, head), bf16),
                pltpu.VMEM((total, n) + piece, bf16),
                pltpu.VMEM((total + steps, 3, head, head), bf16),
                pltpu.VMEM((steps,) + piece, bf16),
                pltpu.VMEM((steps,) + piece, bf16),
                pltpu.VMEM((n, steps, blocks, LANES), f32),
                dma((3, total)),
                dma((total,)),
                dma((total, n, 3)),
                dma((total, n, 3)),
                dma((total, n, 3)),
                dma((total, n, 3)),
                dma((steps, n, 3)),
                dma((steps, n, 3)),
                dma((steps,)),
                dma((steps,)),
                dma((n,)),
                dma((n,)),
        ],
            compiler_params=pltpu.CompilerParams(
                collective_id=0, has_side_effects=True, vmem_limit_bytes=60 * 1024 * 1024
            ),
        )(*operands)
    return (
        outs[0].reshape(queries.shape),
        jnp.swapaxes(outs[1], 1, 2)[None],
        jnp.swapaxes(outs[2], 1, 2)[None],
    )


def solution(mesh):
    n, segs = mesh.shape["tok"], mesh.shape["seg"]
    return jax.shard_map(
        functools.partial(body, n, segs),
        mesh=mesh,
        in_specs=(
            P(None, "seg", None, "tok", None),
            P(None, "seg", None, "tok", None),
            P(None, "seg", None, "tok", None),
            P(None, "seg", None, "tok"),
            P("seg", None, None, "tok"),
            P("seg", None, None, "tok"),
            P(None, None, "tok"),
            P(None, None, "tok"),
        ),
        out_specs=(
            P(None, "seg", None, "tok", None),
            P("seg", None, None, "tok"),
            P("seg", None, None, "tok"),
        ),
        check_vma=False,
    )
```

```python
import functools
import jax
import jax.numpy as jnp
from jax import lax
from jax.experimental import pallas as pl
from jax.experimental.pallas import tpu as pltpu
from jax.sharding import PartitionSpec as P

momentum_decay = 0.9
learn_rate = 0.05
epsilon = 1e-06
LANES = 128
UNROLL = 5
QUAD_VMEM = 40 * 1024 * 1024
MESH = pl.DeviceIdType.MESH
f32 = jnp.float32
bf16 = jnp.bfloat16


def flip(index, mask):
    out, bit = index, 1
    while bit <= mask:
        if mask & bit:
            out = out + bit * (1 - 2 * lax.rem(index // bit, 2))
        bit *= 2
    return out


def sigmoid(x):
    return 0.5 + 0.5 * jnp.tanh(0.5 * x)


def mm(a, b):
    return jnp.dot(a, b, preferred_element_type=f32)


def mm_t(a, b):
    return lax.dot_general(a, b, (((1,), (1,)), ((), ())), preferred_element_type=f32)


def kernel(
    n, segs, steps, blocks, tile,
    k_hbm, v_hbm, q_hbm, rates, w_in, m_in, fw_in, fm_in,
    out_hbm, wstate, mstate,
    kbuf, vbuf, qbuf, obuf, kt, scaled, scaled_t, hid, bgate, bup,
    gsend, grecv, bank, msend, mrecv, sq,
    load_sem, store_sem, gs_sem, gr_sem, os_sem, or_sem, es_sem, er_sem, ms_sem, mr_sem,
    qs_sem, qr_sem,
):
    total = steps * blocks
    rows, head = kbuf.shape[1], kbuf.shape[2]
    width = head // n
    tiles = rows // tile
    order = (1, 0, 2)
    around = tuple(range(n - 1, 0, -1))
    seg = lax.axis_index("seg")
    tok = lax.axis_index("tok")
    first = seg == 0
    last = seg == segs - 1
    peers = [flip(tok, d) for d in range(n)]

    def part(p):
        return pl.ds(pl.multiple_of(p * width, width), width)

    mine = part(tok)

    def to_peer(d):
        return {"seg": seg, "tok": peers[d]}

    down = {"seg": lax.rem(seg + 1, segs), "tok": tok}
    up = {"seg": lax.rem(seg + segs - 1, segs), "tok": tok}

    def rcopy(src, dst, send, recv, device):
        return pltpu.make_async_remote_copy(
            src_ref=src, dst_ref=dst, send_sem=send, recv_sem=recv,
            device_id=device, device_id_type=MESH,
        )

    loads = [[
        pltpu.make_async_copy(src.at[b], dst.at[b], load_sem.at[j, b])
        for b in range(total)
    ] for j, (src, dst) in enumerate(((k_hbm, kbuf), (v_hbm, vbuf), (q_hbm, qbuf)))]

    barrier = pltpu.get_barrier_semaphore()
    for d in range(1, n):
        pl.semaphore_signal(barrier, inc=1, device_id=to_peer(d), device_id_type=MESH)

    @pl.when(jnp.logical_not(last))
    def _():
        pl.semaphore_signal(barrier, inc=1, device_id=down, device_id_type=MESH)

    @pl.when(jnp.logical_not(first))
    def _():
        pl.semaphore_signal(barrier, inc=1, device_id=up, device_id_type=MESH)

    for b in range(total):
        loads[0][b].start()
        loads[1][b].start()
    for b in range(total):
        loads[2][b].start()

    wstate[...] = w_in[...]
    mstate[...] = m_in[...]
    for m in range(3):
        bank[total, m, mine, :] = w_in[m].astype(bf16)
    for s in range(steps):
        drawn = rates[s]
        sums = jnp.sum(drawn * drawn, axis=1, keepdims=True)
        sq[tok, s] = jnp.broadcast_to(sums, (blocks, LANES))

    @pl.when(first)
    def _():
        for s in range(1, steps):
            for m in range(3):
                bank[total + s, m, mine, :] = fw_in[m].astype(bf16)

    neighbours = (seg + segs - 1) // segs + (2 * segs - 2 - seg) // segs
    pl.semaphore_wait(barrier, n - 1 + neighbours)

    def ent_copy(s, d, m):
        place = bank.at[total + s, m, mine, :]
        return rcopy(place, place, es_sem.at[s, d, m], er_sem.at[s, d, m], to_peer(d))

    def sq_copy(d):
        return rcopy(sq.at[tok], sq.at[tok], qs_sem.at[d], qr_sem.at[d], to_peer(d))

    for m in order:
        for d in around:
            ent_copy(0, d, m).start()
    for d in around:
        sq_copy(d).start()

    @pl.when(first)
    def _():
        for s in range(1, steps):
            for m in order:
                for d in around:
                    ent_copy(s, d, m).start()

    def g_copy(b, d, m):
        return rcopy(
            gsend.at[m, part(peers[d]), :], grecv.at[b, d, m],
            gs_sem.at[b, d, m], gr_sem.at[b, d, m], to_peer(d),
        )

    def own_copy(b, d, m):
        place = bank.at[b, m, mine, :]
        return rcopy(place, place, os_sem.at[b, d, m], or_sem.at[b, d, m], to_peer(d))

    def relay_copy(b, s, d, m):
        piece = part(peers[d])
        return rcopy(
            bank.at[b, m, piece, :], bank.at[total + s + 1, m, piece, :],
            es_sem.at[s + 1, d, m], er_sem.at[s + 1, d, m], down,
        )

    def m_copy(s):
        return rcopy(msend.at[s], mrecv.at[s], ms_sem.at[s], mr_sem.at[s], down)

    def prepare(b):
        pltpu.make_async_copy(k_hbm.at[b], kbuf.at[b], load_sem.at[0, b]).wait()
        pltpu.make_async_copy(v_hbm.at[b], vbuf.at[b], load_sem.at[1, b]).wait()
        kt[...] = kbuf[b].T
        s = b // blocks
        row = jnp.broadcast_to(rates[s, pl.ds(b - s * blocks, 1), :], (LANES, rows))
        column = jnp.concatenate([row.T] * (head // LANES), axis=1)
        product = (column * vbuf[b].astype(f32)).astype(bf16)
        scaled[...] = product
        scaled_t[...] = product.T

    def gradients(b, slot):
        w1, w2, w3 = bank[slot, 0], bank[slot, 1], bank[slot, 2]

        @pl.loop(0, tiles, unroll=UNROLL)
        def _(i):
            at = pl.ds(pl.multiple_of(i * tile, tile), tile)
            keys = kbuf[b, at, :]
            back = mm(scaled[at, :], w2)
            gate = mm_t(keys, w1)
            up_pre = mm_t(keys, w3)
            sig = sigmoid(gate)
            act = gate * sig
            slope = sig + act * (1.0 - sig)
            hid[at, :] = (act * up_pre).astype(bf16)
            bgate[at, :] = (back * up_pre * slope).astype(bf16)
            bup[at, :] = (back * act).astype(bf16)

        for m in order:
            if m == 1:
                grad = mm(scaled_t[...], hid[...])
            else:
                grad = mm(kt[...], (bgate if m == 0 else bup)[...]).T
            gsend[m] = grad.astype(bf16)
            for d in around:
                g_copy(b, d, m).start()

    def update(b, m, factor):
        grad = gsend[m, mine, :].astype(f32)
        for d in range(1, n):
            grad = grad + grecv[b, d, m].astype(f32)
        moment = momentum_decay * mstate[m] - grad * factor
        weight = wstate[m]
        stepped = weight - learn_rate * moment
        before = jnp.sum(weight * weight, axis=1, keepdims=True)
        after = jnp.sum(stepped * stepped, axis=1, keepdims=True)
        weight = stepped * jnp.sqrt(before / (after + epsilon))
        mstate[m] = moment
        wstate[m] = weight
        bank[b, m, mine, :] = weight.astype(bf16)

    def apply_fast(b):
        pltpu.make_async_copy(q_hbm.at[b], qbuf.at[b], load_sem.at[2, b]).wait()
        w1, w2, w3 = bank[b, 0], bank[b, 1], bank[b, 2]

        @pl.loop(0, tiles, unroll=UNROLL)
        def _(i):
            at = pl.ds(pl.multiple_of(i * tile, tile), tile)
            asked = qbuf[b, at, :]
            gate = mm_t(asked, w1)
            hidden = (gate * sigmoid(gate) * mm_t(asked, w3)).astype(bf16)
            obuf[b, at, :] = mm_t(hidden, w2).astype(bf16)

        pltpu.make_async_copy(obuf.at[b], out_hbm.at[b], store_sem.at[b]).start()

    prepare(0)
    for d in range(1, n):
        sq_copy(d).wait_recv()

    @pl.loop(0, total)
    def _(b):
        s = b // blocks
        g = b - s * blocks
        inner = (g + blocks - 1) // blocks
        entered = jnp.logical_and(jnp.logical_and(g == 0, s > 0), jnp.logical_not(first))

        @pl.when(g == 0)
        def _():
            for m in order:
                for d in around:
                    ent_copy(s, d, m).wait_recv()

        @pl.when(jnp.logical_and(jnp.logical_and(g == 0, s > 0), first))
        def _():
            wstate[...] = fw_in[...]
            mstate[...] = fm_in[...]

        @pl.when(entered)
        def _():
            for m in order:
                relay_copy(b - 1, s - 1, 0, m).wait_recv()
                wstate[m] = bank[total + s, m, mine, :].astype(f32)

        gradients(b, (total + s) * (1 - inner) + (b - 1) * inner)

        @pl.when(g > 0)
        def _():
            apply_fast(b - 1)

        @pl.when(entered)
        def _():
            m_copy(s - 1).wait_recv()
            mstate[...] = mrecv[s - 1].astype(f32)

        border = jnp.logical_and(g == blocks - 1, s < steps - 1)
        passing = jnp.logical_and(border, jnp.logical_not(last))
        square = sq[0, s, pl.ds(g, 1), :]
        for p in range(1, n):
            square = square + sq[p, s, pl.ds(g, 1), :]
        factor = lax.rsqrt(jnp.concatenate([square] * (head // LANES), axis=1))

        for m in order:
            for d in around:
                g_copy(b, d, m).wait_recv()
            update(b, m, factor)

            @pl.when(passing)
            def _():
                relay_copy(b, s, 0, m).start()

            for d in around:
                own_copy(b, d, m).start()

        @pl.when(passing)
        def _():
            msend[s] = mstate[...].astype(bf16)
            m_copy(s).start()

        for m in order:
            for d in around:
                g_copy(b, d, m).wait_send()

        @pl.when(b < total - 1)
        def _():
            prepare(b + 1)

        for m in order:
            for d in range(1, n):
                own_copy(b, d, m).wait_recv()

                @pl.when(passing)
                def _():
                    relay_copy(b, s, d, m).start()

        @pl.when(g == blocks - 1)
        def _():
            apply_fast(b)

        for m in order:
            for d in around:
                own_copy(b, d, m).wait_send()

        @pl.when(passing)
        def _():
            for m in order:
                for d in range(n):
                    relay_copy(b, s, d, m).wait_send()
            m_copy(s).wait_send()

    for d in around:
        sq_copy(d).wait_send()
        for m in order:
            ent_copy(0, d, m).wait_send()

    @pl.when(first)
    def _():
        for s in range(1, steps):
            for m in order:
                for d in around:
                    ent_copy(s, d, m).wait_send()

    for b in range(total):
        pltpu.make_async_copy(obuf.at[b], out_hbm.at[b], store_sem.at[b]).wait()


def gated(asked, w13):
    both = mm_t(asked, w13)
    half = both.shape[1] // 2
    gate = both[:, :half]
    return (gate * sigmoid(gate) * both[:, half:]).astype(bf16)


def apply_tiles(begin, stop, tile, weights, asked_ref, out_ref):
    @pl.loop(begin, stop, unroll=min(UNROLL, stop - begin))
    def _(i):
        at = pl.ds(pl.multiple_of(i * tile, tile), tile)
        asked = asked_ref[at, :]
        parts = [gated(asked, w13) for w13 in weights[:2]]
        out_ref[at, :] = mm_t(jnp.concatenate(parts, axis=1), weights[2]).astype(bf16)


def quad_kernel(
    segs, steps, blocks, tile,
    k_hbm, v_hbm, q_hbm, rates_hbm, w_hbm, m_hbm, fw_hbm, fm_hbm,
    obuf, usable, asked_last, begun, w_out, m_out,
    kbuf, vbuf, qbuf, kt, scaled, scaled_t, hid, bgu,
    bank, gs, got, mid, wst, mst,
    w_in, m_in, fw_in, fm_in, rates, mx, mr, msend, mrecv, sq,
    load_sem, in_sem, st_s, st_r, en_s, en_r, rl_s, rl_r, mm_s, mm_r, mx_s, mx_r, qs, qr,
):
    total = steps * blocks
    n = 4
    rows, head = kbuf.shape[1], kbuf.shape[2]
    half = head // 2
    tiles = rows // tile
    seg = lax.axis_index("seg")
    tok = lax.axis_index("tok")
    inner = lax.rem(tok, 2)
    outer = tok // 2
    first = seg == 0
    last = seg == segs - 1
    peers = [flip(tok, d) for d in range(n)]

    def to_peer(d):
        return {"seg": seg, "tok": peers[d]}

    gather_to = (to_peer(1), to_peer(2))
    cross_to = (to_peer(2), to_peer(1))
    down = {"seg": lax.rem(seg + 1, segs), "tok": tok}
    up = {"seg": lax.rem(seg + segs - 1, segs), "tok": tok}

    def rcopy(src, dst, send, recv, device):
        return pltpu.make_async_remote_copy(
            src_ref=src, dst_ref=dst, send_sem=send, recv_sem=recv,
            device_id=device, device_id_type=MESH,
        )

    barrier = pltpu.get_barrier_semaphore()
    for d in range(1, n):
        pl.semaphore_signal(barrier, inc=1, device_id=to_peer(d), device_id_type=MESH)

    @pl.when(jnp.logical_not(last))
    def _():
        pl.semaphore_signal(barrier, inc=1, device_id=down, device_id_type=MESH)

    @pl.when(jnp.logical_not(first))
    def _():
        pl.semaphore_signal(barrier, inc=1, device_id=up, device_id_type=MESH)

    inputs = [
        pltpu.make_async_copy(src, dst, in_sem.at[j])
        for j, (src, dst) in enumerate((
            (w_hbm, w_in), (m_hbm, m_in), (rates_hbm, rates), (fw_hbm, fw_in), (fm_hbm, fm_in),
        ))
    ]
    early = [
        pltpu.make_async_copy(src.at[0], dst.at[0], load_sem.at[j])
        for j, (src, dst) in enumerate(((k_hbm, kbuf), (v_hbm, vbuf)))
    ]
    rest = pl.ds(1, total - 1)
    later = [
        pltpu.make_async_copy(k_hbm.at[rest], kbuf.at[rest], load_sem.at[2]),
        pltpu.make_async_copy(v_hbm.at[rest], vbuf.at[rest], load_sem.at[3]),
        pltpu.make_async_copy(q_hbm.at[pl.ds(0, total - 1)], qbuf, load_sem.at[4]),
        pltpu.make_async_copy(q_hbm.at[total - 1], asked_last, load_sem.at[5]),
    ]
    for copy in (*inputs[:3], *early):
        copy.start()

    def fill_bank(e, source):
        bank[e, outer, 0, inner] = source[0].astype(bf16)
        bank[e, outer, 1, inner] = source[2].astype(bf16)
        bank[e, 2, outer, inner] = source[1].astype(bf16)

    def entry_copy(s, j, d):
        e = total + s
        piece = bank.at[e, 2, outer, inner] if j else bank.at[e, outer, :, inner]
        return rcopy(piece, piece, en_s.at[d - 1, j], en_r.at[s, d - 1, j], to_peer(d))

    def start_entry(s):
        @pl.when(outer == 0)
        def _():
            for j in (0, 1):
                for d in (3, 1, 2):
                    entry_copy(s, j, d).start()

        @pl.when(outer == 1)
        def _():
            for j in (1, 0):
                for d in (3, 1, 2):
                    entry_copy(s, j, d).start()

    def arrive_entry(s, c):
        @pl.when(outer == c)
        def _():
            entry_copy(s, 0, 1).wait_recv()

        @pl.when(outer != c)
        def _():
            for d in (2, 3):
                entry_copy(s, 0, d).wait_recv()

    def moment_copies(s, targets):
        return [
            rcopy(mx.at[s], mr.at[s, tok], mx_s.at[d - 1], mx_r.at[s, d - 1], to_peer(d))
            for d in targets
        ]

    def passed_moments(s):
        strip = head // 8
        copies = []
        for d in (1, 2):
            piece = mr.at[s, peers[3 - d], :, pl.ds((d - 1) * strip, strip), :]
            copies.append(rcopy(piece, piece, mx_s.at[1 + d], mx_r.at[s, 1 + d], to_peer(d)))
        return copies

    def square_copies():
        return [
            rcopy(sq.at[tok], sq.at[tok], qs.at[d - 1], qr.at[d - 1], to_peer(d)) for d in (1, 2, 3)
        ]

    def start(copies):
        for copy in copies:
            copy.start()

    def arrive(copies):
        for copy in copies:
            copy.wait_recv()

    def take_weights(s, weights):
        e = total + s
        for item in range(3):
            wst[item] = bank[e, item].astype(f32)
        wst[outer, 0, inner] = weights[0]
        wst[outer, 1, inner] = weights[2]
        wst[2, outer, inner] = weights[1]

    def take_moments(s, moments):
        for o in range(2):
            for i in range(2):
                @pl.when(tok != 2 * o + i)
                def _():
                    mst[o, 0, i] = mr[s, 2 * o + i, 0].astype(f32)
                    mst[o, 1, i] = mr[s, 2 * o + i, 2].astype(f32)
                    mst[2, o, i] = mr[s, 2 * o + i, 1].astype(f32)
        mst[outer, 0, inner] = moments[0]
        mst[outer, 1, inner] = moments[2]
        mst[2, outer, inner] = moments[1]

    inputs[0].wait()
    fill_bank(total, w_in)
    neighbours = (seg + segs - 1) // segs + (2 * segs - 2 - seg) // segs
    pl.semaphore_wait(barrier, n - 1 + neighbours)
    start_entry(0)
    for copy in later:
        copy.start()
    for copy in inputs[3:]:
        copy.start()
    inputs[1].wait()
    mx[0] = m_in[...].astype(bf16)
    inputs[2].wait()
    for s in range(steps):
        drawn = rates[s]
        sums = jnp.sum(drawn * drawn, axis=1, keepdims=True)
        sq[tok, s] = jnp.broadcast_to(sums, (blocks, LANES))
    start(square_copies())

    def prepare_keys(b):
        kt[...] = kbuf[b].T

    def prepare_values(b):
        s = b // blocks
        row = jnp.broadcast_to(rates[s, pl.ds(b - s * blocks, 1), :], (LANES, rows))
        column = jnp.concatenate([row.T] * (head // LANES), axis=1)
        product = (column * vbuf[b].astype(f32)).astype(bf16)
        scaled[...] = product
        scaled_t[...] = product.T

    def pair_copy(b, stage, item, p):
        return rcopy(
            (gs, mid)[stage].at[b, item, p], got.at[b, stage, item, p],
            st_s.at[item, p], st_r.at[lax.rem(b, 2), stage, item, p], (gather_to, cross_to)[stage][p],
        )

    def relay_copy(b, s, item):
        return rcopy(
            bank.at[b, item], bank.at[total + s + 1, item],
            rl_s.at[s, item], rl_r.at[s, item], down,
        )

    def m_copy(s, item):
        return rcopy(msend.at[s, item], mrecv.at[s, item], mm_s.at[s, item], mm_r.at[s, item], down)

    def matrix(slot, item):
        return bank[slot, item].reshape(head, head)

    def flow(b, slot, c):
        w13 = matrix(slot, c)
        w2 = matrix(slot, 2)[:, c * half:(c + 1) * half]

        @pl.loop(0, tiles, unroll=UNROLL)
        def _(i):
            at = pl.ds(pl.multiple_of(i * tile, tile), tile)
            both = mm_t(kbuf[b, at, :], w13)
            back = mm(scaled[at, :], w2)
            gate, up_pre = both[:, :half], both[:, half:]
            sig = sigmoid(gate)
            act = gate * sig
            slope = sig + act * (1.0 - sig)
            hid[at, c * half:(c + 1) * half] = (act * up_pre).astype(bf16)
            bgu[c, at, :half] = (back * up_pre * slope).astype(bf16)
            bgu[c, at, half:] = (back * act).astype(bf16)

    def gradient(b, item):
        if item < 2:
            grad = mm(kt[...], bgu[item]).astype(bf16).T
        else:
            grad = mm(scaled_t[...], hid[...]).astype(bf16)
        gs[b, item] = grad.reshape(gs.shape[2:])

    def launch(b, item):
        for p in range(2):
            pair_copy(b, 0, item, p).start()

    def pair_sum(b, item):
        for p in range(2):
            pair_copy(b, 0, item, p).wait_recv()
            mid[b, item, p] = (gs[b, item, p].astype(f32) + got[b, 0, item, p].astype(f32)).astype(bf16)
            pair_copy(b, 0, item, p).wait_send()
            pair_copy(b, 1, item, p).start()

    def step_half(b, item, p, factor, grad):
        moment = momentum_decay * mst[item, p] - grad * factor
        weight = wst[item, p]
        stepped = weight - learn_rate * moment
        before = jnp.sum(weight * weight, axis=2, keepdims=True)
        after = jnp.sum(stepped * stepped, axis=2, keepdims=True)
        weight = stepped * jnp.sqrt(before / (after + epsilon))
        mst[item, p] = moment
        wst[item, p] = weight
        bank[b, item, p] = weight.astype(bf16)

    def update(b, item):
        s = b // blocks
        g = b - s * blocks
        square = sq[0, s, pl.ds(g, 1), :]
        for p in range(1, n):
            square = square + sq[p, s, pl.ds(g, 1), :]
        factor = lax.rsqrt(jnp.concatenate([square] * (head // LANES), axis=1))

        for p in range(2):
            pair_copy(b, 1, item, p).wait_recv()
            pair_copy(b, 1, item, p).wait_send()
            grad = mid[b, item, p].astype(f32) + got[b, 1, item, p].astype(f32)
            step_half(b, item, p, factor, grad)

    def apply_fast(b, begin, stop):
        apply_tiles(begin, stop, tile, [matrix(b, item) for item in range(3)], qbuf.at[b], obuf.at[b])

    early[0].wait()
    prepare_keys(0)
    early[1].wait()
    prepare_values(0)
    for j in range(2):
        entry_copy(0, j, 3).wait_send()
    start(moment_copies(0, (1, 2)))
    for copy in inputs[3:]:
        copy.wait()
    cut = (tiles + 1) // 2

    @pl.loop(0, total)
    def _(b):
        s = b // blocks
        g = b - s * blocks
        inside = (g + blocks - 1) // blocks
        slot = (total + s) * (1 - inside) + (b - 1) * inside
        entered = jnp.logical_and(jnp.logical_and(g == 0, s > 0), jnp.logical_not(first))
        renewed = jnp.logical_and(jnp.logical_and(g == 0, s > 0), first)
        border = jnp.logical_and(g == blocks - 1, s < steps - 1)
        passing = jnp.logical_and(border, jnp.logical_not(last))

        newly = jnp.logical_and(g == 0, jnp.logical_or(first, s == 0))

        @pl.when(newly)
        def _():
            for d in (1, 2, 3):
                entry_copy(s, 1, d).wait_recv()
            arrive_entry(s, 0)

        @pl.when(entered)
        def _():
            for item in (0, 2):
                relay_copy(b - 1, s - 1, item).wait_recv()

        flow(b, slot, 0)
        gradient(b, 0)
        launch(b, 0)

        @pl.when(g > 0)
        def _():
            update(b - 1, 1)

        @pl.when(newly)
        def _():
            arrive_entry(s, 1)

        @pl.when(entered)
        def _():
            relay_copy(b - 1, s - 1, 1).wait_recv()

        flow(b, slot, 1)
        gradient(b, 2)
        launch(b, 2)
        gradient(b, 1)
        launch(b, 1)

        @pl.when(b == 0)
        def _():
            for copy in later[:3]:
                copy.wait()

        @pl.when(b < total - 1)
        def _():
            prepare_keys(b + 1)

        @pl.when(b == 0)
        def _():
            arrive(moment_copies(0, (1, 2)))
            start(passed_moments(0))

        @pl.when(b > 0)
        def _():
            apply_fast(b - 1, 0, cut)

        pair_sum(b, 0)

        @pl.when(b > 0)
        def _():
            apply_fast(b - 1, cut, tiles)

        pair_sum(b, 2)

        @pl.when(b < total - 1)
        def _():
            prepare_values(b + 1)

        pair_sum(b, 1)

        for step in range(1, steps):
            @pl.when(jnp.logical_and(first, b == 0))
            def _():
                fill_bank(total + step, fw_in)
                for j in range(2):
                    for d in (1, 2) if step == 1 else (1, 2, 3):
                        entry_copy(step - 1, j, d).wait_send()
                start_entry(step)

            @pl.when(jnp.logical_and(first, b == step * blocks - 1))
            def _():
                sent = moment_copies(0, (1, 2)) + passed_moments(0)
                for copy in sent if step == 1 else moment_copies(step - 1, (1, 2, 3)):
                    copy.wait_send()
                mx[step] = fm_in[...].astype(bf16)
                start(moment_copies(step, (1, 2, 3)))

        @pl.when(b == 0)
        def _():
            arrive(square_copies())
            take_weights(0, w_in)
            arrive(passed_moments(0))
            take_moments(0, m_in)

        @pl.when(renewed)
        def _():
            take_weights(s, fw_in)
            arrive(moment_copies(s, (1, 2, 3)))
            take_moments(s, fm_in)

        @pl.when(entered)
        def _():
            for item in range(3):
                wst[item] = bank[total + s, item].astype(f32)
            for item in range(3):
                m_copy(s - 1, item).wait_recv()
                mst[item] = mrecv[s - 1, item].astype(f32)

        def finish(item):
            update(b, item)

            @pl.when(passing)
            def _():
                relay_copy(b, s, item).start()

        finish(0)

        @pl.when(b == total - 1)
        def _():
            later[3].wait()
            w13 = matrix(b, 0)

            @pl.loop(0, tiles, unroll=UNROLL)
            def _(i):
                at = pl.ds(pl.multiple_of(i * tile, tile), tile)
                begun[at, :] = gated(asked_last[at, :], w13)


        finish(2)

        @pl.when(g == blocks - 1)
        def _():
            finish(1)

        @pl.when(passing)
        def _():
            for item in (0, 2, 1):
                msend[s, item] = mst[item].astype(bf16)
                m_copy(s, item).start()

    usable[...] = bank[total - 1]
    for ref, state in ((w_out, wst), (m_out, mst)):
        ref[0] = state[outer, 0, inner]
        ref[2] = state[outer, 1, inner]
        ref[1] = state[2, outer, inner]

    def drain_entry(peers_left, sent):
        for j in range(2):
            for d in peers_left:
                entry_copy(0, j, d).wait_send()
        for copy in sent:
            copy.wait_send()

    @pl.when(first)
    def _():
        drain_entry((1, 2, 3), moment_copies(steps - 1, (1, 2, 3)))

    @pl.when(jnp.logical_not(first))
    def _():
        drain_entry((1, 2), moment_copies(0, (1, 2)) + passed_moments(0))

    for copy in square_copies():
        copy.wait_send()

    @pl.when(jnp.logical_not(last))
    def _():
        for s in range(steps - 1):
            for item in range(3):
                relay_copy(s * blocks + blocks - 1, s, item).wait_send()
                m_copy(s, item).wait_send()


def tail_kernel(
    tile, done, usable, asked, begun, w_ready, m_ready, out_hbm, w_hbm, m_hbm, obuf, sem,
):
    count = done.shape[0]
    rows, head = asked.shape
    copies = [
        pltpu.make_async_copy(src, dst, sem.at[j])
        for j, (src, dst) in enumerate(
            [(w_ready, w_hbm), (m_ready, m_hbm)] + [(done.at[b], out_hbm.at[b]) for b in range(count)]
        )
    ]
    for copy in copies:
        copy.start()
    weights = [usable[item].reshape(head, head) for item in range(3)]
    for i in range(rows // tile):
        at = pl.ds(i * tile, tile)
        hidden = jnp.concatenate([begun[at, :], gated(asked[at, :], weights[1])], axis=1)
        obuf[at, :] = mm_t(hidden, weights[2]).astype(bf16)
        copy = pltpu.make_async_copy(obuf.at[at], out_hbm.at[count, at], sem.at[count + 2 + i])
        copy.start()
        copies.append(copy)
    for copy in copies:
        copy.wait()


def quad_scratch(steps, blocks, rows, head):
    total = steps * blocks
    quarter = head // 4
    flat = (total, rows, head)
    whole = (2, 2, quarter, head)
    piece = (3, quarter, head)
    dma = pltpu.SemaphoreType.DMA
    vmem = pltpu.VMEM
    return [vmem(flat, bf16)] * 2 + [
        vmem((total - 1, rows, head), bf16),
        vmem((head, rows), bf16),
        vmem((rows, head), bf16),
        vmem((head, rows), bf16),
        vmem((rows, head), bf16),
        vmem((2, rows, head), bf16),
        vmem((total + steps, 3) + whole, bf16),
        vmem((total, 3) + whole, bf16),
        vmem((total, 2, 3) + whole, bf16),
        vmem((total, 3) + whole, bf16),
        vmem((3,) + whole, f32),
        vmem((3,) + whole, f32),
        vmem(piece, f32),
        vmem(piece, f32),
        vmem(piece, f32),
        vmem(piece, f32),
        vmem((steps, blocks, rows), f32),
        vmem((steps,) + piece, bf16),
        vmem((steps, 4) + piece, bf16),
        vmem((steps, 3) + whole, bf16),
        vmem((steps, 3) + whole, bf16),
        vmem((4, steps, blocks, LANES), f32),
        dma((6,)),
        dma((5,)),
        dma((3, 2)),
        dma((2, 2, 3, 2)),
        dma((3, 2)),
        dma((steps, 3, 2)),
        dma((steps - 1, 3)),
        dma((steps - 1, 3)),
        dma((steps - 1, 3)),
        dma((steps - 1, 3)),
        dma((4,)),
        dma((steps, 4)),
        dma((3,)),
        dma((3,)),
    ]


def body(n, segs, queries, keys, values, rates, weights, momenta, fresh_w, fresh_m):
    steps, _, blocks, rows, head = queries.shape
    total = steps * blocks
    width = head // n
    tile = 256 if rows % 256 == 0 else rows
    flat = (total, rows, head)
    piece = (3, width, head)
    hbm = pl.BlockSpec(memory_space=pl.ANY)
    vmem = pl.BlockSpec(memory_space=pltpu.VMEM)
    dma = pltpu.SemaphoreType.DMA
    big = (rows, head)
    turned = (head, rows)
    operands = (
        keys.reshape(flat), values.reshape(flat), queries.reshape(flat), rates[:, 0],
        jnp.swapaxes(weights[0], 1, 2), jnp.swapaxes(momenta[0], 1, 2),
        jnp.swapaxes(fresh_w, 1, 2), jnp.swapaxes(fresh_m, 1, 2),
    )
    results = (
        jax.ShapeDtypeStruct(flat, bf16),
        jax.ShapeDtypeStruct(piece, f32),
        jax.ShapeDtypeStruct(piece, f32),
    )
    if n == 4 and head % 256 == 0 and min(steps, blocks) > 1:
        ready = pl.pallas_call(
            functools.partial(quad_kernel, segs, steps, blocks, tile),
            out_shape=(
                jax.ShapeDtypeStruct((total - 1, rows, head), bf16),
                jax.ShapeDtypeStruct((3, 2, 2, head // 4, head), bf16),
                jax.ShapeDtypeStruct(big, bf16),
                jax.ShapeDtypeStruct((rows, head // 2), bf16),
                *results[1:],
            ),
            in_specs=[pl.BlockSpec(memory_space=pltpu.HBM)] * 8,
            out_specs=(vmem,) * 6,
            scratch_shapes=quad_scratch(steps, blocks, rows, head),
            compiler_params=pltpu.CompilerParams(
                collective_id=0, has_side_effects=True, vmem_limit_bytes=QUAD_VMEM
            ),
        )(*(pltpu.with_memory_space_constraint(x, pltpu.HBM) for x in operands))
        outs = pl.pallas_call(
            functools.partial(tail_kernel, tile),
            out_shape=results,
            in_specs=[vmem] * 6,
            out_specs=(hbm,) * 3,
            scratch_shapes=[pltpu.VMEM(big, bf16), dma((total + 1 + rows // tile,))],
            compiler_params=pltpu.CompilerParams(vmem_limit_bytes=16 * 1024 * 1024),
        )(*ready)
    else:
        outs = pl.pallas_call(
            functools.partial(kernel, n, segs, steps, blocks, tile),
            out_shape=results,
            in_specs=[hbm, hbm, hbm, vmem, vmem, vmem, vmem, vmem],
            out_specs=(hbm, vmem, vmem),
            scratch_shapes=[pltpu.VMEM(flat, bf16)] * 4 + [
                pltpu.VMEM(turned, bf16),
                pltpu.VMEM(big, bf16),
                pltpu.VMEM(turned, bf16),
                pltpu.VMEM(big, bf16),
                pltpu.VMEM(big, bf16),
                pltpu.VMEM(big, bf16),
                pltpu.VMEM((3, head, head), bf16),
                pltpu.VMEM((total, n) + piece, bf16),
                pltpu.VMEM((total + steps, 3, head, head), bf16),
                pltpu.VMEM((steps,) + piece, bf16),
                pltpu.VMEM((steps,) + piece, bf16),
                pltpu.VMEM((n, steps, blocks, LANES), f32),
                dma((3, total)),
                dma((total,)),
                dma((total, n, 3)),
                dma((total, n, 3)),
                dma((total, n, 3)),
                dma((total, n, 3)),
                dma((steps, n, 3)),
                dma((steps, n, 3)),
                dma((steps,)),
                dma((steps,)),
                dma((n,)),
                dma((n,)),
        ],
            compiler_params=pltpu.CompilerParams(
                collective_id=0, has_side_effects=True, vmem_limit_bytes=60 * 1024 * 1024
            ),
        )(*operands)
    return (
        outs[0].reshape(queries.shape),
        jnp.swapaxes(outs[1], 1, 2)[None],
        jnp.swapaxes(outs[2], 1, 2)[None],
    )


def solution(mesh):
    n, segs = mesh.shape["tok"], mesh.shape["seg"]
    return jax.shard_map(
        functools.partial(body, n, segs),
        mesh=mesh,
        in_specs=(
            P(None, "seg", None, "tok", None),
            P(None, "seg", None, "tok", None),
            P(None, "seg", None, "tok", None),
            P(None, "seg", None, "tok"),
            P("seg", None, None, "tok"),
            P("seg", None, None, "tok"),
            P(None, None, "tok"),
            P(None, None, "tok"),
        ),
        out_specs=(
            P(None, "seg", None, "tok", None),
            P("seg", None, None, "tok"),
            P("seg", None, None, "tok"),
        ),
        check_vma=False,
    )
```

```python
import functools
import jax
import jax.numpy as jnp
from jax import lax
from jax.experimental import pallas as pl
from jax.experimental.pallas import tpu as pltpu
from jax.sharding import PartitionSpec as P

momentum_decay = 0.9
learn_rate = 0.05
epsilon = 1e-06
LANES = 128
UNROLL = 5
QUAD_VMEM = 40 * 1024 * 1024
MESH = pl.DeviceIdType.MESH
f32 = jnp.float32
bf16 = jnp.bfloat16


def flip(index, mask):
    out, bit = index, 1
    while bit <= mask:
        if mask & bit:
            out = out + bit * (1 - 2 * lax.rem(index // bit, 2))
        bit *= 2
    return out


def sigmoid(x):
    return 0.5 + 0.5 * jnp.tanh(0.5 * x)


def mm(a, b):
    return jnp.dot(a, b, preferred_element_type=f32)


def mm_t(a, b):
    return lax.dot_general(a, b, (((1,), (1,)), ((), ())), preferred_element_type=f32)


def kernel(
    n, segs, steps, blocks, tile,
    k_hbm, v_hbm, q_hbm, rates, w_in, m_in, fw_in, fm_in,
    out_hbm, wstate, mstate,
    kbuf, vbuf, qbuf, obuf, kt, scaled, scaled_t, hid, bgate, bup,
    gsend, grecv, bank, msend, mrecv, sq,
    load_sem, store_sem, gs_sem, gr_sem, os_sem, or_sem, es_sem, er_sem, ms_sem, mr_sem,
    qs_sem, qr_sem,
):
    total = steps * blocks
    rows, head = kbuf.shape[1], kbuf.shape[2]
    width = head // n
    tiles = rows // tile
    order = (1, 0, 2)
    around = tuple(range(n - 1, 0, -1))
    seg = lax.axis_index("seg")
    tok = lax.axis_index("tok")
    first = seg == 0
    last = seg == segs - 1
    peers = [flip(tok, d) for d in range(n)]

    def part(p):
        return pl.ds(pl.multiple_of(p * width, width), width)

    mine = part(tok)

    def to_peer(d):
        return {"seg": seg, "tok": peers[d]}

    down = {"seg": lax.rem(seg + 1, segs), "tok": tok}
    up = {"seg": lax.rem(seg + segs - 1, segs), "tok": tok}

    def rcopy(src, dst, send, recv, device):
        return pltpu.make_async_remote_copy(
            src_ref=src, dst_ref=dst, send_sem=send, recv_sem=recv,
            device_id=device, device_id_type=MESH,
        )

    loads = [[
        pltpu.make_async_copy(src.at[b], dst.at[b], load_sem.at[j, b])
        for b in range(total)
    ] for j, (src, dst) in enumerate(((k_hbm, kbuf), (v_hbm, vbuf), (q_hbm, qbuf)))]

    barrier = pltpu.get_barrier_semaphore()
    for d in range(1, n):
        pl.semaphore_signal(barrier, inc=1, device_id=to_peer(d), device_id_type=MESH)

    @pl.when(jnp.logical_not(last))
    def _():
        pl.semaphore_signal(barrier, inc=1, device_id=down, device_id_type=MESH)

    @pl.when(jnp.logical_not(first))
    def _():
        pl.semaphore_signal(barrier, inc=1, device_id=up, device_id_type=MESH)

    for b in range(total):
        loads[0][b].start()
        loads[1][b].start()
    for b in range(total):
        loads[2][b].start()

    wstate[...] = w_in[...]
    mstate[...] = m_in[...]
    for m in range(3):
        bank[total, m, mine, :] = w_in[m].astype(bf16)
    for s in range(steps):
        drawn = rates[s]
        sums = jnp.sum(drawn * drawn, axis=1, keepdims=True)
        sq[tok, s] = jnp.broadcast_to(sums, (blocks, LANES))

    @pl.when(first)
    def _():
        for s in range(1, steps):
            for m in range(3):
                bank[total + s, m, mine, :] = fw_in[m].astype(bf16)

    neighbours = (seg + segs - 1) // segs + (2 * segs - 2 - seg) // segs
    pl.semaphore_wait(barrier, n - 1 + neighbours)

    def ent_copy(s, d, m):
        place = bank.at[total + s, m, mine, :]
        return rcopy(place, place, es_sem.at[s, d, m], er_sem.at[s, d, m], to_peer(d))

    def sq_copy(d):
        return rcopy(sq.at[tok], sq.at[tok], qs_sem.at[d], qr_sem.at[d], to_peer(d))

    for m in order:
        for d in around:
            ent_copy(0, d, m).start()
    for d in around:
        sq_copy(d).start()

    @pl.when(first)
    def _():
        for s in range(1, steps):
            for m in order:
                for d in around:
                    ent_copy(s, d, m).start()

    def g_copy(b, d, m):
        return rcopy(
            gsend.at[m, part(peers[d]), :], grecv.at[b, d, m],
            gs_sem.at[b, d, m], gr_sem.at[b, d, m], to_peer(d),
        )

    def own_copy(b, d, m):
        place = bank.at[b, m, mine, :]
        return rcopy(place, place, os_sem.at[b, d, m], or_sem.at[b, d, m], to_peer(d))

    def relay_copy(b, s, d, m):
        piece = part(peers[d])
        return rcopy(
            bank.at[b, m, piece, :], bank.at[total + s + 1, m, piece, :],
            es_sem.at[s + 1, d, m], er_sem.at[s + 1, d, m], down,
        )

    def m_copy(s):
        return rcopy(msend.at[s], mrecv.at[s], ms_sem.at[s], mr_sem.at[s], down)

    def prepare(b):
        pltpu.make_async_copy(k_hbm.at[b], kbuf.at[b], load_sem.at[0, b]).wait()
        pltpu.make_async_copy(v_hbm.at[b], vbuf.at[b], load_sem.at[1, b]).wait()
        kt[...] = kbuf[b].T
        s = b // blocks
        row = jnp.broadcast_to(rates[s, pl.ds(b - s * blocks, 1), :], (LANES, rows))
        column = jnp.concatenate([row.T] * (head // LANES), axis=1)
        product = (column * vbuf[b].astype(f32)).astype(bf16)
        scaled[...] = product
        scaled_t[...] = product.T

    def gradients(b, slot):
        w1, w2, w3 = bank[slot, 0], bank[slot, 1], bank[slot, 2]

        @pl.loop(0, tiles, unroll=UNROLL)
        def _(i):
            at = pl.ds(pl.multiple_of(i * tile, tile), tile)
            keys = kbuf[b, at, :]
            back = mm(scaled[at, :], w2)
            gate = mm_t(keys, w1)
            up_pre = mm_t(keys, w3)
            sig = sigmoid(gate)
            act = gate * sig
            slope = sig + act * (1.0 - sig)
            hid[at, :] = (act * up_pre).astype(bf16)
            bgate[at, :] = (back * up_pre * slope).astype(bf16)
            bup[at, :] = (back * act).astype(bf16)

        for m in order:
            if m == 1:
                grad = mm(scaled_t[...], hid[...])
            else:
                grad = mm(kt[...], (bgate if m == 0 else bup)[...]).T
            gsend[m] = grad.astype(bf16)
            for d in around:
                g_copy(b, d, m).start()

    def update(b, m, factor):
        grad = gsend[m, mine, :].astype(f32)
        for d in range(1, n):
            grad = grad + grecv[b, d, m].astype(f32)
        moment = momentum_decay * mstate[m] - grad * factor
        weight = wstate[m]
        stepped = weight - learn_rate * moment
        before = jnp.sum(weight * weight, axis=1, keepdims=True)
        after = jnp.sum(stepped * stepped, axis=1, keepdims=True)
        weight = stepped * jnp.sqrt(before / (after + epsilon))
        mstate[m] = moment
        wstate[m] = weight
        bank[b, m, mine, :] = weight.astype(bf16)

    def apply_fast(b):
        pltpu.make_async_copy(q_hbm.at[b], qbuf.at[b], load_sem.at[2, b]).wait()
        w1, w2, w3 = bank[b, 0], bank[b, 1], bank[b, 2]

        @pl.loop(0, tiles, unroll=UNROLL)
        def _(i):
            at = pl.ds(pl.multiple_of(i * tile, tile), tile)
            asked = qbuf[b, at, :]
            gate = mm_t(asked, w1)
            hidden = (gate * sigmoid(gate) * mm_t(asked, w3)).astype(bf16)
            obuf[b, at, :] = mm_t(hidden, w2).astype(bf16)

        pltpu.make_async_copy(obuf.at[b], out_hbm.at[b], store_sem.at[b]).start()

    prepare(0)
    for d in range(1, n):
        sq_copy(d).wait_recv()

    @pl.loop(0, total)
    def _(b):
        s = b // blocks
        g = b - s * blocks
        inner = (g + blocks - 1) // blocks
        entered = jnp.logical_and(jnp.logical_and(g == 0, s > 0), jnp.logical_not(first))

        @pl.when(g == 0)
        def _():
            for m in order:
                for d in around:
                    ent_copy(s, d, m).wait_recv()

        @pl.when(jnp.logical_and(jnp.logical_and(g == 0, s > 0), first))
        def _():
            wstate[...] = fw_in[...]
            mstate[...] = fm_in[...]

        @pl.when(entered)
        def _():
            for m in order:
                relay_copy(b - 1, s - 1, 0, m).wait_recv()
                wstate[m] = bank[total + s, m, mine, :].astype(f32)

        gradients(b, (total + s) * (1 - inner) + (b - 1) * inner)

        @pl.when(g > 0)
        def _():
            apply_fast(b - 1)

        @pl.when(entered)
        def _():
            m_copy(s - 1).wait_recv()
            mstate[...] = mrecv[s - 1].astype(f32)

        border = jnp.logical_and(g == blocks - 1, s < steps - 1)
        passing = jnp.logical_and(border, jnp.logical_not(last))
        square = sq[0, s, pl.ds(g, 1), :]
        for p in range(1, n):
            square = square + sq[p, s, pl.ds(g, 1), :]
        factor = lax.rsqrt(jnp.concatenate([square] * (head // LANES), axis=1))

        for m in order:
            for d in around:
                g_copy(b, d, m).wait_recv()
            update(b, m, factor)

            @pl.when(passing)
            def _():
                relay_copy(b, s, 0, m).start()

            for d in around:
                own_copy(b, d, m).start()

        @pl.when(passing)
        def _():
            msend[s] = mstate[...].astype(bf16)
            m_copy(s).start()

        for m in order:
            for d in around:
                g_copy(b, d, m).wait_send()

        @pl.when(b < total - 1)
        def _():
            prepare(b + 1)

        for m in order:
            for d in range(1, n):
                own_copy(b, d, m).wait_recv()

                @pl.when(passing)
                def _():
                    relay_copy(b, s, d, m).start()

        @pl.when(g == blocks - 1)
        def _():
            apply_fast(b)

        for m in order:
            for d in around:
                own_copy(b, d, m).wait_send()

        @pl.when(passing)
        def _():
            for m in order:
                for d in range(n):
                    relay_copy(b, s, d, m).wait_send()
            m_copy(s).wait_send()

    for d in around:
        sq_copy(d).wait_send()
        for m in order:
            ent_copy(0, d, m).wait_send()

    @pl.when(first)
    def _():
        for s in range(1, steps):
            for m in order:
                for d in around:
                    ent_copy(s, d, m).wait_send()

    for b in range(total):
        pltpu.make_async_copy(obuf.at[b], out_hbm.at[b], store_sem.at[b]).wait()


def gated(asked, w13):
    both = mm_t(asked, w13)
    half = both.shape[1] // 2
    gate = both[:, :half]
    return (gate * sigmoid(gate) * both[:, half:]).astype(bf16)


def apply_tiles(begin, stop, tile, weights, asked_ref, out_ref):
    @pl.loop(begin, stop, unroll=min(UNROLL, stop - begin))
    def _(i):
        at = pl.ds(pl.multiple_of(i * tile, tile), tile)
        asked = asked_ref[at, :]
        parts = [gated(asked, w13) for w13 in weights[:2]]
        out_ref[at, :] = mm_t(jnp.concatenate(parts, axis=1), weights[2]).astype(bf16)


def quad_kernel(
    segs, steps, blocks, tile,
    k_hbm, v_hbm, q_hbm, rates_hbm, w_hbm, m_hbm, fw_hbm, fm_hbm,
    obuf, usable, asked_last, begun, w_out, m_out,
    kbuf, vbuf, qbuf, kt, scaled, scaled_t, hid, bgu,
    bank, gs, got, mid, wst, mst,
    w_in, m_in, fw_in, fm_in, rates, mx, mr, msend, mrecv, sq,
    load_sem, in_sem, st_s, st_r, en_s, en_r, rl_s, rl_r, mm_s, mm_r, mx_s, mx_r, qs, qr,
):
    total = steps * blocks
    n = 4
    rows, head = kbuf.shape[1], kbuf.shape[2]
    half = head // 2
    tiles = rows // tile
    seg = lax.axis_index("seg")
    tok = lax.axis_index("tok")
    inner = lax.rem(tok, 2)
    outer = tok // 2
    first = seg == 0
    last = seg == segs - 1
    peers = [flip(tok, d) for d in range(n)]

    def to_peer(d):
        return {"seg": seg, "tok": peers[d]}

    gather_to = (to_peer(1), to_peer(2))
    cross_to = (to_peer(2), to_peer(1))
    down = {"seg": lax.rem(seg + 1, segs), "tok": tok}
    up = {"seg": lax.rem(seg + segs - 1, segs), "tok": tok}

    def rcopy(src, dst, send, recv, device):
        return pltpu.make_async_remote_copy(
            src_ref=src, dst_ref=dst, send_sem=send, recv_sem=recv,
            device_id=device, device_id_type=MESH,
        )

    barrier = pltpu.get_barrier_semaphore()
    for d in range(1, n):
        pl.semaphore_signal(barrier, inc=1, device_id=to_peer(d), device_id_type=MESH)

    @pl.when(jnp.logical_not(last))
    def _():
        pl.semaphore_signal(barrier, inc=1, device_id=down, device_id_type=MESH)

    @pl.when(jnp.logical_not(first))
    def _():
        pl.semaphore_signal(barrier, inc=1, device_id=up, device_id_type=MESH)

    inputs = [
        pltpu.make_async_copy(src, dst, in_sem.at[j])
        for j, (src, dst) in enumerate((
            (w_hbm, w_in), (m_hbm, m_in), (rates_hbm, rates), (fw_hbm, fw_in), (fm_hbm, fm_in),
        ))
    ]
    early = [
        pltpu.make_async_copy(src.at[0], dst.at[0], load_sem.at[j])
        for j, (src, dst) in enumerate(((k_hbm, kbuf), (v_hbm, vbuf)))
    ]
    rest = pl.ds(1, total - 1)
    later = [
        pltpu.make_async_copy(k_hbm.at[rest], kbuf.at[rest], load_sem.at[2]),
        pltpu.make_async_copy(v_hbm.at[rest], vbuf.at[rest], load_sem.at[3]),
        pltpu.make_async_copy(q_hbm.at[pl.ds(0, total - 1)], qbuf, load_sem.at[4]),
        pltpu.make_async_copy(q_hbm.at[total - 1], asked_last, load_sem.at[5]),
    ]
    for copy in (*inputs[:3], *early):
        copy.start()

    def fill_bank(e, source):
        bank[e, outer, 0, inner] = source[0].astype(bf16)
        bank[e, outer, 1, inner] = source[2].astype(bf16)
        bank[e, 2, outer, inner] = source[1].astype(bf16)

    def entry_copy(s, j, d):
        e = total + s
        piece = bank.at[e, 2, outer, inner] if j else bank.at[e, outer, :, inner]
        return rcopy(piece, piece, en_s.at[d - 1, j], en_r.at[s, d - 1, j], to_peer(d))

    def start_entry(s):
        @pl.when(outer == 0)
        def _():
            for j in (0, 1):
                for d in (3, 1, 2):
                    entry_copy(s, j, d).start()

        @pl.when(outer == 1)
        def _():
            for j in (1, 0):
                for d in (3, 1, 2):
                    entry_copy(s, j, d).start()

    def arrive_entry(s, c):
        @pl.when(outer == c)
        def _():
            entry_copy(s, 0, 1).wait_recv()

        @pl.when(outer != c)
        def _():
            for d in (2, 3):
                entry_copy(s, 0, d).wait_recv()

    def moment_copies(s, targets):
        return [
            rcopy(mx.at[s], mr.at[s, tok], mx_s.at[d - 1], mx_r.at[s, d - 1], to_peer(d))
            for d in targets
        ]

    def passed_moments(s):
        strip = head // 8
        copies = []
        for d in (1, 2):
            piece = mr.at[s, peers[3 - d], :, pl.ds((d - 1) * strip, strip), :]
            copies.append(rcopy(piece, piece, mx_s.at[1 + d], mx_r.at[s, 1 + d], to_peer(d)))
        return copies

    def square_copies():
        return [
            rcopy(sq.at[tok], sq.at[tok], qs.at[d - 1], qr.at[d - 1], to_peer(d)) for d in (1, 2, 3)
        ]

    def start(copies):
        for copy in copies:
            copy.start()

    def arrive(copies):
        for copy in copies:
            copy.wait_recv()

    def take_weights(s, weights):
        e = total + s
        for item in range(3):
            wst[item] = bank[e, item].astype(f32)
        wst[outer, 0, inner] = weights[0]
        wst[outer, 1, inner] = weights[2]
        wst[2, outer, inner] = weights[1]

    def take_moments(s, moments):
        for o in range(2):
            for i in range(2):
                @pl.when(tok != 2 * o + i)
                def _():
                    mst[o, 0, i] = mr[s, 2 * o + i, 0].astype(f32)
                    mst[o, 1, i] = mr[s, 2 * o + i, 2].astype(f32)
                    mst[2, o, i] = mr[s, 2 * o + i, 1].astype(f32)
        mst[outer, 0, inner] = moments[0]
        mst[outer, 1, inner] = moments[2]
        mst[2, outer, inner] = moments[1]

    inputs[0].wait()
    fill_bank(total, w_in)
    neighbours = (seg + segs - 1) // segs + (2 * segs - 2 - seg) // segs
    pl.semaphore_wait(barrier, n - 1 + neighbours)
    start_entry(0)
    for copy in later:
        copy.start()
    for copy in inputs[3:]:
        copy.start()
    inputs[1].wait()
    mx[0] = m_in[...].astype(bf16)
    inputs[2].wait()
    for s in range(steps):
        drawn = rates[s]
        sums = jnp.sum(drawn * drawn, axis=1, keepdims=True)
        sq[tok, s] = jnp.broadcast_to(sums, (blocks, LANES))
    start(square_copies())

    def prepare_keys(b):
        kt[...] = kbuf[b].T

    def prepare_values(b):
        s = b // blocks
        row = jnp.broadcast_to(rates[s, pl.ds(b - s * blocks, 1), :], (LANES, rows))
        column = jnp.concatenate([row.T] * (head // LANES), axis=1)
        product = (column * vbuf[b].astype(f32)).astype(bf16)
        scaled[...] = product
        scaled_t[...] = product.T

    def pair_copy(b, stage, item, p):
        return rcopy(
            (gs, mid)[stage].at[b, item, p], got.at[b, stage, item, p],
            st_s.at[item, p], st_r.at[lax.rem(b, 2), stage, item, p], (gather_to, cross_to)[stage][p],
        )

    def relay_copy(b, s, item):
        return rcopy(
            bank.at[b, item], bank.at[total + s + 1, item],
            rl_s.at[s, item], rl_r.at[s, item], down,
        )

    def m_copy(s):
        return rcopy(msend.at[s], mrecv.at[s], mm_s.at[s], mm_r.at[s], down)

    def matrix(slot, item):
        return bank[slot, item].reshape(head, head)

    def flow(b, slot, c):
        w13 = matrix(slot, c)
        w2 = matrix(slot, 2)[:, c * half:(c + 1) * half]

        @pl.loop(0, tiles, unroll=UNROLL)
        def _(i):
            at = pl.ds(pl.multiple_of(i * tile, tile), tile)
            both = mm_t(kbuf[b, at, :], w13)
            back = mm(scaled[at, :], w2)
            gate, up_pre = both[:, :half], both[:, half:]
            sig = sigmoid(gate)
            act = gate * sig
            slope = sig + act * (1.0 - sig)
            hid[at, c * half:(c + 1) * half] = (act * up_pre).astype(bf16)
            bgu[c, at, :half] = (back * up_pre * slope).astype(bf16)
            bgu[c, at, half:] = (back * act).astype(bf16)

    def gradient(b, item):
        if item < 2:
            grad = mm(kt[...], bgu[item]).astype(bf16).T
        else:
            grad = mm(scaled_t[...], hid[...]).astype(bf16)
        gs[b, item] = grad.reshape(gs.shape[2:])

    def launch(b, item):
        for p in range(2):
            pair_copy(b, 0, item, p).start()

    def pair_sum(b, item):
        for p in range(2):
            pair_copy(b, 0, item, p).wait_recv()
            mid[b, item, p] = (gs[b, item, p].astype(f32) + got[b, 0, item, p].astype(f32)).astype(bf16)
            pair_copy(b, 0, item, p).wait_send()
            pair_copy(b, 1, item, p).start()

    def step_half(b, item, p, factor, grad):
        moment = momentum_decay * mst[item, p] - grad * factor
        weight = wst[item, p]
        stepped = weight - learn_rate * moment
        before = jnp.sum(weight * weight, axis=2, keepdims=True)
        after = jnp.sum(stepped * stepped, axis=2, keepdims=True)
        weight = stepped * jnp.sqrt(before / (after + epsilon))
        mst[item, p] = moment
        wst[item, p] = weight
        bank[b, item, p] = weight.astype(bf16)

    def update(b, item):
        s = b // blocks
        g = b - s * blocks
        square = sq[0, s, pl.ds(g, 1), :]
        for p in range(1, n):
            square = square + sq[p, s, pl.ds(g, 1), :]
        factor = lax.rsqrt(jnp.concatenate([square] * (head // LANES), axis=1))

        for p in range(2):
            pair_copy(b, 1, item, p).wait_recv()
            pair_copy(b, 1, item, p).wait_send()
            grad = mid[b, item, p].astype(f32) + got[b, 1, item, p].astype(f32)
            step_half(b, item, p, factor, grad)

    def apply_fast(b, begin, stop):
        apply_tiles(begin, stop, tile, [matrix(b, item) for item in range(3)], qbuf.at[b], obuf.at[b])

    early[0].wait()
    prepare_keys(0)
    early[1].wait()
    prepare_values(0)
    for j in range(2):
        entry_copy(0, j, 3).wait_send()
    start(moment_copies(0, (1, 2)))
    for copy in inputs[3:]:
        copy.wait()
    cut = (tiles + 1) // 2

    @pl.loop(0, total)
    def _(b):
        s = b // blocks
        g = b - s * blocks
        inside = (g + blocks - 1) // blocks
        slot = (total + s) * (1 - inside) + (b - 1) * inside
        entered = jnp.logical_and(jnp.logical_and(g == 0, s > 0), jnp.logical_not(first))
        renewed = jnp.logical_and(jnp.logical_and(g == 0, s > 0), first)
        border = jnp.logical_and(g == blocks - 1, s < steps - 1)
        passing = jnp.logical_and(border, jnp.logical_not(last))

        newly = jnp.logical_and(g == 0, jnp.logical_or(first, s == 0))

        @pl.when(newly)
        def _():
            for d in (1, 2, 3):
                entry_copy(s, 1, d).wait_recv()
            arrive_entry(s, 0)

        @pl.when(entered)
        def _():
            for item in (0, 2):
                relay_copy(b - 1, s - 1, item).wait_recv()

        flow(b, slot, 0)
        gradient(b, 0)
        launch(b, 0)

        @pl.when(g > 0)
        def _():
            update(b - 1, 1)

        @pl.when(newly)
        def _():
            arrive_entry(s, 1)

        @pl.when(entered)
        def _():
            relay_copy(b - 1, s - 1, 1).wait_recv()

        flow(b, slot, 1)
        gradient(b, 2)
        launch(b, 2)
        gradient(b, 1)
        launch(b, 1)

        @pl.when(b == 0)
        def _():
            for copy in later[:3]:
                copy.wait()

        @pl.when(b < total - 1)
        def _():
            prepare_keys(b + 1)

        @pl.when(b == 0)
        def _():
            arrive(moment_copies(0, (1, 2)))
            start(passed_moments(0))

        @pl.when(b > 0)
        def _():
            apply_fast(b - 1, 0, cut)

        pair_sum(b, 0)

        @pl.when(b > 0)
        def _():
            apply_fast(b - 1, cut, tiles)

        pair_sum(b, 2)

        @pl.when(b < total - 1)
        def _():
            prepare_values(b + 1)

        pair_sum(b, 1)

        for step in range(1, steps):
            @pl.when(jnp.logical_and(first, b == 0))
            def _():
                fill_bank(total + step, fw_in)
                for j in range(2):
                    for d in (1, 2) if step == 1 else (1, 2, 3):
                        entry_copy(step - 1, j, d).wait_send()
                start_entry(step)

            @pl.when(jnp.logical_and(first, b == step * blocks - 1))
            def _():
                sent = moment_copies(0, (1, 2)) + passed_moments(0)
                for copy in sent if step == 1 else moment_copies(step - 1, (1, 2, 3)):
                    copy.wait_send()
                mx[step] = fm_in[...].astype(bf16)
                start(moment_copies(step, (1, 2, 3)))

        @pl.when(b == 0)
        def _():
            arrive(square_copies())
            take_weights(0, w_in)
            arrive(passed_moments(0))
            take_moments(0, m_in)

        @pl.when(renewed)
        def _():
            take_weights(s, fw_in)
            arrive(moment_copies(s, (1, 2, 3)))
            take_moments(s, fm_in)

        @pl.when(entered)
        def _():
            for item in range(3):
                wst[item] = bank[total + s, item].astype(f32)
            m_copy(s - 1).wait_recv()
            for item in range(3):
                mst[item] = mrecv[s - 1, item].astype(f32)

        def finish(item):
            update(b, item)

            @pl.when(passing)
            def _():
                relay_copy(b, s, item).start()

        finish(0)

        @pl.when(b == total - 1)
        def _():
            later[3].wait()
            w13 = matrix(b, 0)

            @pl.loop(0, tiles, unroll=UNROLL)
            def _(i):
                at = pl.ds(pl.multiple_of(i * tile, tile), tile)
                begun[at, :] = gated(asked_last[at, :], w13)


        finish(2)

        @pl.when(g == blocks - 1)
        def _():
            finish(1)

        @pl.when(passing)
        def _():
            for item in (0, 2, 1):
                msend[s, item] = mst[item].astype(bf16)
            m_copy(s).start()

    usable[...] = bank[total - 1]
    for ref, state in ((w_out, wst), (m_out, mst)):
        ref[0] = state[outer, 0, inner]
        ref[2] = state[outer, 1, inner]
        ref[1] = state[2, outer, inner]

    def drain_entry(peers_left, sent):
        for j in range(2):
            for d in peers_left:
                entry_copy(0, j, d).wait_send()
        for copy in sent:
            copy.wait_send()

    @pl.when(first)
    def _():
        drain_entry((1, 2, 3), moment_copies(steps - 1, (1, 2, 3)))

    @pl.when(jnp.logical_not(first))
    def _():
        drain_entry((1, 2), moment_copies(0, (1, 2)) + passed_moments(0))

    for copy in square_copies():
        copy.wait_send()

    @pl.when(jnp.logical_not(last))
    def _():
        for s in range(steps - 1):
            for item in range(3):
                relay_copy(s * blocks + blocks - 1, s, item).wait_send()
            m_copy(s).wait_send()


def tail_kernel(
    tile, done, usable, asked, begun, w_ready, m_ready, out_hbm, w_hbm, m_hbm, obuf, sem,
):
    count = done.shape[0]
    rows, head = asked.shape
    copies = [
        pltpu.make_async_copy(src, dst, sem.at[j])
        for j, (src, dst) in enumerate(
            [(w_ready, w_hbm), (m_ready, m_hbm)] + [(done.at[b], out_hbm.at[b]) for b in range(count)]
        )
    ]
    for copy in copies:
        copy.start()
    weights = [usable[item].reshape(head, head) for item in range(3)]
    for i in range(rows // tile):
        at = pl.ds(i * tile, tile)
        hidden = jnp.concatenate([begun[at, :], gated(asked[at, :], weights[1])], axis=1)
        obuf[at, :] = mm_t(hidden, weights[2]).astype(bf16)
        copy = pltpu.make_async_copy(obuf.at[at], out_hbm.at[count, at], sem.at[count + 2 + i])
        copy.start()
        copies.append(copy)
    for copy in copies:
        copy.wait()


def quad_scratch(steps, blocks, rows, head):
    total = steps * blocks
    quarter = head // 4
    flat = (total, rows, head)
    whole = (2, 2, quarter, head)
    piece = (3, quarter, head)
    dma = pltpu.SemaphoreType.DMA
    vmem = pltpu.VMEM
    return [vmem(flat, bf16)] * 2 + [
        vmem((total - 1, rows, head), bf16),
        vmem((head, rows), bf16),
        vmem((rows, head), bf16),
        vmem((head, rows), bf16),
        vmem((rows, head), bf16),
        vmem((2, rows, head), bf16),
        vmem((total + steps, 3) + whole, bf16),
        vmem((total, 3) + whole, bf16),
        vmem((total, 2, 3) + whole, bf16),
        vmem((total, 3) + whole, bf16),
        vmem((3,) + whole, f32),
        vmem((3,) + whole, f32),
        vmem(piece, f32),
        vmem(piece, f32),
        vmem(piece, f32),
        vmem(piece, f32),
        vmem((steps, blocks, rows), f32),
        vmem((steps,) + piece, bf16),
        vmem((steps, 4) + piece, bf16),
        vmem((steps, 3) + whole, bf16),
        vmem((steps, 3) + whole, bf16),
        vmem((4, steps, blocks, LANES), f32),
        dma((6,)),
        dma((5,)),
        dma((3, 2)),
        dma((2, 2, 3, 2)),
        dma((3, 2)),
        dma((steps, 3, 2)),
        dma((steps - 1, 3)),
        dma((steps - 1, 3)),
        dma((steps - 1,)),
        dma((steps - 1,)),
        dma((4,)),
        dma((steps, 4)),
        dma((3,)),
        dma((3,)),
    ]


def body(n, segs, queries, keys, values, rates, weights, momenta, fresh_w, fresh_m):
    steps, _, blocks, rows, head = queries.shape
    total = steps * blocks
    width = head // n
    tile = 256 if rows % 256 == 0 else rows
    flat = (total, rows, head)
    piece = (3, width, head)
    hbm = pl.BlockSpec(memory_space=pl.ANY)
    vmem = pl.BlockSpec(memory_space=pltpu.VMEM)
    dma = pltpu.SemaphoreType.DMA
    big = (rows, head)
    turned = (head, rows)
    operands = (
        keys.reshape(flat), values.reshape(flat), queries.reshape(flat), rates[:, 0],
        jnp.swapaxes(weights[0], 1, 2), jnp.swapaxes(momenta[0], 1, 2),
        jnp.swapaxes(fresh_w, 1, 2), jnp.swapaxes(fresh_m, 1, 2),
    )
    results = (
        jax.ShapeDtypeStruct(flat, bf16),
        jax.ShapeDtypeStruct(piece, f32),
        jax.ShapeDtypeStruct(piece, f32),
    )
    if n == 4 and head % 256 == 0 and min(steps, blocks) > 1:
        ready = pl.pallas_call(
            functools.partial(quad_kernel, segs, steps, blocks, tile),
            out_shape=(
                jax.ShapeDtypeStruct((total - 1, rows, head), bf16),
                jax.ShapeDtypeStruct((3, 2, 2, head // 4, head), bf16),
                jax.ShapeDtypeStruct(big, bf16),
                jax.ShapeDtypeStruct((rows, head // 2), bf16),
                *results[1:],
            ),
            in_specs=[pl.BlockSpec(memory_space=pltpu.HBM)] * 8,
            out_specs=(vmem,) * 6,
            scratch_shapes=quad_scratch(steps, blocks, rows, head),
            compiler_params=pltpu.CompilerParams(
                collective_id=0, has_side_effects=True, vmem_limit_bytes=QUAD_VMEM
            ),
        )(*(pltpu.with_memory_space_constraint(x, pltpu.HBM) for x in operands))
        outs = pl.pallas_call(
            functools.partial(tail_kernel, tile),
            out_shape=results,
            in_specs=[vmem] * 6,
            out_specs=(hbm,) * 3,
            scratch_shapes=[pltpu.VMEM(big, bf16), dma((total + 1 + rows // tile,))],
            compiler_params=pltpu.CompilerParams(vmem_limit_bytes=16 * 1024 * 1024),
        )(*ready)
    else:
        outs = pl.pallas_call(
            functools.partial(kernel, n, segs, steps, blocks, tile),
            out_shape=results,
            in_specs=[hbm, hbm, hbm, vmem, vmem, vmem, vmem, vmem],
            out_specs=(hbm, vmem, vmem),
            scratch_shapes=[pltpu.VMEM(flat, bf16)] * 4 + [
                pltpu.VMEM(turned, bf16),
                pltpu.VMEM(big, bf16),
                pltpu.VMEM(turned, bf16),
                pltpu.VMEM(big, bf16),
                pltpu.VMEM(big, bf16),
                pltpu.VMEM(big, bf16),
                pltpu.VMEM((3, head, head), bf16),
                pltpu.VMEM((total, n) + piece, bf16),
                pltpu.VMEM((total + steps, 3, head, head), bf16),
                pltpu.VMEM((steps,) + piece, bf16),
                pltpu.VMEM((steps,) + piece, bf16),
                pltpu.VMEM((n, steps, blocks, LANES), f32),
                dma((3, total)),
                dma((total,)),
                dma((total, n, 3)),
                dma((total, n, 3)),
                dma((total, n, 3)),
                dma((total, n, 3)),
                dma((steps, n, 3)),
                dma((steps, n, 3)),
                dma((steps,)),
                dma((steps,)),
                dma((n,)),
                dma((n,)),
        ],
            compiler_params=pltpu.CompilerParams(
                collective_id=0, has_side_effects=True, vmem_limit_bytes=60 * 1024 * 1024
            ),
        )(*operands)
    return (
        outs[0].reshape(queries.shape),
        jnp.swapaxes(outs[1], 1, 2)[None],
        jnp.swapaxes(outs[2], 1, 2)[None],
    )


def solution(mesh):
    n, segs = mesh.shape["tok"], mesh.shape["seg"]
    return jax.shard_map(
        functools.partial(body, n, segs),
        mesh=mesh,
        in_specs=(
            P(None, "seg", None, "tok", None),
            P(None, "seg", None, "tok", None),
            P(None, "seg", None, "tok", None),
            P(None, "seg", None, "tok"),
            P("seg", None, None, "tok"),
            P("seg", None, None, "tok"),
            P(None, None, "tok"),
            P(None, None, "tok"),
        ),
        out_specs=(
            P(None, "seg", None, "tok", None),
            P("seg", None, None, "tok"),
            P("seg", None, None, "tok"),
        ),
        check_vma=False,
    )
```
